32 devices in a mesh: dp: 1 (over z), tp: 32 (over y, x, core).
Axes of the slice: x: 4, y: 4, z: 1, core: 2. Of those that a mesh axis runs over, the one named last changes fastest.
The devices are a block of a 4x4x8 slice.
Arguments:
- x_a: bfloat16 [4096, 2048], P(('dp', 'tp'))
- x_b: bfloat16 [4096, 2048], P(('dp', 'tp'))
- labels_a: int32 [4096], P(('dp', 'tp'))
- labels_b: int32 [4096], P(('dp', 'tp'))
- w_head: bfloat16 [2048, 49152], P(None, 'tp')
Outputs:
- output 1: float32 [2], P('dp')
- output 2: bfloat16 [2048, 49152], P('dp', 'tp')
- output 3: bfloat16 [4096, 2048], P(('dp', 'tp'))
- output 4: bfloat16 [4096, 2048], P(('dp', 'tp'))
All inputs are finite; a program needn't handle non-finite values.
Results may differ from the reference program's by a relative error of at most 0.001.
Values are sent between devices in bfloat16 or wider.
A program may use at most 768 MiB of HBM per device.

```python
import math
import jax
import jax.numpy as jnp
from jax import lax

TOKENS = 4096
HIDDEN = 2048
VOCAB = 49152
VOCAB_SPLIT = 32


def draw_labels(label_key):
    value_key, first_key, gap_key = jax.random.split(label_key, 3)
    label_ids = jax.random.randint(value_key, (TOKENS,), 0, VOCAB, jnp.int32)
    first_pos = jax.random.randint(first_key, (), 0, TOKENS, jnp.int32)
    second_pos = (first_pos + jax.random.randint(gap_key, (), 1, TOKENS, jnp.int32)) % TOKENS
    return label_ids.at[first_pos].set(0).at[second_pos].set(VOCAB - 1)


def setup_inputs(seed: int = 0, part: int = 0) -> dict:
    part_key = jax.random.fold_in(jax.random.key(seed), part)
    key_xa, key_xb, key_la, key_lb = jax.random.split(part_key, 4)
    x_a = jax.random.normal(key_xa, (TOKENS, HIDDEN), jnp.float32).astype(jnp.bfloat16)
    x_b = jax.random.normal(key_xb, (TOKENS, HIDDEN), jnp.float32).astype(jnp.bfloat16)
    w_scale = 2.5 / math.sqrt(HIDDEN)
    w_head = (jax.random.normal(jax.random.key(seed + 1), (HIDDEN, VOCAB), jnp.float32) * w_scale).astype(jnp.bfloat16)
    return {"x_a": x_a, "x_b": x_b, "labels_a": draw_labels(key_la), "labels_b": draw_labels(key_lb), "w_head": w_head}


def reference(x_a, x_b, labels_a, labels_b, w_head):
    shard_cols = VOCAB // VOCAB_SPLIT
    w_blocks = w_head.reshape(HIDDEN, VOCAB_SPLIT, shard_cols).transpose(1, 0, 2)
    offsets = jnp.arange(VOCAB_SPLIT, dtype=jnp.int32) * shard_cols
    x_flat = jnp.concatenate([x_a, x_b], axis=0)
    label_flat = jnp.concatenate([labels_a, labels_b], axis=0)
    col_ids = jnp.arange(shard_cols, dtype=jnp.int32)[None, :]

    def block_stats(block_args):
        w_block, offset = block_args
        logits = jnp.dot(x_flat, w_block, preferred_element_type=jnp.float32)
        block_max = jnp.max(logits, axis=1)
        block_sum = jnp.sum(jnp.exp(logits - block_max[:, None]), axis=1)
        label_hit = col_ids == (label_flat - offset)[:, None]
        block_target = jnp.sum(jnp.where(label_hit, logits, 0.0), axis=1)
        return block_max, block_sum, block_target

    all_max, all_sum, all_target = lax.map(block_stats, (w_blocks, offsets))
    row_max = jnp.max(all_max, axis=0)
    row_sum = jnp.sum(all_sum * jnp.exp(all_max - row_max[None, :]), axis=0)
    target = jnp.sum(all_target, axis=0)
    loss_tok = row_max + jnp.log(row_sum) - target
    losses = jnp.stack([jnp.mean(loss_tok[:TOKENS]), jnp.mean(loss_tok[TOKENS:])])

    def block_grad(dx_acc, block_args):
        w_block, offset = block_args
        logits = jnp.dot(x_flat, w_block, preferred_element_type=jnp.float32)
        label_hit = col_ids == (label_flat - offset)[:, None]
        probs = jnp.exp(logits - row_max[:, None]) / row_sum[:, None]
        grad_logits = ((probs - label_hit.astype(jnp.float32)) / TOKENS).astype(jnp.bfloat16)
        grad_block = jnp.dot(x_flat.T, grad_logits, preferred_element_type=jnp.float32).astype(jnp.bfloat16)
        dx_acc = dx_acc + jnp.dot(grad_logits, w_block.T, preferred_element_type=jnp.float32)
        return dx_acc, grad_block

    dx_init = jnp.zeros((2 * TOKENS, HIDDEN), jnp.float32)
    dx_sum, grad_blocks = lax.scan(block_grad, dx_init, (w_blocks, offsets))
    grad_w = grad_blocks.transpose(1, 0, 2).reshape(HIDDEN, VOCAB)
    grad_x = dx_sum.astype(jnp.bfloat16)
    return losses, grad_w, grad_x[:TOKENS], grad_x[TOKENS:]
```

```python
import functools
import math

import jax
import jax.numpy as jnp
from jax import lax
from jax.experimental import pallas as pl
from jax.experimental.pallas import tpu as pltpu
from jax.sharding import PartitionSpec as P

MESH = pl.DeviceIdType.MESH
F32 = jnp.float32
BF16 = jnp.bfloat16
RINGS = 4
BLOCKS = 4
HALF = 3
PIECES = 2 * HALF
MBLOCKS = 8
BUFS = 3


def head_kernel(group, xa, xb, la, lb, w, loss, dw, dxa, dxb, e_hbm, xt_hbm,
                wv, xg, stage, xts, xtb, buf, dwr, dwb, dxo, m_store, s_store, t_store, labc,
                lab_in, st_out, st_in, bc_in, bc_out, ls_out, ls_in,
                x_sem, w_sem, wp_sem, lab_sem, ag_send, ag_recv, e_sem, xt_sem, xtr_sem, st_send, st_recv,
                bc_send, bc_recv, ls_sem, rs_send, rs_recv, credit, dw_send, dw_recv, dw_credit, dwo_sem, dxo_sem):
    chips = group // 2
    side = math.isqrt(chips)
    rows = xa.shape[0]
    slot_rows = 2 * rows
    rt = slot_rows // RINGS
    hb = xg.shape[2]
    pc = hb
    shard = w.shape[1]
    tokens = rows * group
    mb_rows = w.shape[0] // MBLOCKS
    lanes = lab_in.shape[2]

    me = lax.axis_index("tp")
    core = lax.rem(me, 2)
    chip = me // 2
    partner = me + 1 - 2 * core
    cx = lax.rem(chip, side)
    cy = chip // side
    diag = lax.rem(cx + cy, side)
    pos = (side * cy + diag, side * lax.rem(cx + 1, side) + diag)

    def dev(c):
        return {"tp": 2 * c + core}

    def chip_at(cycle, p):
        major, minor = p // side, lax.rem(p, side)
        if cycle == 0:
            yy = major
            xx = lax.rem(minor - major + side, side)
        else:
            xx = lax.rem(major + side - 1, side)
            yy = lax.rem(minor + 1 - major + side, side)
        return yy * side + xx

    def source(r, k):
        sign = -1 if r % 2 == 0 else 1
        return chip_at(r // 2, lax.rem(pos[r // 2] + sign * k + 2 * chips, chips))

    up = [source(r, 1) for r in range(RINGS)]
    down = [source(r, -1) for r in range(RINGS)]

    for b in range(BLOCKS):
        cols = pl.ds(b * hb, hb)
        pltpu.make_async_copy(xa.at[:, cols], xg.at[b, pl.ds(0, rows)], x_sem.at[2 * b]).start()
        pltpu.make_async_copy(xb.at[:, cols], xg.at[b, pl.ds(rows, rows)], x_sem.at[2 * b + 1]).start()
    pltpu.make_async_copy(w, wv.at[0], w_sem.at[0]).start()

    barrier = pltpu.get_barrier_semaphore()

    def hello(d, carry):
        pl.semaphore_signal(barrier, inc=1, device_id=dev(lax.rem(chip + d, chips)), device_id_type=MESH)
        return carry

    lax.fori_loop(1, chips, hello, 0)
    pl.semaphore_signal(barrier, inc=1, device_id={"tp": partner}, device_id_type=MESH)
    my_lab = lab_in.at[chip]
    my_lab[0:1, :] = la[...].astype(F32)
    my_lab[1:2, :] = lb[...].astype(F32)
    pl.semaphore_wait(barrier, chips)

    def ag_copy(k, j, r):
        src = xg.at[j, pl.ds(pl.multiple_of(k * slot_rows + r * rt, rt), rt)]
        dst = xg.at[j, pl.ds(pl.multiple_of((k + 1) * slot_rows + r * rt, rt), rt)]
        return pltpu.make_async_remote_copy(
            src_ref=src, dst_ref=dst, send_sem=ag_send.at[lax.rem(k, 4), j * RINGS + r],
            recv_sem=ag_recv.at[k + 1, j * RINGS + r], device_id=dev(down[r]), device_id_type=MESH)

    for b in range(BLOCKS):
        cols = pl.ds(b * hb, hb)
        pltpu.make_async_copy(xa.at[:, cols], xg.at[b, pl.ds(0, rows)], x_sem.at[2 * b]).wait()
        pltpu.make_async_copy(xb.at[:, cols], xg.at[b, pl.ds(rows, rows)], x_sem.at[2 * b + 1]).wait()
        for r in range(RINGS):
            ag_copy(0, b, r).start()

    w_swap = pltpu.make_async_remote_copy(
        src_ref=w, dst_ref=wv.at[1], send_sem=wp_sem.at[0], recv_sem=wp_sem.at[1],
        device_id={"tp": partner}, device_id_type=MESH)
    w_swap.start()

    def lab_copy(d):
        return pltpu.make_async_remote_copy(
            src_ref=lab_in.at[chip], dst_ref=lab_in.at[chip], send_sem=lab_sem.at[0, d], recv_sem=lab_sem.at[1, d],
            device_id=dev(lax.rem(chip + d, chips)), device_id_type=MESH)

    def lab_start(d, carry):
        lab_copy(d).start()
        return carry

    def lab_wait(d, carry):
        lab_copy(d).wait()
        return carry

    lax.fori_loop(1, chips, lab_start, 0)
    pltpu.make_async_copy(w, wv.at[0], w_sem.at[0]).wait()

    sub_i = lax.broadcasted_iota(jnp.int32, (rt, 128), 0)
    lane_i = lax.broadcasted_iota(jnp.int32, (rt, 128), 1)
    eye = sub_i == lane_i
    row_lane = lax.broadcasted_iota(jnp.int32, (1, 128), 1)
    lab_sub = lax.broadcasted_iota(jnp.int32, (rt, lanes), 0)
    lab_lane = lax.broadcasted_iota(jnp.int32, (rt, lanes), 1)
    piece_lane = lax.broadcasted_iota(jnp.int32, (slot_rows, 128), 1)

    def to_row(col):
        return jnp.sum(jnp.where(eye, col, 0.0), axis=0, keepdims=True)

    def to_col(row):
        return jnp.sum(jnp.where(eye, row, 0.0), axis=1, keepdims=True)

    def fill_labels(k):
        for r in range(RINGS):
            row = lab_in[source(r, k), r // 2:r // 2 + 1, :]
            col = jnp.sum(jnp.where(lab_lane == lab_sub + (r % 2) * rt, row, 0.0), axis=1, keepdims=True)
            labc[r * rt:(r + 1) * rt, :] = jnp.broadcast_to(col.astype(jnp.int32), (rt, 128))

    def base(lp):
        owner = me if lp < HALF else partner
        return owner * shard + (lp % HALF) * pc

    chunk = slot_rows // 8
    piece_iota = lax.broadcasted_iota(jnp.int32, (chunk, pc), 1)

    def z_piece(slot, lp):
        k0 = pl.multiple_of(slot * slot_rows, slot_rows)
        z = None
        for b in range(BLOCKS):
            part = jnp.dot(xg[b, pl.ds(k0, slot_rows), :],
                           wv[lp // HALF, b * hb:(b + 1) * hb, (lp % HALF) * pc:(lp % HALF + 1) * pc],
                           preferred_element_type=F32)
            z = part if z is None else z + part
        stage[lp] = z
        off = base(lp)
        for c in range(8):
            rs = slice(c * chunk, (c + 1) * chunk)
            zc = stage[lp, rs, :]
            m = jnp.max(zc, axis=1, keepdims=True)
            e = jnp.exp(zc - m)
            hit = piece_iota == labc[rs, 0:1] - off
            stage[lp, rs, :] = e
            m_store[pl.ds(pl.multiple_of(k0 + c * chunk, chunk), chunk), lp:lp + 1] = m
            s_store[rs, lp:lp + 1] = jnp.sum(e, axis=1, keepdims=True)
            t_store[rs, lp:lp + 1] = jnp.sum(jnp.where(hit, zc, 0.0), axis=1, keepdims=True)

    def e_write(slot, lp):
        return pltpu.make_async_copy(stage.at[lp], e_hbm.at[slot, lp], e_sem.at[lp])

    def xt_write(slot):
        return pltpu.make_async_copy(
            xts, xt_hbm.at[:, pl.ds(pl.multiple_of(slot * slot_rows, slot_rows), slot_rows)], xt_sem.at[0])

    def st_copy(slot, r):
        return pltpu.make_async_remote_copy(
            src_ref=st_out.at[slot, r], dst_ref=st_in.at[slot, r], send_sem=st_send.at[slot],
            recv_sem=st_recv.at[slot], device_id=dev(source(r, slot)), device_id_type=MESH)

    def poll(k, j):
        @pl.when(k < chips)
        def _():
            for r in range(RINGS):
                ag_copy(k - 1, j, r).wait_recv()

        @pl.when(k < chips - 1)
        def _():
            @pl.when(k >= 4)
            def _():
                for r in range(RINGS):
                    ag_copy(k - 4, j, r).wait_send()
            for r in range(RINGS):
                ag_copy(k, j, r).start()

    def gather_step(k, carry):
        slot = k - 1
        poll(k, 0)

        @pl.when(slot == 1)
        def _():
            lax.fori_loop(1, chips, lab_wait, 0)

        @pl.when(slot >= 1)
        def _():
            for lp in range(PIECES):
                e_write(slot - 1, lp).wait()
            xt_write(slot - 1).wait()

        fill_labels(slot)
        k0 = pl.multiple_of(slot * slot_rows, slot_rows)
        for blk in range(HALF):
            if blk == 1:
                @pl.when(slot == 0)
                def _():
                    w_swap.wait()
            for lp in (2 * blk, 2 * blk + 1):
                z_piece(slot, lp)
            for lp in (2 * blk, 2 * blk + 1):
                e_write(slot, lp).start()
            poll(k, blk + 1)
        for b in range(BLOCKS):
            xts[b * hb:(b + 1) * hb, :] = xg[b, pl.ds(k0, slot_rows), :].T
        xt_write(slot).start()

        valid = piece_lane < PIECES
        m_all = m_store[pl.ds(k0, slot_rows), :]
        m = jnp.max(jnp.where(valid, m_all, -jnp.inf), axis=1, keepdims=True)
        s = jnp.sum(jnp.where(valid, s_store[...] * jnp.exp(m_all - m), 0.0), axis=1, keepdims=True)
        t = jnp.sum(jnp.where(valid, t_store[...], 0.0), axis=1, keepdims=True)
        for r in range(RINGS):
            rs = slice(r * rt, (r + 1) * rt)
            tile = st_out.at[slot, r]
            tile[0:1, :] = to_row(m[rs])
            tile[1:2, :] = to_row(s[rs])
            tile[2:3, :] = to_row(t[rs])

        @pl.when(slot == 0)
        def _():
            for r in range(RINGS):
                st_in[0, r] = st_out[0, r]

        @pl.when(slot >= 1)
        def _():
            for r in range(RINGS):
                st_copy(slot, r).start()
        return carry

    lax.fori_loop(1, chips + 1, gather_step, 0)

    for lp in range(PIECES):
        e_write(chips - 1, lp).wait()

    def e_read(slot, lp):
        return pltpu.make_async_copy(e_hbm.at[slot, lp], stage.at[lp], e_sem.at[lp])

    for lp in range(PIECES):
        e_read(1, lp).start()
    xt_write(chips - 1).wait()

    def xt_read(mb):
        return pltpu.make_async_copy(
            xt_hbm.at[pl.ds(pl.multiple_of(mb * mb_rows, mb_rows), mb_rows), :], xtb.at[lax.rem(mb, 2)],
            xtr_sem.at[lax.rem(mb, 2)])

    xt_read(0).start()
    buf[0] = jnp.zeros(buf.shape[1:], F32)
    for k in range(chips - 5, chips - 1):
        for j in range(BLOCKS):
            for r in range(RINGS):
                ag_copy(k, j, r).wait_send()

    def st_wait(k, carry):
        pltpu.make_async_copy(st_in.at[k], st_in.at[k], st_recv.at[k]).wait()
        return carry

    lax.fori_loop(1, chips, st_wait, 0)
    inside = row_lane < rt
    parts = []
    for r in range(RINGS):
        m = st_in[0, r, 0:1, :]
        for k in range(1, chips):
            m = jnp.maximum(m, st_in[k, r, 0:1, :])
        s = jnp.zeros_like(m)
        t = jnp.zeros_like(m)
        for k in range(chips):
            s = s + st_in[k, r, 1:2, :] * jnp.exp(st_in[k, r, 0:1, :] - m)
            t = t + st_in[k, r, 2:3, :]
        bc_out[r:r + 1, :] = m
        bc_out[RINGS + r:RINGS + r + 1, :] = s
        parts.append(jnp.sum(jnp.where(inside, m + jnp.log(s) - t, 0.0), axis=1, keepdims=True))
    for mb in range(2):
        both = jnp.broadcast_to(parts[2 * mb] + parts[2 * mb + 1], (1, 128))
        bc_out[mb:mb + 1, :] = jnp.where(inside, bc_out[mb:mb + 1, :], both)
    bc_in[chip] = bc_out[...]

    def bc_copy(d):
        return pltpu.make_async_remote_copy(
            src_ref=bc_out, dst_ref=bc_in.at[chip], send_sem=bc_send.at[d], recv_sem=bc_recv.at[d],
            device_id=dev(lax.rem(chip + d, chips)), device_id_type=MESH)

    def bc_start(d, carry):
        bc_copy(d).start()
        return carry

    def bc_wait(d, carry):
        bc_copy(d).wait()
        return carry

    lax.fori_loop(1, chips, bc_start, 0)
    lax.fori_loop(1, chips, bc_wait, 0)

    def st_done(k, carry):
        pltpu.make_async_copy(st_out.at[k], st_out.at[k], st_send.at[k]).wait()
        return carry

    lax.fori_loop(1, chips, st_done, 0)
    total = bc_in[0]
    for c in range(1, chips):
        total = total + bc_in[c]
    ls_out[...] = total
    ls_copy = pltpu.make_async_remote_copy(
        src_ref=ls_out, dst_ref=ls_in, send_sem=ls_sem.at[0], recv_sem=ls_sem.at[1],
        device_id={"tp": partner}, device_id_type=MESH)
    ls_copy.start()

    def form_g(slot, prefetch):
        k0 = pl.multiple_of(slot * slot_rows, slot_rows)
        fill_labels(slot)
        m_cols = []
        inv_cols = []
        for r in range(RINGS):
            src = source(r, slot)
            m_cols.append(to_col(bc_in[src, r:r + 1, :]))
            inv_cols.append(1.0 / (to_col(bc_in[src, RINGS + r:RINGS + r + 1, :]) * tokens))
        for r in range(RINGS):
            rs = slice(r * rt, (r + 1) * rt)
            krs = pl.ds(pl.multiple_of(k0 + r * rt, rt), rt)
            s_store[rs, :] = jnp.exp(m_store[krs, :] - m_cols[r]) * inv_cols[r]
        for lp in range(PIECES):
            e_read(slot, lp).wait()
            off = base(lp)
            for c in range(8):
                rs = slice(c * chunk, (c + 1) * chunk)
                hit = piece_iota == labc[rs, 0:1] - off
                g = stage[lp, rs, :] * s_store[rs, lp:lp + 1] - jnp.where(hit, 1.0 / tokens, 0.0)
                xg[lp, pl.ds(pl.multiple_of(k0 + c * chunk, chunk), chunk), :] = g.astype(BF16)
            prefetch(lp)

    def start_next(slot):
        def go(lp):
            e_read(slot, lp).start()
        return go

    form_g(1, start_next(2))

    def rs_copy(s, j, r):
        b0, b1 = lax.rem(s, BUFS), lax.rem(s + 1, BUFS)
        return pltpu.make_async_remote_copy(
            src_ref=buf.at[b0, j, pl.ds(r * rt, rt)], dst_ref=buf.at[b1, j, pl.ds(r * rt, rt)],
            send_sem=rs_send.at[b0, j, r], recv_sem=rs_recv.at[b1, j, r],
            device_id=dev(down[r]), device_id_type=MESH)

    def dw_copy(mb, o):
        return pltpu.make_async_remote_copy(
            src_ref=stage.at[o], dst_ref=dwr.at[lax.rem(mb, 2), o], send_sem=dw_send.at[o],
            recv_sem=dw_recv.at[lax.rem(mb, 2), o], device_id={"tp": partner}, device_id_type=MESH)

    def dw_out(mb, o):
        return pltpu.make_async_copy(
            dwb.at[o], dw.at[pl.ds(pl.multiple_of(mb * mb_rows, mb_rows), mb_rows),
                             pl.ds(pl.multiple_of(o * pc, pc), pc)], dwo_sem.at[o])

    def dx_out(j):
        cols = pl.ds(pl.multiple_of(j * hb, hb), hb)
        return (pltpu.make_async_copy(dxo.at[j, pl.ds(0, rows)], dxa.at[:, cols], dxo_sem.at[j, 0]),
                pltpu.make_async_copy(dxo.at[j, pl.ds(rows, rows)], dxb.at[:, cols], dxo_sem.at[j, 1]))

    last = chips - 1
    g_steps = chips - 1
    dw_first = chips

    def scatter_step(i, carry):
        s = i // BLOCKS
        j = lax.rem(i, BLOCKS)
        k0 = pl.multiple_of(lax.rem(s + 1, chips) * slot_rows, slot_rows)
        b0 = lax.rem(s, BUFS)

        @pl.when(s >= 1)
        def _():
            for r in range(RINGS):
                rs_copy(s - 1, j, r).wait_recv()

        tile = None
        for lp in range(PIECES):
            part = lax.dot_general(
                xg[lp, pl.ds(k0, slot_rows), :],
                wv[lp // HALF, pl.ds(pl.multiple_of(j * hb, hb), hb), (lp % HALF) * pc:(lp % HALF + 1) * pc],
                (((1,), (1,)), ((), ())), preferred_element_type=F32)
            tile = part if tile is None else tile + part
        buf[b0, j] = buf[b0, j] + tile

        @pl.when(s < last)
        def _():
            @pl.when(s >= 2)
            def _():
                for r in range(RINGS):
                    pl.semaphore_wait(credit.at[j, r], 1)
            for r in range(RINGS):
                rs_copy(s, j, r).start()

        @pl.when(s == last)
        def _():
            dxo[j] = buf[b0, j].astype(BF16)
            for c in dx_out(j):
                c.start()

        @pl.when(i < g_steps)
        def _():
            nxt = lax.rem(i + 2, chips)

            def prefetch(lp):
                @pl.when(i < g_steps - 1)
                def _():
                    e_read(lax.rem(i + 3, chips), lp).start()
            form_g(nxt, prefetch)

        @pl.when((i >= dw_first) & (i < dw_first + MBLOCKS * PIECES))
        def _():
            q = i - dw_first
            mb = q // PIECES
            o = lax.rem(q, PIECES)
            lp = lax.rem(o + HALF, PIECES)

            @pl.when(o == 0)
            def _():
                xt_read(mb).wait()

                @pl.when(mb < MBLOCKS - 1)
                def _():
                    xt_read(mb + 1).start()

                @pl.when(mb >= 2)
                def _():
                    pl.semaphore_wait(dw_credit, 1)

            @pl.when((o < HALF) & (mb >= 1))
            def _():
                dw_copy(mb - 1, o).wait_send()
            stage[o] = jnp.dot(xtb[lax.rem(mb, 2)], xg[lp], preferred_element_type=F32)

            @pl.when(o < HALF)
            def _():
                dw_copy(mb, o).start()

            @pl.when(o >= HALF)
            def _():
                h = o - HALF
                dw_copy(mb, h).wait_recv()

                @pl.when(mb >= 1)
                def _():
                    dw_out(mb - 1, h).wait()
                dwb[h] = (stage[o] + dwr[lax.rem(mb, 2), h]).astype(BF16)
                dw_out(mb, h).start()

                @pl.when((h == HALF - 1) & (mb < MBLOCKS - 2))
                def _():
                    pl.semaphore_signal(dw_credit, inc=1, device_id={"tp": partner}, device_id_type=MESH)

        @pl.when(s >= 1)
        def _():
            for r in range(RINGS):
                rs_copy(s - 1, j, r).wait_send()

            @pl.when(s - 1 <= last - 3)
            def _():
                for r in range(RINGS):
                    pl.semaphore_signal(credit.at[j, r], inc=1, device_id=dev(up[r]), device_id_type=MESH)
        return carry

    lax.fori_loop(0, chips * BLOCKS, scatter_step, 0)

    ls_copy.wait()
    both = (ls_out[...] + ls_in[...]) * (1.0 / tokens)
    loss[0] = both[0, lanes - 1]
    loss[1] = both[1, lanes - 1]
    for o in range(HALF):
        dw_copy(MBLOCKS - 1, o).wait_send()
        dw_out(MBLOCKS - 1, o).wait()
    for j in range(BLOCKS):
        for c in dx_out(j):
            c.wait()


def solution(mesh):
    group = mesh.shape["tp"]
    chips = group // 2

    def local_step(x_a, x_b, labels_a, labels_b, w_local):
        rows, hidden = x_a.shape
        shard = w_local.shape[1]
        slot_rows = 2 * rows
        all_rows = chips * slot_rows
        hb = hidden // BLOCKS
        pc = shard // HALF
        mb_rows = hidden // MBLOCKS
        any_spec = pl.BlockSpec(memory_space=pl.ANY)
        vmem_spec = pl.BlockSpec(memory_space=pltpu.VMEM)
        dma = pltpu.SemaphoreType.DMA
        regular = pltpu.SemaphoreType.REGULAR
        out = pl.pallas_call(
            functools.partial(head_kernel, group),
            name="head",
            out_shape=(
                jax.ShapeDtypeStruct((2,), F32),
                jax.ShapeDtypeStruct((hidden, shard), BF16),
                jax.ShapeDtypeStruct((rows, hidden), BF16),
                jax.ShapeDtypeStruct((rows, hidden), BF16),
                jax.ShapeDtypeStruct((chips, PIECES, slot_rows, pc), F32),
                jax.ShapeDtypeStruct((hidden, all_rows), BF16),
            ),
            in_specs=[any_spec, any_spec, vmem_spec, vmem_spec, any_spec],
            out_specs=(pl.BlockSpec(memory_space=pltpu.SMEM), any_spec, any_spec, any_spec, any_spec, any_spec),
            scratch_shapes=[
                pltpu.VMEM((2, hidden, shard), BF16),
                pltpu.VMEM((PIECES, all_rows, pc), BF16),
                pltpu.VMEM((PIECES, slot_rows, pc), F32),
                pltpu.VMEM((hidden, slot_rows), BF16),
                pltpu.VMEM((2, mb_rows, all_rows), BF16),
                pltpu.VMEM((BUFS, BLOCKS, slot_rows, hb), F32),
                pltpu.VMEM((2, HALF, mb_rows, pc), F32),
                pltpu.VMEM((HALF, mb_rows, pc), BF16),
                pltpu.VMEM((BLOCKS, slot_rows, hb), BF16),
                pltpu.VMEM((all_rows, 128), F32),
                pltpu.VMEM((slot_rows, 128), F32),
                pltpu.VMEM((slot_rows, 128), F32),
                pltpu.VMEM((slot_rows, 128), jnp.int32),
                pltpu.VMEM((chips, 8, rows), F32),
                pltpu.VMEM((chips, RINGS, 8, 128), F32),
                pltpu.VMEM((chips, RINGS, 8, 128), F32),
                pltpu.VMEM((chips, 8, 128), F32),
                pltpu.VMEM((8, 128), F32),
                pltpu.VMEM((8, 128), F32),
                pltpu.VMEM((8, 128), F32),
                dma((2 * BLOCKS,)),
                dma((1,)),
                dma((2,)),
                dma((2, chips)),
                dma((4, BLOCKS * RINGS)),
                dma((chips, BLOCKS * RINGS)),
                dma((PIECES,)),
                dma((1,)),
                dma((2,)),
                dma((chips,)),
                dma((chips,)),
                dma((chips,)),
                dma((chips,)),
                dma((2,)),
                dma((BUFS, BLOCKS, RINGS)),
                dma((BUFS, BLOCKS, RINGS)),
                regular((BLOCKS, RINGS)),
                dma((HALF,)),
                dma((2, HALF)),
                regular,
                dma((HALF,)),
                dma((BLOCKS, 2)),
            ],
            compiler_params=pltpu.CompilerParams(
                collective_id=0, has_side_effects=True, vmem_limit_bytes=67043328),
        )(x_a, x_b, labels_a.reshape(1, rows), labels_b.reshape(1, rows), w_local)
        return out[0], out[1], out[2], out[3]

    row_spec = P(("dp", "tp"), None)
    label_spec = P(("dp", "tp"))
    return jax.shard_map(local_step, mesh=mesh, in_specs=(row_spec, row_spec, label_spec, label_spec, P(None, "tp")), out_specs=(P("dp"), P("dp", "tp"), row_spec, row_spec), check_vma=False)
```

```python
import functools
import math

import jax
import jax.numpy as jnp
from jax import lax
from jax.experimental import pallas as pl
from jax.experimental.pallas import tpu as pltpu
from jax.sharding import PartitionSpec as P

MESH = pl.DeviceIdType.MESH
F32 = jnp.float32
BF16 = jnp.bfloat16
RINGS = 4
BLOCKS = 4
HALF = 3
PIECES = 2 * HALF
MBLOCKS = 8
BUFS = 3


def head_kernel(group, *refs):
    chips = group // 2
    dma = pltpu.SemaphoreType.DMA
    regular = pltpu.SemaphoreType.REGULAR
    pl.run_scoped(
        functools.partial(head_body, group, *refs),
        x_sem=dma((2 * BLOCKS,)), w_sem=dma((1,)), wp_sem=dma((2,)), lab_sem=dma((2, chips)), sync=regular((3,)),
        ag_send=dma((4, BLOCKS * RINGS)), ag_recv=dma((chips, BLOCKS * RINGS)),
        e_sem=dma((PIECES,)), er_sem=dma((2,)), xt_sem=dma((1,)), xtr_sem=dma((2,)),
        st_send=dma((chips,)), st_recv=dma((chips,)), bc_send=dma((chips,)), bc_recv=dma((chips,)), ls_sem=dma((2,)),
        rs_send=dma((BUFS, BLOCKS, RINGS)), rs_recv=dma((BUFS, BLOCKS, RINGS)), credit=regular((BLOCKS, RINGS)),
        dw_send=dma((HALF,)), dw_recv=dma((2, HALF)), dw_credit=regular, dwo_sem=dma((HALF,)), dxo_sem=dma((BLOCKS, 2)))


def head_body(group, xa, xb, la, lb, w, loss, dw, dxa, dxb, e_hbm, xt_hbm,
              wv, xg, stage, stage1, xts, xtb, buf, dwb, m_run, s_run, t_run, labc,
              lab_in, st_out, st_in, bc_in, bc_out, ls_out, ls_in,
              x_sem, w_sem, wp_sem, lab_sem, sync, ag_send, ag_recv, e_sem, er_sem, xt_sem, xtr_sem, st_send, st_recv,
              bc_send, bc_recv, ls_sem, rs_send, rs_recv, credit, dw_send, dw_recv, dw_credit, dwo_sem, dxo_sem):
    chips = group // 2
    side = math.isqrt(chips)
    rows = xa.shape[0]
    slot_rows = 2 * rows
    rt = slot_rows // RINGS
    hb = xg.shape[2]
    pc = hb
    shard = w.shape[1]
    tokens = rows * group
    mb_rows = w.shape[0] // MBLOCKS
    lanes = lab_in.shape[2]

    me = lax.axis_index("tp")
    core = lax.rem(me, 2)
    chip = me // 2
    partner = me + 1 - 2 * core
    cx = lax.rem(chip, side)
    cy = chip // side
    diag = lax.rem(cx + cy, side)
    pos = (side * cy + diag, side * lax.rem(cx + 1, side) + diag)

    def dev(c):
        return {"tp": 2 * c + core}

    def chip_at(cycle, p):
        major, minor = p // side, lax.rem(p, side)
        if cycle == 0:
            yy = major
            xx = lax.rem(minor - major + side, side)
        else:
            xx = lax.rem(major + side - 1, side)
            yy = lax.rem(minor + 1 - major + side, side)
        return yy * side + xx

    def source(r, k):
        sign = -1 if r % 2 == 0 else 1
        return chip_at(r // 2, lax.rem(pos[r // 2] + sign * k + 2 * chips, chips))

    up = [source(r, 1) for r in range(RINGS)]
    down = [source(r, -1) for r in range(RINGS)]

    for b in range(BLOCKS):
        cols = pl.ds(b * hb, hb)
        pltpu.make_async_copy(xa.at[:, cols], xg.at[b, pl.ds(0, rows)], x_sem.at[2 * b]).start()
        pltpu.make_async_copy(xb.at[:, cols], xg.at[b, pl.ds(rows, rows)], x_sem.at[2 * b + 1]).start()
    pltpu.make_async_copy(w, wv.at[0], w_sem.at[0]).start()

    barrier = pltpu.get_barrier_semaphore()

    def is_near(c):
        near = c == up[0]
        for r in range(1, RINGS):
            near = near | (c == up[r])
        return near

    for r in range(RINGS):
        pl.semaphore_signal(barrier, inc=1, device_id=dev(up[r]), device_id_type=MESH)
    pl.semaphore_signal(barrier, inc=1, device_id={"tp": partner}, device_id_type=MESH)
    my_lab = lab_in.at[chip]
    my_lab[0:1, :] = la[...].astype(F32)
    my_lab[1:2, :] = lb[...].astype(F32)
    with jax.named_scope("barrier"):
        pl.semaphore_wait(barrier, RINGS + 1)

    def ag_copy(k, j, r):
        src = xg.at[j, pl.ds(pl.multiple_of(k * slot_rows + r * rt, rt), rt)]
        dst = xg.at[j, pl.ds(pl.multiple_of((k + 1) * slot_rows + r * rt, rt), rt)]
        return pltpu.make_async_remote_copy(
            src_ref=src, dst_ref=dst, send_sem=ag_send.at[lax.rem(k, 4), j * RINGS + r],
            recv_sem=ag_recv.at[k + 1, j * RINGS + r], device_id=dev(down[r]), device_id_type=MESH)

    for b in range(BLOCKS):
        cols = pl.ds(b * hb, hb)
        pltpu.make_async_copy(xa.at[:, cols], xg.at[b, pl.ds(0, rows)], x_sem.at[2 * b]).wait()
        pltpu.make_async_copy(xb.at[:, cols], xg.at[b, pl.ds(rows, rows)], x_sem.at[2 * b + 1]).wait()
        for r in range(RINGS):
            ag_copy(0, b, r).start()

    w_swap = pltpu.make_async_remote_copy(
        src_ref=w, dst_ref=wv.at[1], send_sem=wp_sem.at[0], recv_sem=wp_sem.at[1],
        device_id={"tp": partner}, device_id_type=MESH)
    w_swap.start()

    def lab_copy(d):
        return pltpu.make_async_remote_copy(
            src_ref=lab_in.at[chip], dst_ref=lab_in.at[chip], send_sem=lab_sem.at[0, d], recv_sem=lab_sem.at[1, d],
            device_id=dev(lax.rem(chip + d, chips)), device_id_type=MESH)

    def lab_start(near):
        def go(d, carry):
            is_to = is_near(lax.rem(chip + d, chips))

            @pl.when(is_to if near else jnp.logical_not(is_to))
            def _():
                lab_copy(d).start()
            return carry
        lax.fori_loop(1, chips, go, 0)

    def lab_wait(near):
        def go(d, carry):
            is_from = is_near(lax.rem(chip + chips - d, chips))

            @pl.when(is_from if near else jnp.logical_not(is_from))
            def _():
                lab_copy(d).wait_recv()
            return carry
        lax.fori_loop(1, chips, go, 0)

    def sync_signal(n):
        for r in range(RINGS):
            pl.semaphore_signal(sync.at[n], inc=1, device_id=dev(up[r]), device_id_type=MESH)

    def sync_wait(n):
        pl.semaphore_wait(sync.at[n], RINGS)

    lab_start(True)
    sync_signal(0)
    with jax.named_scope("w_wait"):
        pltpu.make_async_copy(w, wv.at[0], w_sem.at[0]).wait()

    sub_i = lax.broadcasted_iota(jnp.int32, (rt, 128), 0)
    lane_i = lax.broadcasted_iota(jnp.int32, (rt, 128), 1)
    eye = sub_i == lane_i
    row_lane = lax.broadcasted_iota(jnp.int32, (1, 128), 1)
    lab_sub = lax.broadcasted_iota(jnp.int32, (rt, lanes), 0)
    lab_lane = lax.broadcasted_iota(jnp.int32, (rt, lanes), 1)

    def to_row(col):
        return jnp.sum(jnp.where(eye, col, 0.0), axis=0, keepdims=True)

    def to_col(row):
        return jnp.sum(jnp.where(eye, row, 0.0), axis=1, keepdims=True)

    def fill_labels(lab, sources):
        for r in range(RINGS):
            row = lab_in[sources[r], r // 2:r // 2 + 1, :]
            col = jnp.sum(jnp.where(lab_lane == lab_sub + (r % 2) * rt, row, 0.0), axis=1, keepdims=True)
            lab[r * rt:(r + 1) * rt, :] = jnp.broadcast_to(col.astype(jnp.int32), (rt, 128))

    def sources_of(k):
        return [source(r, k) for r in range(RINGS)]

    def base(lp):
        owner = me if lp < HALF else partner
        return owner * shard + (lp % HALF) * pc

    chunk = slot_rows // 8
    lane_iota = lax.broadcasted_iota(jnp.int32, (chunk, 128), 1)
    cols4 = [slice(c * 128, (c + 1) * 128) for c in range(pc // 128)]
    shift = slice(pc, pc + 128)

    def z_dot(k0, lp):
        z = None
        for b in range(BLOCKS):
            part = jnp.dot(xg[b, pl.ds(k0, slot_rows), :],
                           wv[lp // HALF, b * hb:(b + 1) * hb, (lp % HALF) * pc:(lp % HALF + 1) * pc],
                           preferred_element_type=F32)
            z = part if z is None else z + part
        stage[lp, :, 0:pc] = z

    def z_stats(lp, lab):
        off = base(lp)
        for c in range(8):
            rs = slice(c * chunk, (c + 1) * chunk)
            z = [stage[lp, rs, cs] for cs in cols4]
            m = functools.reduce(jnp.maximum, z)
            e = [jnp.exp(v - m) for v in z]
            rel = lab[rs, :] - off
            t = functools.reduce(jnp.add, [jnp.where(lane_iota + i * 128 == rel, v, 0.0) for i, v in enumerate(z)])
            s = functools.reduce(jnp.add, e)
            for cs, v in zip(cols4, e):
                stage[lp, rs, cs] = v
            stage[lp, rs, shift] = m
            if lp == 0:
                m_run[rs, :] = m
                s_run[rs, :] = s
                t_run[rs, :] = t
            else:
                old = m_run[rs, :]
                new = jnp.maximum(old, m)
                m_run[rs, :] = new
                s_run[rs, :] = s_run[rs, :] * jnp.exp(old - new) + s * jnp.exp(m - new)
                t_run[rs, :] = t_run[rs, :] + t

    def e_write(slot, lp):
        return pltpu.make_async_copy(stage.at[lp], e_hbm.at[slot, lp], e_sem.at[lp])

    def xt_write(slot):
        return pltpu.make_async_copy(
            xts, xt_hbm.at[:, pl.ds(pl.multiple_of(slot * slot_rows, slot_rows), slot_rows)], xt_sem.at[0])

    def st_copy(slot, r):
        return pltpu.make_async_remote_copy(
            src_ref=st_out.at[slot, r], dst_ref=st_in.at[slot, r], send_sem=st_send.at[slot],
            recv_sem=st_recv.at[slot], device_id=dev(source(r, slot)), device_id_type=MESH)

    def poll(k, j):
        @pl.when(k < chips)
        def _():
            for r in range(RINGS):
                ag_copy(k - 1, j, r).wait_recv()

        @pl.when(k < chips - 1)
        def _():
            @pl.when(k >= 4)
            def _():
                for r in range(RINGS):
                    ag_copy(k - 4, j, r).wait_send()
            for r in range(RINGS):
                ag_copy(k, j, r).start()

    fill_labels(labc.at[0], [chip] * RINGS)

    def gather_step(k, carry):
        slot = k - 1
        k0 = pl.multiple_of(slot * slot_rows, slot_rows)
        lab = labc.at[lax.rem(slot, 2)]
        ahead = sources_of(lax.rem(slot + 1, chips))

        @pl.when(slot >= 1)
        def _():
            for lp in range(PIECES):
                e_write(slot - 1, lp).wait()
            xt_write(slot - 1).wait()

        with jax.named_scope("z0"):
            z_dot(k0, 0)
            z_dot(k0, 1)
            z_stats(0, lab)
        e_write(slot, 0).start()
        poll(k, 0)

        @pl.when(slot == 0)
        def _():
            sync_wait(0)
            sync_signal(1)
            w_swap.wait()

        with jax.named_scope("z1"):
            z_dot(k0, 2)
            z_dot(k0, 3)
            z_stats(1, lab)
            z_stats(2, lab)
        for lp in (1, 2):
            e_write(slot, lp).start()
        poll(k, 1)

        @pl.when(slot == 0)
        def _():
            sync_wait(1)
            sync_signal(2)
            lab_wait(True)

        @pl.when(slot == 1)
        def _():
            lab_wait(False)
        with jax.named_scope("z2"):
            z_dot(k0, 4)
            z_dot(k0, 5)
            z_stats(3, lab)
            z_stats(4, lab)
            fill_labels(labc.at[lax.rem(slot + 1, 2)], ahead)
            for b in range(BLOCKS):
                xts[b * hb:(b + 1) * hb, :] = xg[b, pl.ds(k0, slot_rows), :].T
        for lp in (3, 4):
            e_write(slot, lp).start()
        xt_write(slot).start()
        poll(k, 2)
        with jax.named_scope("z_end"):
            z_stats(5, lab)
        e_write(slot, 5).start()

        stats_scope = jax.named_scope("stats")
        stats_scope.__enter__()
        lane_m = m_run[...]
        m = jnp.max(lane_m, axis=1, keepdims=True)
        s = jnp.sum(s_run[...] * jnp.exp(lane_m - m), axis=1, keepdims=True)
        t = jnp.sum(t_run[...], axis=1, keepdims=True)
        for r in range(RINGS):
            rs = slice(r * rt, (r + 1) * rt)
            tile = st_out.at[slot, r]
            tile[0:1, :] = to_row(m[rs])
            tile[1:2, :] = to_row(s[rs])
            tile[2:3, :] = to_row(t[rs])
        stats_scope.__exit__(None, None, None)

        @pl.when(slot == 0)
        def _():
            for r in range(RINGS):
                st_in[0, r] = st_out[0, r]

        @pl.when(slot >= 1)
        def _():
            for r in range(RINGS):
                st_copy(slot, r).start()

        @pl.when(slot == 0)
        def _():
            sync_wait(2)
            lab_start(False)
        poll(k, 3)
        return carry

    lax.fori_loop(1, chips + 1, gather_step, 0)

    def e_read(slot, odd):
        return pltpu.make_async_copy(e_hbm.at[slot], stage1 if odd else stage, er_sem.at[odd])

    e_read(1, 1).start()
    for lp in range(PIECES):
        e_write(chips - 1, lp).wait()
    e_read(2, 0).start()
    xt_write(chips - 1).wait()

    def xt_read(mb):
        return pltpu.make_async_copy(
            xt_hbm.at[pl.ds(pl.multiple_of(mb * mb_rows, mb_rows), mb_rows), :], xtb.at[lax.rem(mb, 2)],
            xtr_sem.at[lax.rem(mb, 2)])

    xt_read(0).start()
    buf[0] = jnp.zeros(buf.shape[1:], F32)
    for k in range(chips - 5, chips - 1):
        for j in range(BLOCKS):
            for r in range(RINGS):
                ag_copy(k, j, r).wait_send()

    def st_wait(k, carry):
        pltpu.make_async_copy(st_in.at[k], st_in.at[k], st_recv.at[k]).wait()
        return carry

    with jax.named_scope("st_wait"):
        lax.fori_loop(1, chips, st_wait, 0)
    inside = row_lane < rt
    parts = []
    for r in range(RINGS):
        m = st_in[0, r, 0:1, :]
        for k in range(1, chips):
            m = jnp.maximum(m, st_in[k, r, 0:1, :])
        s = jnp.zeros_like(m)
        t = jnp.zeros_like(m)
        for k in range(chips):
            s = s + st_in[k, r, 1:2, :] * jnp.exp(st_in[k, r, 0:1, :] - m)
            t = t + st_in[k, r, 2:3, :]
        bc_out[r:r + 1, :] = m
        bc_out[RINGS + r:RINGS + r + 1, :] = s
        parts.append(jnp.sum(jnp.where(inside, m + jnp.log(s) - t, 0.0), axis=1, keepdims=True))
    for mb in range(2):
        both = jnp.broadcast_to(parts[2 * mb] + parts[2 * mb + 1], (1, 128))
        bc_out[mb:mb + 1, :] = jnp.where(inside, bc_out[mb:mb + 1, :], both)
    bc_in[chip] = bc_out[...]

    def bc_copy(d):
        return pltpu.make_async_remote_copy(
            src_ref=bc_out, dst_ref=bc_in.at[chip], send_sem=bc_send.at[d], recv_sem=bc_recv.at[d],
            device_id=dev(lax.rem(chip + d, chips)), device_id_type=MESH)

    def bc_start(d, carry):
        bc_copy(d).start()
        return carry

    def bc_wait_near(d, carry):
        @pl.when(is_near(lax.rem(chip + chips - d, chips)))
        def _():
            bc_copy(d).wait_recv()
        return carry

    def bc_wait_far(d, carry):
        @pl.when(jnp.logical_not(is_near(lax.rem(chip + chips - d, chips))))
        def _():
            bc_copy(d).wait_recv()
        bc_copy(d).wait_send()
        lab_copy(d).wait_send()
        pltpu.make_async_copy(st_out.at[d], st_out.at[d], st_send.at[d]).wait()
        return carry

    ls_copy = pltpu.make_async_remote_copy(
        src_ref=ls_out, dst_ref=ls_in, send_sem=ls_sem.at[0], recv_sem=ls_sem.at[1],
        device_id={"tp": partner}, device_id_type=MESH)

    lax.fori_loop(1, chips, bc_start, 0)
    with jax.named_scope("bc_near"):
        lax.fori_loop(1, chips, bc_wait_near, 0)

    def form_g(slot, src_stage):
        k0 = pl.multiple_of(slot * slot_rows, slot_rows)
        sources = sources_of(slot)
        lab = labc.at[0]
        fill_labels(lab, sources)
        for r in range(RINGS):
            rs = slice(r * rt, (r + 1) * rt)
            m_run[rs, :] = jnp.broadcast_to(to_col(bc_in[sources[r], r:r + 1, :]), (rt, 128))
            s_run[rs, :] = jnp.broadcast_to(
                1.0 / (to_col(bc_in[sources[r], RINGS + r:RINGS + r + 1, :]) * tokens), (rt, 128))
        for lp in range(PIECES):
            off = base(lp)
            for c in range(8):
                rs = slice(c * chunk, (c + 1) * chunk)
                rel = lab[rs, :] - off
                scale = jnp.exp(src_stage[lp, rs, shift] - m_run[rs, :]) * s_run[rs, :]
                for i, cs in enumerate(cols4):
                    g = src_stage[lp, rs, cs] * scale - jnp.where(lane_iota + i * 128 == rel, 1.0 / tokens, 0.0)
                    xg[lp, pl.ds(pl.multiple_of(k0 + c * chunk, chunk), chunk), cs] = g.astype(BF16)

    e_read(1, 1).wait()
    with jax.named_scope("g_first"):
        form_g(1, stage1)
    e_read(3, 1).start()

    def rs_copy(s, j, r):
        b0, b1 = lax.rem(s, BUFS), lax.rem(s + 1, BUFS)
        return pltpu.make_async_remote_copy(
            src_ref=buf.at[b0, j, pl.ds(r * rt, rt)], dst_ref=buf.at[b1, j, pl.ds(r * rt, rt)],
            send_sem=rs_send.at[b0, j, r], recv_sem=rs_recv.at[b1, j, r],
            device_id=dev(down[r]), device_id_type=MESH)

    def dw_copy(mb, o):
        return pltpu.make_async_remote_copy(
            src_ref=stage.at[o, :, pl.ds(0, pc)], dst_ref=stage1.at[lax.rem(mb, 2) * HALF + o, :, pl.ds(0, pc)], send_sem=dw_send.at[o],
            recv_sem=dw_recv.at[lax.rem(mb, 2), o], device_id={"tp": partner}, device_id_type=MESH)

    def dw_out(mb, o):
        return pltpu.make_async_copy(
            dwb.at[o], dw.at[pl.ds(pl.multiple_of(mb * mb_rows, mb_rows), mb_rows),
                             pl.ds(pl.multiple_of(o * pc, pc), pc)], dwo_sem.at[o])

    def dx_out(j):
        cols = pl.ds(pl.multiple_of(j * hb, hb), hb)
        return (pltpu.make_async_copy(xtb.at[0, pl.ds(0, rows), cols], dxa.at[:, cols], dxo_sem.at[j, 0]),
                pltpu.make_async_copy(xtb.at[0, pl.ds(rows, rows), cols], dxb.at[:, cols], dxo_sem.at[j, 1]))

    last = chips - 1
    g_iters = chips // 2
    dw_iters = MBLOCKS * PIECES
    dw_from = 1 + g_iters
    own_from = dw_from + dw_iters
    assert own_from == last * BLOCKS - BLOCKS + 1

    def dx_dot(slot, j):
        k0 = pl.multiple_of(slot * slot_rows, slot_rows)
        tile = None
        for lp in range(PIECES):
            part = lax.dot_general(
                xg[lp, pl.ds(k0, slot_rows), :],
                wv[lp // HALF, pl.ds(pl.multiple_of(j * hb, hb), hb), (lp % HALF) * pc:(lp % HALF + 1) * pc],
                (((1,), (1,)), ((), ())), preferred_element_type=F32)
            tile = part if tile is None else tile + part
        return tile

    def rs_arrive(s, j):
        with jax.named_scope("rs_wait"):
            for r in range(RINGS):
                rs_copy(s - 1, j, r).wait_recv()

    def rs_send_on(s, j):
        @pl.when(s >= 2)
        def _():
            for r in range(RINGS):
                pl.semaphore_wait(credit.at[j, r], 1)
        for r in range(RINGS):
            rs_copy(s, j, r).start()

    def rs_release(s, j):
        for r in range(RINGS):
            rs_copy(s - 1, j, r).wait_send()

        @pl.when(s - 1 <= last - 3)
        def _():
            for r in range(RINGS):
                pl.semaphore_signal(credit.at[j, r], inc=1, device_id=dev(up[r]), device_id_type=MESH)

    def scatter_g(i, carry):
        s = i // BLOCKS
        j = lax.rem(i, BLOCKS)
        b0 = lax.rem(s, BUFS)

        @pl.when(s >= 1)
        def _():
            rs_arrive(s, j)

        even = lax.rem(2 * i, chips)
        e_read(even, 0).wait()
        with jax.named_scope("dx_g"):
            buf[b0, j] = buf[b0, j] + dx_dot(s + 1, j)
            form_g(even, stage)
        rs_send_on(s, j)

        @pl.when(i < g_iters)
        def _():
            e_read(lax.rem(2 * i + 2, chips), 0).start()
            e_read(2 * i + 1, 1).wait()
            with jax.named_scope("g"):
                form_g(2 * i + 1, stage1)

        @pl.when(i < g_iters - 1)
        def _():
            e_read(2 * i + 3, 1).start()

        @pl.when(s >= 1)
        def _():
            rs_release(s, j)
        return carry

    with jax.named_scope("dx_first"):
        buf[0, 0] = dx_dot(1, 0)
    rs_send_on(0, 0)
    with jax.named_scope("bc_far"):
        lax.fori_loop(1, chips, bc_wait_far, 0)
    lax.fori_loop(1, 1 + g_iters, scatter_g, 0)
    pl.semaphore_signal(dw_credit, inc=1, device_id={"tp": partner}, device_id_type=MESH)
    total = bc_in[0]
    for c in range(1, chips):
        total = total + bc_in[c]
    ls_out[...] = total
    ls_copy.start()

    def scatter_dw(i, carry):
        s = i // BLOCKS
        j = lax.rem(i, BLOCKS)
        b0 = lax.rem(s, BUFS)
        q = i - dw_from
        mb = q // PIECES
        o = lax.rem(q, PIECES)
        rs_arrive(s, j)

        @pl.when(o == 0)
        def _():
            xt_read(mb).wait()

            @pl.when(mb < MBLOCKS - 1)
            def _():
                xt_read(mb + 1).start()

        @pl.when((o < HALF) & (mb >= 1))
        def _():
            dw_copy(mb - 1, o).wait_send()

        with jax.named_scope("dx_dw"):
            buf[b0, j] = buf[b0, j] + dx_dot(s + 1, j)
            stage[o, :, 0:pc] = jnp.dot(xtb[lax.rem(mb, 2)], xg[lax.rem(o + HALF, PIECES)], preferred_element_type=F32)
        rs_send_on(s, j)

        @pl.when((o == 0) & (mb != 1))
        def _():
            pl.semaphore_wait(dw_credit, 1)

        @pl.when(o < HALF)
        def _():
            dw_copy(mb, o).start()

        @pl.when(o >= HALF)
        def _():
            h = o - HALF
            dw_copy(mb, h).wait_recv()

            @pl.when(mb >= 1)
            def _():
                dw_out(mb - 1, h).wait()
            dwb[h] = (stage[o, :, 0:pc] + stage1[lax.rem(mb, 2) * HALF + h, :, 0:pc]).astype(BF16)
            dw_out(mb, h).start()

            @pl.when((h == HALF - 1) & (mb < MBLOCKS - 2))
            def _():
                pl.semaphore_signal(dw_credit, inc=1, device_id={"tp": partner}, device_id_type=MESH)

        rs_release(s, j)
        return carry

    lax.fori_loop(dw_from, own_from, scatter_dw, 0)

    def scatter_own(i, carry):
        s = i // BLOCKS
        j = lax.rem(i, BLOCKS)
        b0 = lax.rem(s, BUFS)
        rs_arrive(s, j)
        with jax.named_scope("dx"):
            buf[b0, j] = buf[b0, j] + dx_dot(s + 1, j)
        rs_send_on(s, j)

        with jax.named_scope("own"):
            stage1[j, :, 0:pc] = dx_dot(0, j)

        @pl.when(j == 1)
        def _():
            stage1[0, :, 0:pc] = dx_dot(0, 0)
        rs_release(s, j)
        return carry

    lax.fori_loop(own_from, last * BLOCKS, scatter_own, 0)

    def scatter_last(j, carry):
        rs_arrive(last, j)
        with jax.named_scope("out"):
            xtb[0, 0:slot_rows, pl.ds(pl.multiple_of(j * hb, hb), hb)] = (buf[last % BUFS, j] + stage1[j, :, 0:pc]).astype(BF16)
        for c in dx_out(j):
            c.start()
        rs_release(last, j)
        return carry

    lax.fori_loop(0, BLOCKS, scatter_last, 0)

    ls_copy.wait()
    both = (ls_out[...] + ls_in[...]) * (1.0 / tokens)
    loss[0] = both[0, lanes - 1]
    loss[1] = both[1, lanes - 1]
    for o in range(HALF):
        dw_copy(MBLOCKS - 1, o).wait_send()
        dw_out(MBLOCKS - 1, o).wait()
    for j in range(BLOCKS):
        for c in dx_out(j):
            c.wait()


def solution(mesh):
    group = mesh.shape["tp"]
    chips = group // 2

    def local_step(x_a, x_b, labels_a, labels_b, w_local):
        rows, hidden = x_a.shape
        shard = w_local.shape[1]
        slot_rows = 2 * rows
        all_rows = chips * slot_rows
        hb = hidden // BLOCKS
        pc = shard // HALF
        mb_rows = hidden // MBLOCKS
        any_spec = pl.BlockSpec(memory_space=pl.ANY)
        vmem_spec = pl.BlockSpec(memory_space=pltpu.VMEM)
        out = pl.pallas_call(
            functools.partial(head_kernel, group),
            name="head",
            out_shape=(
                jax.ShapeDtypeStruct((2,), F32),
                jax.ShapeDtypeStruct((hidden, shard), BF16),
                jax.ShapeDtypeStruct((rows, hidden), BF16),
                jax.ShapeDtypeStruct((rows, hidden), BF16),
                jax.ShapeDtypeStruct((chips, PIECES, slot_rows, pc + 128), F32),
                jax.ShapeDtypeStruct((hidden, all_rows), BF16),
            ),
            in_specs=[any_spec, any_spec, vmem_spec, vmem_spec, any_spec],
            out_specs=(pl.BlockSpec(memory_space=pltpu.SMEM), any_spec, any_spec, any_spec, any_spec, any_spec),
            scratch_shapes=[
                pltpu.VMEM((2, hidden, shard), BF16),
                pltpu.VMEM((PIECES, all_rows, pc), BF16),
                pltpu.VMEM((PIECES, slot_rows, pc + 128), F32),
                pltpu.VMEM((PIECES, slot_rows, pc + 128), F32),
                pltpu.VMEM((hidden, slot_rows), BF16),
                pltpu.VMEM((2, mb_rows, all_rows), BF16),
                pltpu.VMEM((BUFS, BLOCKS, slot_rows, hb), F32),
                pltpu.VMEM((HALF, mb_rows, pc), BF16),
                pltpu.VMEM((slot_rows, 128), F32),
                pltpu.VMEM((slot_rows, 128), F32),
                pltpu.VMEM((slot_rows, 128), F32),
                pltpu.VMEM((2, slot_rows, 128), jnp.int32),
                pltpu.VMEM((chips, 8, rows), F32),
                pltpu.VMEM((chips, RINGS, 8, 128), F32),
                pltpu.VMEM((chips, RINGS, 8, 128), F32),
                pltpu.VMEM((chips, 8, 128), F32),
                pltpu.VMEM((8, 128), F32),
                pltpu.VMEM((8, 128), F32),
                pltpu.VMEM((8, 128), F32),
            ],
            compiler_params=pltpu.CompilerParams(
                collective_id=0, has_side_effects=True, vmem_limit_bytes=67043328),
        )(x_a, x_b, labels_a.reshape(1, rows), labels_b.reshape(1, rows), w_local)
        return out[0], out[1], out[2], out[3]

    row_spec = P(("dp", "tp"), None)
    label_spec = P(("dp", "tp"))
    return jax.shard_map(local_step, mesh=mesh, in_specs=(row_spec, row_spec, label_spec, label_spec, P(None, "tp")), out_specs=(P("dp"), P("dp", "tp"), row_spec, row_spec), check_vma=False)
```

```python
import functools
import math

import jax
import jax.numpy as jnp
from jax import lax
from jax.experimental import pallas as pl
from jax.experimental.pallas import tpu as pltpu
from jax.sharding import PartitionSpec as P

MESH = pl.DeviceIdType.MESH
F32 = jnp.float32
BF16 = jnp.bfloat16
RINGS = 4
BLOCKS = 4
HALF = 3
PIECES = 2 * HALF
MBLOCKS = 8
BUFS = 3


def head_kernel(group, *refs):
    chips = group // 2
    dma = pltpu.SemaphoreType.DMA
    regular = pltpu.SemaphoreType.REGULAR
    pl.run_scoped(
        functools.partial(head_body, group, *refs),
        x_sem=dma((2 * BLOCKS,)), w_sem=dma((HALF,)), wp_sem=dma((2, HALF)), lab_sem=dma((2, chips)), sync=regular((3,)),
        ag_send=dma((4, BLOCKS * RINGS)), ag_recv=dma((chips, BLOCKS * RINGS)),
        e_sem=dma((HALF,)), er_sem=dma((2,)), xt_sem=dma((MBLOCKS,)), xtr_sem=dma((2,)),
        run_send=dma((chips, RINGS)), run_recv=dma((chips, RINGS)), bc_send=dma((chips,)), bc_recv=dma((chips,)),
        ls_sem=dma((2,)), rs_send=dma((BUFS, BLOCKS, RINGS)), rs_recv=dma((BUFS, BLOCKS, RINGS)),
        credit=regular((BLOCKS, RINGS)), dw_send=dma((HALF,)), dw_recv=dma((2, HALF)), dw_credit=regular,
        dwo_sem=dma((HALF,)), dxo_sem=dma((BLOCKS, 2)))


def head_body(group, xa, xb, la, lb, w, loss, dw, dxa, dxb, e_hbm, xt_hbm,
              wv, xg, stage, xtb, buf, dwb, m_run, s_run, t_run, labc,
              lab_in, run_out, run_in, bc_in, bc_out, ls_out, ls_in,
              x_sem, w_sem, wp_sem, lab_sem, sync, ag_send, ag_recv, e_sem, er_sem, xt_sem, xtr_sem, run_send, run_recv,
              bc_send, bc_recv, ls_sem, rs_send, rs_recv, credit, dw_send, dw_recv, dw_credit, dwo_sem, dxo_sem):
    chips = group // 2
    side = math.isqrt(chips)
    rows = xa.shape[0]
    slot_rows = 2 * rows
    rt = slot_rows // RINGS
    hb = xg.shape[2]
    pc = hb
    shard = w.shape[1]
    tokens = rows * group
    mb_rows = w.shape[0] // MBLOCKS
    lanes = lab_in.shape[2]

    me = lax.axis_index("tp")
    core = lax.rem(me, 2)
    chip = me // 2
    partner = me + 1 - 2 * core
    cx = lax.rem(chip, side)
    cy = chip // side
    diag = lax.rem(cx + cy, side)
    pos = (side * cy + diag, side * lax.rem(cx + 1, side) + diag)

    def dev(c):
        return {"tp": 2 * c + core}

    def chip_at(cycle, p):
        major, minor = p // side, lax.rem(p, side)
        if cycle == 0:
            yy = major
            xx = lax.rem(minor - major + side, side)
        else:
            xx = lax.rem(major + side - 1, side)
            yy = lax.rem(minor + 1 - major + side, side)
        return yy * side + xx

    def source(r, k):
        sign = -1 if r % 2 == 0 else 1
        return chip_at(r // 2, lax.rem(pos[r // 2] + sign * k + 2 * chips, chips))

    up = [source(r, 1) for r in range(RINGS)]
    down = [source(r, -1) for r in range(RINGS)]

    for b in range(BLOCKS):
        cols = pl.ds(b * hb, hb)
        pltpu.make_async_copy(xa.at[:, cols], xg.at[b, pl.ds(0, rows)], x_sem.at[2 * b]).start()
        pltpu.make_async_copy(xb.at[:, cols], xg.at[b, pl.ds(rows, rows)], x_sem.at[2 * b + 1]).start()

    def w_load(h):
        return pltpu.make_async_copy(w.at[:, pl.ds(h * pc, pc)], wv.at[h], w_sem.at[h])

    def w_swap(h):
        return pltpu.make_async_remote_copy(
            src_ref=w.at[:, pl.ds(h * pc, pc)], dst_ref=wv.at[HALF + h], send_sem=wp_sem.at[0, h],
            recv_sem=wp_sem.at[1, h], device_id={"tp": partner}, device_id_type=MESH)

    for h in range(HALF):
        w_load(h).start()

    barrier = pltpu.get_barrier_semaphore()

    def is_near(c):
        near = c == up[0]
        for r in range(1, RINGS):
            near = near | (c == up[r])
        return near

    for r in range(RINGS):
        pl.semaphore_signal(barrier, inc=1, device_id=dev(up[r]), device_id_type=MESH)
    pl.semaphore_signal(barrier, inc=1, device_id={"tp": partner}, device_id_type=MESH)
    my_lab = lab_in.at[chip]
    my_lab[0:1, :] = la[...].astype(F32)
    my_lab[1:2, :] = lb[...].astype(F32)
    buf[0] = jnp.zeros(buf.shape[1:], F32)
    with jax.named_scope("barrier"):
        pl.semaphore_wait(barrier, RINGS + 1)

    def ag_copy(k, j, r):
        src = xg.at[j, pl.ds(pl.multiple_of(k * slot_rows + r * rt, rt), rt)]
        dst = xg.at[j, pl.ds(pl.multiple_of((k + 1) * slot_rows + r * rt, rt), rt)]
        return pltpu.make_async_remote_copy(
            src_ref=src, dst_ref=dst, send_sem=ag_send.at[lax.rem(k, 4), j * RINGS + r],
            recv_sem=ag_recv.at[k + 1, j * RINGS + r], device_id=dev(down[r]), device_id_type=MESH)

    for b in range(BLOCKS):
        cols = pl.ds(b * hb, hb)
        pltpu.make_async_copy(xa.at[:, cols], xg.at[b, pl.ds(0, rows)], x_sem.at[2 * b]).wait()
        pltpu.make_async_copy(xb.at[:, cols], xg.at[b, pl.ds(rows, rows)], x_sem.at[2 * b + 1]).wait()
        for r in range(RINGS):
            ag_copy(0, b, r).start()

    for h in range(HALF):
        w_swap(h).start()

    def lab_copy(d):
        return pltpu.make_async_remote_copy(
            src_ref=lab_in.at[chip], dst_ref=lab_in.at[chip], send_sem=lab_sem.at[0, d], recv_sem=lab_sem.at[1, d],
            device_id=dev(lax.rem(chip + d, chips)), device_id_type=MESH)

    def lab_start(near):
        def go(d, carry):
            is_to = is_near(lax.rem(chip + d, chips))

            @pl.when(is_to if near else jnp.logical_not(is_to))
            def _():
                lab_copy(d).start()
            return carry
        lax.fori_loop(1, chips, go, 0)

    def lab_wait(near):
        def go(d, carry):
            is_from = is_near(lax.rem(chip + chips - d, chips))

            @pl.when(is_from if near else jnp.logical_not(is_from))
            def _():
                lab_copy(d).wait_recv()
            return carry
        lax.fori_loop(1, chips, go, 0)

    def sync_signal(n):
        for r in range(RINGS):
            pl.semaphore_signal(sync.at[n], inc=1, device_id=dev(up[r]), device_id_type=MESH)

    def sync_wait(n):
        pl.semaphore_wait(sync.at[n], RINGS)

    lab_start(True)
    sync_signal(0)
    for h in range(HALF):
        w_load(h).wait()

    sub_i = lax.broadcasted_iota(jnp.int32, (rt, 128), 0)
    lane_i = lax.broadcasted_iota(jnp.int32, (rt, 128), 1)
    eye = sub_i == lane_i
    row_lane = lax.broadcasted_iota(jnp.int32, (1, 128), 1)
    lab_sub = lax.broadcasted_iota(jnp.int32, (rt, lanes), 0)
    lab_lane = lax.broadcasted_iota(jnp.int32, (rt, lanes), 1)

    def to_row(col):
        return jnp.sum(jnp.where(eye, col, 0.0), axis=0, keepdims=True)

    def to_col(row):
        return jnp.sum(jnp.where(eye, row, 0.0), axis=1, keepdims=True)

    def fill_labels(lab, sources):
        for r in range(RINGS):
            row = lab_in[sources[r], r // 2:r // 2 + 1, :]
            col = jnp.sum(jnp.where(lab_lane == lab_sub + (r % 2) * rt, row, 0.0), axis=1, keepdims=True)
            lab[r * rt:(r + 1) * rt, :] = jnp.broadcast_to(col.astype(jnp.int32), (rt, 128))

    def sources_of(k):
        return [source(r, k) for r in range(RINGS)]

    def base(lp):
        owner = me if lp < HALF else partner
        return owner * shard + (lp % HALF) * pc

    chunk = slot_rows // 8
    lane_iota = lax.broadcasted_iota(jnp.int32, (chunk, 128), 1)
    cols4 = [slice(c * 128, (c + 1) * 128) for c in range(pc // 128)]
    shift = slice(pc, pc + 128)

    def z_dot(k0, lp):
        z = None
        for b in range(BLOCKS):
            part = jnp.dot(xg[b, pl.ds(k0, slot_rows), :], wv[lp, b * hb:(b + 1) * hb, :], preferred_element_type=F32)
            z = part if z is None else z + part
        stage[0, lp, :, 0:pc] = z

    def z_stats(lp, lab):
        off = base(lp)
        for c in range(8):
            rs = slice(c * chunk, (c + 1) * chunk)
            z = [stage[0, lp, rs, cs] for cs in cols4]
            m = functools.reduce(jnp.maximum, z)
            e = [jnp.exp(v - m) for v in z]
            rel = lab[rs, :] - off
            t = functools.reduce(jnp.add, [jnp.where(lane_iota + i * 128 == rel, v, 0.0) for i, v in enumerate(z)])
            s = functools.reduce(jnp.add, e)
            for cs, v in zip(cols4, e):
                stage[0, lp, rs, cs] = v
            stage[0, lp, rs, shift] = m
            if lp == 0:
                m_run[rs, :] = m
                s_run[rs, :] = s
                t_run[rs, :] = t
            else:
                old = m_run[rs, :]
                new = jnp.maximum(old, m)
                m_run[rs, :] = new
                s_run[rs, :] = s_run[rs, :] * jnp.exp(old - new) + s * jnp.exp(m - new)
                t_run[rs, :] = t_run[rs, :] + t

    def e_write(slot, pair):
        two = pl.ds(2 * pair, 2)
        return pltpu.make_async_copy(stage.at[0, two], e_hbm.at[slot, two], e_sem.at[pair])

    def xt_write(slot, mb):
        return pltpu.make_async_copy(
            xtb.at[1, :, pl.ds(mb * mb_rows, slot_rows)],
            xt_hbm.at[pl.ds(mb * mb_rows, mb_rows), pl.ds(pl.multiple_of(slot * slot_rows, slot_rows), slot_rows)],
            xt_sem.at[mb])

    def run_copy(slot, r):
        return pltpu.make_async_remote_copy(
            src_ref=run_out.at[slot, r], dst_ref=run_in.at[slot + 1, r], send_sem=run_send.at[slot, r],
            recv_sem=run_recv.at[slot + 1, r], device_id=dev(down[r]), device_id_type=MESH)

    def join_stats(slot):
        with jax.named_scope("stats"):
            lane_m = m_run[...]
            m = jnp.max(lane_m, axis=1, keepdims=True)
            s = jnp.sum(s_run[...] * jnp.exp(lane_m - m), axis=1, keepdims=True)
            t = jnp.sum(t_run[...], axis=1, keepdims=True)
            rows_mst = [[to_row(v[r * rt:(r + 1) * rt]) for v in (m, s, t)] for r in range(RINGS)]

        @pl.when(slot >= 1)
        def _():
            for r in range(RINGS):
                run_copy(slot - 1, r).wait_recv()
        for r in range(RINGS):
            m_r, s_r, t_r = rows_mst[r]
            m_in = run_in[slot, r, 0:1, :]
            m_new = jnp.maximum(m_in, m_r)
            run_out[slot, r, 0:1, :] = m_new
            run_out[slot, r, 1:2, :] = s_r * jnp.exp(m_r - m_new) + run_in[slot, r, 1:2, :] * jnp.exp(m_in - m_new)
            run_out[slot, r, 2:3, :] = t_r + run_in[slot, r, 2:3, :]

    def poll(k, j):
      with jax.named_scope("poll"):
        @pl.when(k < chips)
        def _():
            for r in range(RINGS):
                ag_copy(k - 1, j, r).wait_recv()

        @pl.when(k < chips - 1)
        def _():
            @pl.when(k >= 4)
            def _():
                for r in range(RINGS):
                    ag_copy(k - 4, j, r).wait_send()
            for r in range(RINGS):
                ag_copy(k, j, r).start()

    fill_labels(labc.at[0], [chip] * RINGS)
    for r in range(RINGS):
        run_in[0, r, 0:1, :] = jnp.full((1, 128), -jnp.inf, F32)
        run_in[0, r, 1:3, :] = jnp.zeros((2, 128), F32)

    def gather_step(k, carry):
        slot = k - 1
        k0 = pl.multiple_of(slot * slot_rows, slot_rows)
        here = labc.at[lax.rem(slot, 2)]
        other = labc.at[lax.rem(slot + 1, 2)]
        ahead = sources_of(lax.rem(slot + 1, chips))

        @pl.when(slot >= 1)
        def _():
            e_write(slot - 1, 0).wait()

        with jax.named_scope("u0"):
            z_dot(k0, 0)
            z_dot(k0, 1)
            z_stats(4, other)
            z_stats(5, other)

        @pl.when(slot == 0)
        def _():
            poll(k, 0)
        poll(k, 1)

        @pl.when(slot >= 1)
        def _():
            e_write(slot - 1, 2).start()
            join_stats(slot - 1)
            for r in range(RINGS):
                run_copy(slot - 1, r).start()
            e_write(slot - 1, 1).wait()

        @pl.when(slot == 0)
        def _():
            sync_wait(0)
            sync_signal(1)
            w_swap(0).wait()

        with jax.named_scope("u1"):
            z_dot(k0, 2)
            z_dot(k0, 3)
            z_stats(0, here)
            z_stats(1, here)
        e_write(slot, 0).start()
        poll(k, 2)

        @pl.when(slot == 0)
        def _():
            sync_wait(1)
            sync_signal(2)
            lab_wait(True)
            poll(k, 3)
            poll(k + 1, 0)
            w_swap(1).wait()
            w_swap(2).wait()

        @pl.when(slot >= 1)
        def _():
            e_write(slot - 1, 2).wait()
            for mb in range(MBLOCKS):
                xt_write(slot - 1, mb).wait()

        @pl.when(slot == 1)
        def _():
            lab_wait(False)

        with jax.named_scope("u2"):
            z_dot(k0, 4)
            z_dot(k0, 5)
            z_stats(2, here)
            z_stats(3, here)
            fill_labels(other, ahead)
            for mb in range(MBLOCKS):
                at = mb * mb_rows % hb
                xtb[1, :, mb * mb_rows:(mb + 1) * mb_rows] = xg[mb * mb_rows // hb, pl.ds(k0, slot_rows), at:at + mb_rows].T
        e_write(slot, 1).start()
        for mb in range(MBLOCKS):
            xt_write(slot, mb).start()

        @pl.when(slot >= 1)
        def _():
            poll(k, 3)
            poll(k + 1, 0)

        @pl.when(slot == 0)
        def _():
            sync_wait(2)
            lab_start(False)
        return carry

    lax.fori_loop(1, chips + 1, gather_step, 0)
    with jax.named_scope("flush"):
        z_stats(4, labc.at[(chips - 1) % 2])
        z_stats(5, labc.at[(chips - 1) % 2])
    e_write(chips - 1, 2).start()
    join_stats(chips - 1)

    inside = row_lane < rt
    parts = []
    for r in range(RINGS):
        m, s, t = (run_out[chips - 1, r, i:i + 1, :] for i in range(3))
        bc_out[r:r + 1, :] = m
        bc_out[RINGS + r:RINGS + r + 1, :] = s
        parts.append(jnp.sum(jnp.where(inside, m + jnp.log(s) - t, 0.0), axis=1, keepdims=True))
    for mb in range(2):
        both = jnp.broadcast_to(parts[2 * mb] + parts[2 * mb + 1], (1, 128))
        bc_out[mb:mb + 1, :] = jnp.where(inside, bc_out[mb:mb + 1, :], both)
    bc_in[chip] = bc_out[...]

    def bc_copy(d):
        return pltpu.make_async_remote_copy(
            src_ref=bc_out, dst_ref=bc_in.at[chip], send_sem=bc_send.at[d], recv_sem=bc_recv.at[d],
            device_id=dev(lax.rem(chip + d, chips)), device_id_type=MESH)

    def bc_start(d, carry):
        bc_copy(d).start()
        return carry

    first_four = [source(r, 2) for r in range(RINGS)]

    def is_first(c):
        near = c == first_four[0]
        for r in range(1, RINGS):
            near = near | (c == first_four[r])
        return near

    def bc_wait_first(d, carry):
        @pl.when(is_first(lax.rem(chip + chips - d, chips)))
        def _():
            bc_copy(d).wait_recv()
        return carry

    def bc_wait_rest(d, carry):
        @pl.when(jnp.logical_not(is_first(lax.rem(chip + chips - d, chips))))
        def _():
            bc_copy(d).wait_recv()
        bc_copy(d).wait_send()
        lab_copy(d).wait_send()
        for r in range(RINGS):
            run_copy(d - 1, r).wait_send()
        return carry

    ls_copy = pltpu.make_async_remote_copy(
        src_ref=ls_out, dst_ref=ls_in, send_sem=ls_sem.at[0], recv_sem=ls_sem.at[1],
        device_id={"tp": partner}, device_id_type=MESH)

    lax.fori_loop(1, chips, bc_start, 0)

    def e_read(g):
        return pltpu.make_async_copy(e_hbm.at[lax.rem(g, chips)], stage.at[lax.rem(g, 2)], er_sem.at[lax.rem(g, 2)])

    e_read(1).start()
    for pair in range(HALF):
        e_write(chips - 1, pair).wait()
    e_read(2).start()
    for mb in range(MBLOCKS):
        xt_write(chips - 1, mb).wait()

    def xt_read(mb):
        return pltpu.make_async_copy(
            xt_hbm.at[pl.ds(pl.multiple_of(mb * mb_rows, mb_rows), mb_rows), :], xtb.at[lax.rem(mb, 2)],
            xtr_sem.at[lax.rem(mb, 2)])

    xt_read(0).start()
    for k in range(chips - 5, chips - 1):
        for j in range(BLOCKS):
            for r in range(RINGS):
                ag_copy(k, j, r).wait_send()

    with jax.named_scope("bc_first"):
        lax.fori_loop(1, chips, bc_wait_first, 0)

    def form_g(g):
        slot = lax.rem(g, chips)
        half = lax.rem(g, 2)
        k0 = pl.multiple_of(slot * slot_rows, slot_rows)
        sources = sources_of(slot)
        holders = sources_of(lax.rem(slot + 1, chips))
        lab = labc.at[0]
        fill_labels(lab, sources)
        for r in range(RINGS):
            rs = slice(r * rt, (r + 1) * rt)
            m_run[rs, :] = jnp.broadcast_to(to_col(bc_in[holders[r], r:r + 1, :]), (rt, 128))
            s_run[rs, :] = jnp.broadcast_to(
                1.0 / (to_col(bc_in[holders[r], RINGS + r:RINGS + r + 1, :]) * tokens), (rt, 128))
        for lp in range(PIECES):
            off = base(lp)
            for c in range(8):
                rs = slice(c * chunk, (c + 1) * chunk)
                rel = lab[rs, :] - off
                scale = jnp.exp(stage[half, lp, rs, shift] - m_run[rs, :]) * s_run[rs, :]
                for i, cs in enumerate(cols4):
                    v = stage[half, lp, rs, cs] * scale - jnp.where(lane_iota + i * 128 == rel, 1.0 / tokens, 0.0)
                    xg[lp, pl.ds(pl.multiple_of(k0 + c * chunk, chunk), chunk), cs] = v.astype(BF16)

    e_read(1).wait()
    with jax.named_scope("g_first"):
        form_g(1)
    e_read(3).start()

    def rs_copy(s, j, r):
        b0, b1 = lax.rem(s, BUFS), lax.rem(s + 1, BUFS)
        return pltpu.make_async_remote_copy(
            src_ref=buf.at[b0, j, pl.ds(r * rt, rt)], dst_ref=buf.at[b1, j, pl.ds(r * rt, rt)],
            send_sem=rs_send.at[b0, j, r], recv_sem=rs_recv.at[b1, j, r],
            device_id=dev(down[r]), device_id_type=MESH)

    def dw_copy(mb, o):
        return pltpu.make_async_remote_copy(
            src_ref=stage.at[0, o, :, pl.ds(0, pc)], dst_ref=stage.at[1, lax.rem(mb, 2) * HALF + o, :, pl.ds(0, pc)],
            send_sem=dw_send.at[o],
            recv_sem=dw_recv.at[lax.rem(mb, 2), o], device_id={"tp": partner}, device_id_type=MESH)

    def dw_out(mb, o):
        return pltpu.make_async_copy(
            dwb.at[o], dw.at[pl.ds(pl.multiple_of(mb * mb_rows, mb_rows), mb_rows),
                             pl.ds(pl.multiple_of(o * pc, pc), pc)], dwo_sem.at[o])

    def dx_out(j):
        cols = pl.ds(pl.multiple_of(j * hb, hb), hb)
        return (pltpu.make_async_copy(xtb.at[0, pl.ds(0, rows), cols], dxa.at[:, cols], dxo_sem.at[j, 0]),
                pltpu.make_async_copy(xtb.at[0, pl.ds(rows, rows), cols], dxb.at[:, cols], dxo_sem.at[j, 1]))

    last = chips - 1
    dw_from = 3 * BLOCKS
    own_from = last * BLOCKS
    assert own_from - dw_from == MBLOCKS * PIECES and dw_from - 1 + BLOCKS == chips - 1

    def dx_dot(slot, j):
        k0 = pl.multiple_of(slot * slot_rows, slot_rows)
        tile = None
        for lp in range(PIECES):
            part = lax.dot_general(
                xg[lp, pl.ds(k0, slot_rows), :],
                wv[lp, pl.ds(pl.multiple_of(j * hb, hb), hb), :],
                (((1,), (1,)), ((), ())), preferred_element_type=F32)
            tile = part if tile is None else tile + part
        return tile

    def rs_arrive(s, j):
        with jax.named_scope("rs_wait"):
            for r in range(RINGS):
                rs_copy(s - 1, j, r).wait_recv()

    def rs_send_on(s, j):
        @pl.when(s >= 2)
        def _():
            for r in range(RINGS):
                pl.semaphore_wait(credit.at[j, r], 1)
        for r in range(RINGS):
            rs_copy(s, j, r).start()

    def rs_release(s, j):
        for r in range(RINGS):
            rs_copy(s - 1, j, r).wait_send()

        @pl.when(s - 1 <= last - 3)
        def _():
            for r in range(RINGS):
                pl.semaphore_signal(credit.at[j, r], inc=1, device_id=dev(up[r]), device_id_type=MESH)

    def scatter_g(i, carry):
        s = i // BLOCKS
        j = lax.rem(i, BLOCKS)
        b0 = lax.rem(s, BUFS)
        double = s == 1
        g = jnp.where(s == 0, i + 1, jnp.where(double, 2 * i - BLOCKS + 1, i + BLOCKS + 1))

        @pl.when(s >= 1)
        def _():
            rs_arrive(s, j)

        e_read(g).wait()
        with jax.named_scope("dx_g"):
            buf[b0, j] = buf[b0, j] + dx_dot(s + 1, j)
            form_g(g)
        rs_send_on(s, j)

        @pl.when(g + 2 <= chips)
        def _():
            e_read(g + 2).start()

        @pl.when(double)
        def _():
            e_read(g + 1).wait()
            with jax.named_scope("g"):
                form_g(g + 1)

            @pl.when(g + 3 <= chips)
            def _():
                e_read(g + 3).start()

        @pl.when(s >= 1)
        def _():
            rs_release(s, j)
        return carry

    with jax.named_scope("dx_first"):
        buf[0, 0] = dx_dot(1, 0)
    rs_send_on(0, 0)
    with jax.named_scope("bc_far"):
        lax.fori_loop(1, chips, bc_wait_rest, 0)
    lax.fori_loop(1, dw_from, scatter_g, 0)
    pl.semaphore_signal(dw_credit, inc=1, device_id={"tp": partner}, device_id_type=MESH)
    total = bc_in[0]
    for c in range(1, chips):
        total = total + bc_in[c]
    ls_out[...] = total
    ls_copy.start()

    def scatter_dw(i, carry):
        s = i // BLOCKS
        j = lax.rem(i, BLOCKS)
        b0 = lax.rem(s, BUFS)
        q = i - dw_from
        mb = q // PIECES
        o = lax.rem(q, PIECES)
        rs_arrive(s, j)

        @pl.when(o == 0)
        def _():
            xt_read(mb).wait()

            @pl.when(mb < MBLOCKS - 1)
            def _():
                xt_read(mb + 1).start()

        @pl.when((o < HALF) & (mb >= 1))
        def _():
            dw_copy(mb - 1, o).wait_send()

        with jax.named_scope("dx_dw"):
            buf[b0, j] = buf[b0, j] + dx_dot(s + 1, j)
            stage[0, o, :, 0:pc] = jnp.dot(xtb[lax.rem(mb, 2)], xg[lax.rem(o + HALF, PIECES)], preferred_element_type=F32)
        rs_send_on(s, j)

        @pl.when((o == 0) & (mb != 1))
        def _():
            pl.semaphore_wait(dw_credit, 1)

        @pl.when(o < HALF)
        def _():
            dw_copy(mb, o).start()

        @pl.when(o >= HALF)
        def _():
            h = o - HALF
            dw_copy(mb, h).wait_recv()

            @pl.when(mb >= 1)
            def _():
                dw_out(mb - 1, h).wait()
            dwb[h] = (stage[0, o, :, 0:pc] + stage[1, lax.rem(mb, 2) * HALF + h, :, 0:pc]).astype(BF16)
            dw_out(mb, h).start()

            @pl.when((h == HALF - 1) & (mb < MBLOCKS - 2))
            def _():
                pl.semaphore_signal(dw_credit, inc=1, device_id={"tp": partner}, device_id_type=MESH)

        rs_release(s, j)
        return carry

    lax.fori_loop(dw_from, own_from, scatter_dw, 0)

    def scatter_last(j, carry):
        with jax.named_scope("own"):
            stage[0, PIECES - 1, :, 0:pc] = dx_dot(0, j)
        rs_arrive(last, j)
        with jax.named_scope("out"):
            xtb[0, 0:slot_rows, pl.ds(pl.multiple_of(j * hb, hb), hb)] = (
                buf[last % BUFS, j] + stage[0, PIECES - 1, :, 0:pc]).astype(BF16)
        for c in dx_out(j):
            c.start()
        rs_release(last, j)
        return carry

    lax.fori_loop(0, BLOCKS, scatter_last, 0)

    ls_copy.wait()
    both = (ls_out[...] + ls_in[...]) * (1.0 / tokens)
    loss[0] = both[0, lanes - 1]
    loss[1] = both[1, lanes - 1]
    for o in range(HALF):
        dw_copy(MBLOCKS - 1, o).wait_send()
        dw_out(MBLOCKS - 1, o).wait()
    for j in range(BLOCKS):
        for c in dx_out(j):
            c.wait()


def solution(mesh):
    group = mesh.shape["tp"]
    chips = group // 2

    def local_step(x_a, x_b, labels_a, labels_b, w_local):
        rows, hidden = x_a.shape
        shard = w_local.shape[1]
        slot_rows = 2 * rows
        all_rows = chips * slot_rows
        hb = hidden // BLOCKS
        pc = shard // HALF
        mb_rows = hidden // MBLOCKS
        any_spec = pl.BlockSpec(memory_space=pl.ANY)
        vmem_spec = pl.BlockSpec(memory_space=pltpu.VMEM)
        out = pl.pallas_call(
            functools.partial(head_kernel, group),
            name="head",
            out_shape=(
                jax.ShapeDtypeStruct((2,), F32),
                jax.ShapeDtypeStruct((hidden, shard), BF16),
                jax.ShapeDtypeStruct((rows, hidden), BF16),
                jax.ShapeDtypeStruct((rows, hidden), BF16),
                jax.ShapeDtypeStruct((chips, PIECES, slot_rows, pc + 128), F32),
                jax.ShapeDtypeStruct((hidden, all_rows), BF16),
            ),
            in_specs=[any_spec, any_spec, vmem_spec, vmem_spec, any_spec],
            out_specs=(pl.BlockSpec(memory_space=pltpu.SMEM), any_spec, any_spec, any_spec, any_spec, any_spec),
            scratch_shapes=[
                pltpu.VMEM((PIECES, hidden, pc), BF16),
                pltpu.VMEM((PIECES, all_rows, pc), BF16),
                pltpu.VMEM((2, PIECES, slot_rows, pc + 128), F32),
                pltpu.VMEM((2, mb_rows, all_rows), BF16),
                pltpu.VMEM((BUFS, BLOCKS, slot_rows, hb), F32),
                pltpu.VMEM((HALF, mb_rows, pc), BF16),
                pltpu.VMEM((slot_rows, 128), F32),
                pltpu.VMEM((slot_rows, 128), F32),
                pltpu.VMEM((slot_rows, 128), F32),
                pltpu.VMEM((2, slot_rows, 128), jnp.int32),
                pltpu.VMEM((chips, 8, rows), F32),
                pltpu.VMEM((chips, RINGS, 8, 128), F32),
                pltpu.VMEM((chips, RINGS, 8, 128), F32),
                pltpu.VMEM((chips, 8, 128), F32),
                pltpu.VMEM((8, 128), F32),
                pltpu.VMEM((8, 128), F32),
                pltpu.VMEM((8, 128), F32),
            ],
            compiler_params=pltpu.CompilerParams(
                collective_id=0, has_side_effects=True, vmem_limit_bytes=67043328),
        )(x_a, x_b, labels_a.reshape(1, rows), labels_b.reshape(1, rows), w_local)
        return out[0], out[1], out[2], out[3]

    row_spec = P(("dp", "tp"), None)
    label_spec = P(("dp", "tp"))
    return jax.shard_map(local_step, mesh=mesh, in_specs=(row_spec, row_spec, label_spec, label_spec, P(None, "tp")), out_specs=(P("dp"), P("dp", "tp"), row_spec, row_spec), check_vma=False)
```

```python
import functools
import math

import jax
import jax.numpy as jnp
from jax import lax
from jax.experimental import pallas as pl
from jax.experimental.pallas import tpu as pltpu
from jax.sharding import PartitionSpec as P

MESH = pl.DeviceIdType.MESH
F32 = jnp.float32
BF16 = jnp.bfloat16
RINGS = 4
BLOCKS = 4
HALF = 3
PIECES = 2 * HALF
MBLOCKS = 8
BUFS = 3


class Both:
    def __init__(self, *copies):
        self.copies = copies

    def start(self):
        for c in self.copies:
            c.start()

    def wait(self):
        for c in self.copies:
            c.wait()


def head_kernel(group, *refs):
    chips = group // 2
    dma = pltpu.SemaphoreType.DMA
    regular = pltpu.SemaphoreType.REGULAR
    pl.run_scoped(
        functools.partial(head_body, group, *refs),
        x_sem=dma((2 * BLOCKS,)), w_sem=dma((HALF,)), wp_sem=dma((2, HALF)), lab_sem=dma((2, chips)), sync=regular((3,)),
        ag_send=dma((4, BLOCKS * RINGS)), ag_recv=dma((chips, BLOCKS * RINGS)),
        e_sem=dma((2, HALF)), er_sem=dma((2, 2)), xt_sem=dma((MBLOCKS,)), xtr_sem=dma((2,)),
        run_send=dma((chips, RINGS)), run_recv=dma((chips, RINGS)), bc_send=dma((chips,)), bc_recv=dma((chips,)),
        ls_sem=dma((2,)), rs_send=dma((BUFS, BLOCKS, RINGS)), rs_recv=dma((BUFS, BLOCKS, RINGS)),
        credit=regular((BLOCKS, RINGS)), dw_send=dma((HALF,)), dw_recv=dma((2, HALF)), dw_credit=regular,
        dwo_sem=dma((HALF,)), dxo_sem=dma((BLOCKS, 2)))


def head_body(group, xa, xb, la, lb, w, loss, dw, dxa, dxb, e_hbm, m_hbm, xt_hbm,
              wv, xg, stage, shift, xtb, buf, dwb, m_run, s_run, t_run, labc,
              lab_in, run_out, run_in, bc_in, bc_out, ls_out, ls_in,
              x_sem, w_sem, wp_sem, lab_sem, sync, ag_send, ag_recv, e_sem, er_sem, xt_sem, xtr_sem, run_send, run_recv,
              bc_send, bc_recv, ls_sem, rs_send, rs_recv, credit, dw_send, dw_recv, dw_credit, dwo_sem, dxo_sem):
    chips = group // 2
    side = math.isqrt(chips)
    rows = xa.shape[0]
    slot_rows = 2 * rows
    rt = slot_rows // RINGS
    hb = xg.shape[2]
    pc = hb
    shard = w.shape[1]
    tokens = rows * group
    mb_rows = w.shape[0] // MBLOCKS
    lanes = lab_in.shape[2]

    me = lax.axis_index("tp")
    core = lax.rem(me, 2)
    chip = me // 2
    partner = me + 1 - 2 * core
    cx = lax.rem(chip, side)
    cy = chip // side
    diag = lax.rem(cx + cy, side)
    pos = (side * cy + diag, side * lax.rem(cx + 1, side) + diag)

    def dev(c):
        return {"tp": 2 * c + core}

    def chip_at(cycle, p):
        major, minor = p // side, lax.rem(p, side)
        if cycle == 0:
            yy = major
            xx = lax.rem(minor - major + side, side)
        else:
            xx = lax.rem(major + side - 1, side)
            yy = lax.rem(minor + 1 - major + side, side)
        return yy * side + xx

    def source(r, k):
        sign = -1 if r % 2 == 0 else 1
        return chip_at(r // 2, lax.rem(pos[r // 2] + sign * k + 2 * chips, chips))

    up = [source(r, 1) for r in range(RINGS)]
    down = [source(r, -1) for r in range(RINGS)]

    for b in range(BLOCKS):
        cols = pl.ds(b * hb, hb)
        pltpu.make_async_copy(xa.at[:, cols], xg.at[b, pl.ds(0, rows)], x_sem.at[2 * b]).start()
        pltpu.make_async_copy(xb.at[:, cols], xg.at[b, pl.ds(rows, rows)], x_sem.at[2 * b + 1]).start()

    def w_load(h):
        return pltpu.make_async_copy(w.at[:, pl.ds(h * pc, pc)], wv.at[h], w_sem.at[h])

    def w_swap(h):
        return pltpu.make_async_remote_copy(
            src_ref=w.at[:, pl.ds(h * pc, pc)], dst_ref=wv.at[HALF + h], send_sem=wp_sem.at[0, h],
            recv_sem=wp_sem.at[1, h], device_id={"tp": partner}, device_id_type=MESH)

    for h in range(HALF):
        w_load(h).start()

    barrier = pltpu.get_barrier_semaphore()

    def is_near(c):
        near = c == up[0]
        for r in range(1, RINGS):
            near = near | (c == up[r])
        return near

    for r in range(RINGS):
        pl.semaphore_signal(barrier, inc=1, device_id=dev(up[r]), device_id_type=MESH)
    pl.semaphore_signal(barrier, inc=1, device_id={"tp": partner}, device_id_type=MESH)
    my_lab = lab_in.at[chip]
    my_lab[0:1, :] = la[...].astype(F32)
    my_lab[1:2, :] = lb[...].astype(F32)
    buf[0] = jnp.zeros(buf.shape[1:], F32)
    with jax.named_scope("barrier"):
        pl.semaphore_wait(barrier, RINGS + 1)

    def ag_copy(k, j, r):
        src = xg.at[j, pl.ds(pl.multiple_of(k * slot_rows + r * rt, rt), rt)]
        dst = xg.at[j, pl.ds(pl.multiple_of((k + 1) * slot_rows + r * rt, rt), rt)]
        return pltpu.make_async_remote_copy(
            src_ref=src, dst_ref=dst, send_sem=ag_send.at[lax.rem(k, 4), j * RINGS + r],
            recv_sem=ag_recv.at[k + 1, j * RINGS + r], device_id=dev(down[r]), device_id_type=MESH)

    for b in range(BLOCKS):
        cols = pl.ds(b * hb, hb)
        pltpu.make_async_copy(xa.at[:, cols], xg.at[b, pl.ds(0, rows)], x_sem.at[2 * b]).wait()
        pltpu.make_async_copy(xb.at[:, cols], xg.at[b, pl.ds(rows, rows)], x_sem.at[2 * b + 1]).wait()
        for r in range(RINGS):
            ag_copy(0, b, r).start()

    for h in range(HALF):
        w_swap(h).start()

    def lab_copy(d):
        return pltpu.make_async_remote_copy(
            src_ref=lab_in.at[chip], dst_ref=lab_in.at[chip], send_sem=lab_sem.at[0, d], recv_sem=lab_sem.at[1, d],
            device_id=dev(lax.rem(chip + d, chips)), device_id_type=MESH)

    def lab_start(near):
        def go(d, carry):
            is_to = is_near(lax.rem(chip + d, chips))

            @pl.when(is_to if near else jnp.logical_not(is_to))
            def _():
                lab_copy(d).start()
            return carry
        lax.fori_loop(1, chips, go, 0)

    def lab_wait(near):
        def go(d, carry):
            is_from = is_near(lax.rem(chip + chips - d, chips))

            @pl.when(is_from if near else jnp.logical_not(is_from))
            def _():
                lab_copy(d).wait_recv()
            return carry
        lax.fori_loop(1, chips, go, 0)

    def sync_signal(n):
        for r in range(RINGS):
            pl.semaphore_signal(sync.at[n], inc=1, device_id=dev(up[r]), device_id_type=MESH)

    def sync_wait(n):
        pl.semaphore_wait(sync.at[n], RINGS)

    lab_start(True)
    sync_signal(0)
    for h in range(HALF):
        w_load(h).wait()

    sub_i = lax.broadcasted_iota(jnp.int32, (rt, 128), 0)
    lane_i = lax.broadcasted_iota(jnp.int32, (rt, 128), 1)
    eye = sub_i == lane_i
    row_lane = lax.broadcasted_iota(jnp.int32, (1, 128), 1)
    lab_sub = lax.broadcasted_iota(jnp.int32, (rt, lanes), 0)
    lab_lane = lax.broadcasted_iota(jnp.int32, (rt, lanes), 1)

    def to_row(col):
        return jnp.sum(jnp.where(eye, col, 0.0), axis=0, keepdims=True)

    def to_col(row):
        return jnp.sum(jnp.where(eye, row, 0.0), axis=1, keepdims=True)

    def fill_labels(lab, sources):
        for r in range(RINGS):
            row = lab_in[sources[r], r // 2:r // 2 + 1, :]
            col = jnp.sum(jnp.where(lab_lane == lab_sub + (r % 2) * rt, row, 0.0), axis=1, keepdims=True)
            lab[r * rt:(r + 1) * rt, :] = jnp.broadcast_to(col.astype(jnp.int32), (rt, 128))

    def sources_of(k):
        return [source(r, k) for r in range(RINGS)]

    def base(lp):
        owner = me if lp < HALF else partner
        return owner * shard + (lp % HALF) * pc

    chunk = slot_rows // 8
    per = pc // 128
    lane_at = [lax.broadcasted_iota(jnp.int32, (chunk, 128), 1) + i * 128 for i in range(per)]
    vregs = [(i // per, i % per, slice(i % per * 128, (i % per + 1) * 128)) for i in range(2 * per)]

    def hits(lab_rows, pair):
        rel = [lab_rows - base(2 * pair), lab_rows - base(2 * pair + 1)]
        return [lane_at[n] == rel[h] for h, n, _ in vregs]

    def z_dot(k0, lp):
        z = None
        for b in range(BLOCKS):
            part = jnp.dot(xg[b, pl.ds(k0, slot_rows), :], wv[lp, b * hb:(b + 1) * hb, :], preferred_element_type=F32)
            z = part if z is None else z + part
        stage[0, lp // 2, lp % 2] = z

    def z_stats(pair, lab):
        for c in range(8):
            rs = slice(c * chunk, (c + 1) * chunk)
            z = [stage[0, pair, h, rs, cs] for h, _, cs in vregs]
            m = functools.reduce(jnp.maximum, z)
            e = [jnp.exp(v - m) for v in z]
            t = functools.reduce(jnp.add, [jnp.where(h, v, 0.0) for h, v in zip(hits(lab[rs, :], pair), z)])
            s = functools.reduce(jnp.add, e)
            for (h, _, cs), v in zip(vregs, e):
                stage[0, pair, h, rs, cs] = v
            shift[0, pair, rs, :] = m
            if pair == 0:
                m_run[rs, :] = m
                s_run[rs, :] = s
                t_run[rs, :] = t
            else:
                old = m_run[rs, :]
                new = jnp.maximum(old, m)
                m_run[rs, :] = new
                s_run[rs, :] = s_run[rs, :] * jnp.exp(old - new) + s * jnp.exp(m - new)
                t_run[rs, :] = t_run[rs, :] + t

    def e_write(slot, pair):
        return Both(pltpu.make_async_copy(stage.at[0, pair], e_hbm.at[slot, pair], e_sem.at[0, pair]),
                    pltpu.make_async_copy(shift.at[0, pair], m_hbm.at[slot, pair], e_sem.at[1, pair]))

    def xt_write(slot, mb):
        return pltpu.make_async_copy(
            xtb.at[1, :, pl.ds(mb * mb_rows, slot_rows)],
            xt_hbm.at[pl.ds(mb * mb_rows, mb_rows), pl.ds(pl.multiple_of(slot * slot_rows, slot_rows), slot_rows)],
            xt_sem.at[mb])

    def run_copy(slot, r):
        return pltpu.make_async_remote_copy(
            src_ref=run_out.at[slot, r], dst_ref=run_in.at[slot + 1, r], send_sem=run_send.at[slot, r],
            recv_sem=run_recv.at[slot + 1, r], device_id=dev(down[r]), device_id_type=MESH)

    def join_stats(slot):
        with jax.named_scope("stats"):
            lane_m = m_run[...]
            m = jnp.max(lane_m, axis=1, keepdims=True)
            s = jnp.sum(s_run[...] * jnp.exp(lane_m - m), axis=1, keepdims=True)
            t = jnp.sum(t_run[...], axis=1, keepdims=True)
            rows_mst = [[to_row(v[r * rt:(r + 1) * rt]) for v in (m, s, t)] for r in range(RINGS)]

        @pl.when(slot >= 1)
        def _():
            for r in range(RINGS):
                run_copy(slot - 1, r).wait_recv()
        for r in range(RINGS):
            m_r, s_r, t_r = rows_mst[r]
            m_in = run_in[slot, r, 0:1, :]
            m_new = jnp.maximum(m_in, m_r)
            run_out[slot, r, 0:1, :] = m_new
            run_out[slot, r, 1:2, :] = s_r * jnp.exp(m_r - m_new) + run_in[slot, r, 1:2, :] * jnp.exp(m_in - m_new)
            run_out[slot, r, 2:3, :] = t_r + run_in[slot, r, 2:3, :]

    def poll(k, j):
      with jax.named_scope("poll"):
        @pl.when(k < chips)
        def _():
            for r in range(RINGS):
                ag_copy(k - 1, j, r).wait_recv()

        @pl.when(k < chips - 1)
        def _():
            @pl.when(k >= 4)
            def _():
                for r in range(RINGS):
                    ag_copy(k - 4, j, r).wait_send()
            for r in range(RINGS):
                ag_copy(k, j, r).start()

    fill_labels(labc.at[0], [chip] * RINGS)
    for r in range(RINGS):
        run_in[0, r, 0:1, :] = jnp.full((1, 128), -jnp.inf, F32)
        run_in[0, r, 1:3, :] = jnp.zeros((2, 128), F32)

    def gather_step(k, carry):
        slot = k - 1
        k0 = pl.multiple_of(slot * slot_rows, slot_rows)
        here = labc.at[lax.rem(slot, 2)]
        other = labc.at[lax.rem(slot + 1, 2)]
        ahead = sources_of(lax.rem(slot + 1, chips))

        @pl.when(slot >= 1)
        def _():
            e_write(slot - 1, 0).wait()

        with jax.named_scope("u0"):
            z_dot(k0, 0)
            z_dot(k0, 1)
            z_stats(2, other)

        @pl.when(slot == 0)
        def _():
            poll(k, 0)

        @pl.when(k == 2)
        def _():
            poll(k, 3)

        @pl.when(k == 3)
        def _():
            poll(k, 2)

        @pl.when((k < 2) | (k > 3))
        def _():
            poll(k, 1)

        @pl.when(slot >= 1)
        def _():
            e_write(slot - 1, 2).start()
            join_stats(slot - 1)
            for r in range(RINGS):
                run_copy(slot - 1, r).start()
            e_write(slot - 1, 1).wait()

        @pl.when(slot == 0)
        def _():
            sync_wait(0)
            sync_signal(1)
            w_swap(0).wait()

        with jax.named_scope("u1"):
            z_dot(k0, 2)
            z_dot(k0, 3)
            z_stats(0, here)
        e_write(slot, 0).start()

        @pl.when(k == 2)
        def _():
            poll(k + 1, 0)

        @pl.when(k == 3)
        def _():
            poll(k, 3)

        @pl.when((k < 2) | (k > 3))
        def _():
            poll(k, 2)

        @pl.when(slot == 0)
        def _():
            sync_wait(1)
            sync_signal(2)
            lab_wait(True)
            poll(k, 3)
            poll(k + 1, 0)
            poll(k + 1, 1)
            w_swap(1).wait()
            w_swap(2).wait()

        @pl.when(slot >= 1)
        def _():
            e_write(slot - 1, 2).wait()
            for mb in range(MBLOCKS):
                xt_write(slot - 1, mb).wait()

        @pl.when(slot == 1)
        def _():
            lab_wait(False)

        with jax.named_scope("u2"):
            z_dot(k0, 4)
            z_dot(k0, 5)
            z_stats(1, here)
            fill_labels(other, ahead)
            for mb in range(MBLOCKS):
                at = mb * mb_rows % hb
                xtb[1, :, mb * mb_rows:(mb + 1) * mb_rows] = xg[mb * mb_rows // hb, pl.ds(k0, slot_rows), at:at + mb_rows].T
        e_write(slot, 1).start()
        for mb in range(MBLOCKS):
            xt_write(slot, mb).start()

        for early in range(1, 4):
            @pl.when(k == early)
            def _():
                poll(k + 1, 3 - early)

        @pl.when(k >= 4)
        def _():
            poll(k, 3)
            poll(k + 1, 0)

        @pl.when(slot == 0)
        def _():
            sync_wait(2)
            lab_start(False)
        return carry

    lax.fori_loop(1, chips + 1, gather_step, 0)
    with jax.named_scope("flush"):
        z_stats(2, labc.at[(chips - 1) % 2])
    e_write(chips - 1, 2).start()
    join_stats(chips - 1)

    inside = row_lane < rt
    parts = []
    for r in range(RINGS):
        m, s, t = (run_out[chips - 1, r, i:i + 1, :] for i in range(3))
        bc_out[r:r + 1, :] = m
        bc_out[RINGS + r:RINGS + r + 1, :] = s
        parts.append(jnp.sum(jnp.where(inside, m + jnp.log(s) - t, 0.0), axis=1, keepdims=True))
    for mb in range(2):
        both = jnp.broadcast_to(parts[2 * mb] + parts[2 * mb + 1], (1, 128))
        bc_out[mb:mb + 1, :] = jnp.where(inside, bc_out[mb:mb + 1, :], both)
    bc_in[chip] = bc_out[...]

    def bc_copy(d):
        return pltpu.make_async_remote_copy(
            src_ref=bc_out, dst_ref=bc_in.at[chip], send_sem=bc_send.at[d], recv_sem=bc_recv.at[d],
            device_id=dev(lax.rem(chip + d, chips)), device_id_type=MESH)

    def bc_start(d, carry):
        bc_copy(d).start()
        return carry

    first_four = [source(r, 2) for r in range(RINGS)]

    def is_first(c):
        near = c == first_four[0]
        for r in range(1, RINGS):
            near = near | (c == first_four[r])
        return near

    def bc_wait_first(d, carry):
        @pl.when(is_first(lax.rem(chip + chips - d, chips)))
        def _():
            bc_copy(d).wait_recv()
        return carry

    def bc_wait_rest(d, carry):
        @pl.when(jnp.logical_not(is_first(lax.rem(chip + chips - d, chips))))
        def _():
            bc_copy(d).wait_recv()
        bc_copy(d).wait_send()
        lab_copy(d).wait_send()
        for r in range(RINGS):
            run_copy(d - 1, r).wait_send()
        return carry

    ls_copy = pltpu.make_async_remote_copy(
        src_ref=ls_out, dst_ref=ls_in, send_sem=ls_sem.at[0], recv_sem=ls_sem.at[1],
        device_id={"tp": partner}, device_id_type=MESH)

    lax.fori_loop(1, chips, bc_start, 0)

    def e_read(g):
        slot, half = lax.rem(g, chips), lax.rem(g, 2)
        return Both(pltpu.make_async_copy(e_hbm.at[slot], stage.at[half], er_sem.at[0, half]),
                    pltpu.make_async_copy(m_hbm.at[slot], shift.at[half], er_sem.at[1, half]))

    e_read(1).start()
    for pair in range(HALF):
        e_write(chips - 1, pair).wait()
    e_read(2).start()
    for mb in range(MBLOCKS):
        xt_write(chips - 1, mb).wait()

    def xt_read(mb):
        return pltpu.make_async_copy(
            xt_hbm.at[pl.ds(pl.multiple_of(mb * mb_rows, mb_rows), mb_rows), :], xtb.at[lax.rem(mb, 2)],
            xtr_sem.at[lax.rem(mb, 2)])

    xt_read(0).start()
    for k in range(chips - 5, chips - 1):
        for j in range(BLOCKS):
            for r in range(RINGS):
                ag_copy(k, j, r).wait_send()

    with jax.named_scope("bc_first"):
        lax.fori_loop(1, chips, bc_wait_first, 0)

    def form_g(g):
        slot = lax.rem(g, chips)
        half = lax.rem(g, 2)
        k0 = pl.multiple_of(slot * slot_rows, slot_rows)
        sources = sources_of(slot)
        holders = sources_of(lax.rem(slot + 1, chips))
        lab = labc.at[0]
        fill_labels(lab, sources)
        for r in range(RINGS):
            rs = slice(r * rt, (r + 1) * rt)
            m_run[rs, :] = jnp.broadcast_to(to_col(bc_in[holders[r], r:r + 1, :]), (rt, 128))
            s_run[rs, :] = jnp.broadcast_to(
                1.0 / (to_col(bc_in[holders[r], RINGS + r:RINGS + r + 1, :]) * tokens), (rt, 128))
        for pair in range(HALF):
            for c in range(8):
                rs = slice(c * chunk, (c + 1) * chunk)
                krs = pl.ds(pl.multiple_of(k0 + c * chunk, chunk), chunk)
                scale = jnp.exp(shift[half, pair, rs, :] - m_run[rs, :]) * s_run[rs, :]
                for (h, _, cs), hit in zip(vregs, hits(lab[rs, :], pair)):
                    v = stage[half, pair, h, rs, cs] * scale - jnp.where(hit, 1.0 / tokens, 0.0)
                    xg[2 * pair + h, krs, cs] = v.astype(BF16)

    e_read(1).wait()
    with jax.named_scope("g_first"):
        form_g(1)
    e_read(3).start()

    def rs_copy(s, j, r):
        b0, b1 = lax.rem(s, BUFS), lax.rem(s + 1, BUFS)
        return pltpu.make_async_remote_copy(
            src_ref=buf.at[b0, j, pl.ds(r * rt, rt)], dst_ref=buf.at[b1, j, pl.ds(r * rt, rt)],
            send_sem=rs_send.at[b0, j, r], recv_sem=rs_recv.at[b1, j, r],
            device_id=dev(down[r]), device_id_type=MESH)

    def tile_at(h, o):
        return (h, o // 2, lax.rem(o, 2))

    def dw_copy(mb, o):
        return pltpu.make_async_remote_copy(
            src_ref=stage.at[tile_at(0, o)], dst_ref=stage.at[tile_at(1, lax.rem(mb, 2) * HALF + o)],
            send_sem=dw_send.at[o],
            recv_sem=dw_recv.at[lax.rem(mb, 2), o], device_id={"tp": partner}, device_id_type=MESH)

    def dw_out(mb, o):
        return pltpu.make_async_copy(
            dwb.at[o], dw.at[pl.ds(pl.multiple_of(mb * mb_rows, mb_rows), mb_rows),
                             pl.ds(pl.multiple_of(o * pc, pc), pc)], dwo_sem.at[o])

    def dx_out(j):
        cols = pl.ds(pl.multiple_of(j * hb, hb), hb)
        return (pltpu.make_async_copy(xtb.at[0, pl.ds(0, rows), cols], dxa.at[:, cols], dxo_sem.at[j, 0]),
                pltpu.make_async_copy(xtb.at[0, pl.ds(rows, rows), cols], dxb.at[:, cols], dxo_sem.at[j, 1]))

    last = chips - 1
    dw_from = 3 * BLOCKS
    own_from = last * BLOCKS
    assert own_from - dw_from == MBLOCKS * PIECES and dw_from - 1 + BLOCKS == chips - 1

    def dx_dot(slot, j):
        k0 = pl.multiple_of(slot * slot_rows, slot_rows)
        tile = None
        for lp in range(PIECES):
            part = lax.dot_general(
                xg[lp, pl.ds(k0, slot_rows), :],
                wv[lp, pl.ds(pl.multiple_of(j * hb, hb), hb), :],
                (((1,), (1,)), ((), ())), preferred_element_type=F32)
            tile = part if tile is None else tile + part
        return tile

    def rs_arrive(s, j):
        with jax.named_scope("rs_wait"):
            for r in range(RINGS):
                rs_copy(s - 1, j, r).wait_recv()

    def rs_send_on(s, j):
        @pl.when(s >= 2)
        def _():
            for r in range(RINGS):
                pl.semaphore_wait(credit.at[j, r], 1)
        for r in range(RINGS):
            rs_copy(s, j, r).start()

    def rs_release(s, j):
        for r in range(RINGS):
            rs_copy(s - 1, j, r).wait_send()

        @pl.when(s - 1 <= last - 3)
        def _():
            for r in range(RINGS):
                pl.semaphore_signal(credit.at[j, r], inc=1, device_id=dev(up[r]), device_id_type=MESH)

    def scatter_g(i, carry):
        s = i // BLOCKS
        j = lax.rem(i, BLOCKS)
        b0 = lax.rem(s, BUFS)
        double = s == 1
        g = jnp.where(s == 0, i + 1, jnp.where(double, 2 * i - BLOCKS + 1, i + BLOCKS + 1))

        @pl.when(s >= 1)
        def _():
            rs_arrive(s, j)

        e_read(g).wait()
        with jax.named_scope("dx_g"):
            buf[b0, j] = buf[b0, j] + dx_dot(s + 1, j)
            form_g(g)
        rs_send_on(s, j)

        @pl.when(g + 2 <= chips)
        def _():
            e_read(g + 2).start()

        @pl.when(double)
        def _():
            e_read(g + 1).wait()
            with jax.named_scope("g"):
                form_g(g + 1)

            @pl.when(g + 3 <= chips)
            def _():
                e_read(g + 3).start()

        @pl.when(s >= 1)
        def _():
            rs_release(s, j)
        return carry

    with jax.named_scope("dx_first"):
        buf[0, 0] = dx_dot(1, 0)
    rs_send_on(0, 0)
    with jax.named_scope("bc_far"):
        lax.fori_loop(1, chips, bc_wait_rest, 0)
    lax.fori_loop(1, dw_from, scatter_g, 0)
    pl.semaphore_signal(dw_credit, inc=1, device_id={"tp": partner}, device_id_type=MESH)
    total = bc_in[0]
    for c in range(1, chips):
        total = total + bc_in[c]
    ls_out[...] = total
    ls_copy.start()

    def scatter_dw(i, carry):
        s = i // BLOCKS
        j = lax.rem(i, BLOCKS)
        b0 = lax.rem(s, BUFS)
        q = i - dw_from
        mb = q // PIECES
        o = lax.rem(q, PIECES)
        rs_arrive(s, j)

        @pl.when(o == 0)
        def _():
            xt_read(mb).wait()

            @pl.when(mb < MBLOCKS - 1)
            def _():
                xt_read(mb + 1).start()

        @pl.when((o < HALF) & (mb >= 1))
        def _():
            dw_copy(mb - 1, o).wait_send()

        with jax.named_scope("dx_dw"):
            buf[b0, j] = buf[b0, j] + dx_dot(s + 1, j)
            stage[tile_at(0, o)] = jnp.dot(xtb[lax.rem(mb, 2)], xg[lax.rem(o + HALF, PIECES)], preferred_element_type=F32)
        rs_send_on(s, j)

        @pl.when((o == 0) & (mb != 1))
        def _():
            pl.semaphore_wait(dw_credit, 1)

        @pl.when(o < HALF)
        def _():
            dw_copy(mb, o).start()

        @pl.when(o >= HALF)
        def _():
            h = o - HALF
            dw_copy(mb, h).wait_recv()

            @pl.when(mb >= 1)
            def _():
                dw_out(mb - 1, h).wait()
            dwb[h] = (stage[tile_at(0, o)] + stage[tile_at(1, lax.rem(mb, 2) * HALF + h)]).astype(BF16)
            dw_out(mb, h).start()

            @pl.when((h == HALF - 1) & (mb < MBLOCKS - 2))
            def _():
                pl.semaphore_signal(dw_credit, inc=1, device_id={"tp": partner}, device_id_type=MESH)

        rs_release(s, j)
        return carry

    lax.fori_loop(dw_from, own_from, scatter_dw, 0)

    def scatter_last(j, carry):
        with jax.named_scope("own"):
            stage[0, HALF - 1, 1] = dx_dot(0, j)
        rs_arrive(last, j)
        with jax.named_scope("out"):
            xtb[0, 0:slot_rows, pl.ds(pl.multiple_of(j * hb, hb), hb)] = (
                buf[last % BUFS, j] + stage[0, HALF - 1, 1]).astype(BF16)
        for c in dx_out(j):
            c.start()
        rs_release(last, j)
        return carry

    lax.fori_loop(0, BLOCKS, scatter_last, 0)

    ls_copy.wait()
    both = (ls_out[...] + ls_in[...]) * (1.0 / tokens)
    loss[0] = both[0, lanes - 1]
    loss[1] = both[1, lanes - 1]
    for o in range(HALF):
        dw_copy(MBLOCKS - 1, o).wait_send()
        dw_out(MBLOCKS - 1, o).wait()
    for j in range(BLOCKS):
        for c in dx_out(j):
            c.wait()


def copy_kernel(loss, dw, dxa, dxb, loss_out, dw_out, dxa_out, dxb_out, dw_v, dxa_v, dxb_v, in_sem, out_sem):
    moves = []
    for n, (src, via, dst) in enumerate(((dw, dw_v, dw_out), (dxa, dxa_v, dxa_out), (dxb, dxb_v, dxb_out))):
        parts = MBLOCKS if n == 0 else 1
        size = src.shape[0] // parts
        for p in range(parts):
            at = pl.ds(p * size, size)
            moves.append((pltpu.make_async_copy(src.at[at], via.at[at], in_sem.at[n, p]),
                          pltpu.make_async_copy(via.at[at], dst.at[at], out_sem.at[n, p])))
    for load, _ in moves:
        load.start()
    loss_out[0] = loss[0]
    loss_out[1] = loss[1]
    for load, store in moves:
        load.wait()
        store.start()
    for _, store in moves:
        store.wait()


def solution(mesh):
    group = mesh.shape["tp"]
    chips = group // 2

    def local_step(x_a, x_b, labels_a, labels_b, w_local):
        rows, hidden = x_a.shape
        shard = w_local.shape[1]
        slot_rows = 2 * rows
        all_rows = chips * slot_rows
        hb = hidden // BLOCKS
        pc = shard // HALF
        mb_rows = hidden // MBLOCKS
        any_spec = pl.BlockSpec(memory_space=pl.ANY)
        vmem_spec = pl.BlockSpec(memory_space=pltpu.VMEM)
        out = pl.pallas_call(
            functools.partial(head_kernel, group),
            name="head",
            out_shape=(
                jax.ShapeDtypeStruct((2,), F32),
                jax.ShapeDtypeStruct((hidden, shard), BF16),
                jax.ShapeDtypeStruct((rows, hidden), BF16),
                jax.ShapeDtypeStruct((rows, hidden), BF16),
                jax.ShapeDtypeStruct((chips, HALF, 2, slot_rows, pc), F32),
                jax.ShapeDtypeStruct((chips, HALF, slot_rows, 128), F32),
                jax.ShapeDtypeStruct((hidden, all_rows), BF16),
            ),
            in_specs=[any_spec, any_spec, vmem_spec, vmem_spec, any_spec],
            out_specs=(pl.BlockSpec(memory_space=pltpu.SMEM),) + (any_spec,) * 6,
            scratch_shapes=[
                pltpu.VMEM((PIECES, hidden, pc), BF16),
                pltpu.VMEM((PIECES, all_rows, pc), BF16),
                pltpu.VMEM((2, HALF, 2, slot_rows, pc), F32),
                pltpu.VMEM((2, HALF, slot_rows, 128), F32),
                pltpu.VMEM((2, mb_rows, all_rows), BF16),
                pltpu.VMEM((BUFS, BLOCKS, slot_rows, hb), F32),
                pltpu.VMEM((HALF, mb_rows, pc), BF16),
                pltpu.VMEM((slot_rows, 128), F32),
                pltpu.VMEM((slot_rows, 128), F32),
                pltpu.VMEM((slot_rows, 128), F32),
                pltpu.VMEM((2, slot_rows, 128), jnp.int32),
                pltpu.VMEM((chips, 2, rows), F32),
                pltpu.VMEM((chips, RINGS, 4, 128), F32),
                pltpu.VMEM((chips, RINGS, 4, 128), F32),
                pltpu.VMEM((chips, 8, 128), F32),
                pltpu.VMEM((8, 128), F32),
                pltpu.VMEM((8, 128), F32),
                pltpu.VMEM((8, 128), F32),
            ],
            compiler_params=pltpu.CompilerParams(
                collective_id=0, has_side_effects=True, vmem_limit_bytes=67043328),
        )(x_a, x_b, labels_a.reshape(1, rows), labels_b.reshape(1, rows), w_local)
        results = out[:4]
        return pl.pallas_call(
            copy_kernel,
            name="results",
            out_shape=tuple(jax.ShapeDtypeStruct(v.shape, v.dtype) for v in results),
            in_specs=[pl.BlockSpec(memory_space=pltpu.SMEM), any_spec, any_spec, any_spec],
            out_specs=(pl.BlockSpec(memory_space=pltpu.SMEM), any_spec, any_spec, any_spec),
            scratch_shapes=[pltpu.VMEM(v.shape, v.dtype) for v in results[1:]] + [
                pltpu.SemaphoreType.DMA((3, MBLOCKS)), pltpu.SemaphoreType.DMA((3, MBLOCKS))],
        )(*results)

    row_spec = P(("dp", "tp"), None)
    label_spec = P(("dp", "tp"))
    return jax.shard_map(local_step, mesh=mesh, in_specs=(row_spec, row_spec, label_spec, label_spec, P(None, "tp")), out_specs=(P("dp"), P("dp", "tp"), row_spec, row_spec), check_vma=False)
```

```python
import functools
import math

import jax
import jax.numpy as jnp
from jax import lax
from jax.experimental import pallas as pl
from jax.experimental.pallas import tpu as pltpu
from jax.sharding import PartitionSpec as P

MESH = pl.DeviceIdType.MESH
F32 = jnp.float32
BF16 = jnp.bfloat16
RINGS = 4
BLOCKS = 4
HALF = 3
PIECES = 2 * HALF
MBLOCKS = 8
BUFS = 3
AHEAD = (1, 5, 10)


class Both:
    def __init__(self, *copies):
        self.copies = copies

    def start(self):
        for c in self.copies:
            c.start()

    def wait(self):
        for c in self.copies:
            c.wait()


def head_kernel(group, *refs):
    chips = group // 2
    dma = pltpu.SemaphoreType.DMA
    regular = pltpu.SemaphoreType.REGULAR
    pl.run_scoped(
        functools.partial(head_body, group, *refs),
        x_sem=dma((2 * BLOCKS,)), w_sem=dma((HALF,)), wp_sem=dma((2, HALF)), lab_sem=dma((2, chips)), sync=regular((3,)),
        ag_send=dma((4, BLOCKS * RINGS)), ag_recv=dma((chips, BLOCKS * RINGS)),
        e_sem=dma((2, HALF)), er_sem=dma((2, 2)), xt_sem=dma((MBLOCKS,)), xtr_sem=dma((2,)),
        run_send=dma((chips, RINGS)), run_recv=dma((chips, RINGS)), bc_send=dma((chips,)), bc_recv=dma((chips,)),
        ls_sem=dma((2,)), rs_send=dma((BUFS, BLOCKS, RINGS)), rs_recv=dma((BUFS, BLOCKS, RINGS)),
        credit=regular((BLOCKS, RINGS)), dw_send=dma((HALF,)), dw_recv=dma((2, HALF)), dw_credit=regular,
        dwo_sem=dma((HALF,)), dxo_sem=dma((BLOCKS, 2)))


def head_body(group, xa, xb, la, lb, w, loss, dw, dxa, dxb, e_hbm, m_hbm, xt_hbm,
              wv, xg, stage, shift, xtb, buf, dwb, m_run, s_run, t_run, labc,
              lab_in, run_out, run_in, bc_in, bc_out, ls_out, ls_in,
              x_sem, w_sem, wp_sem, lab_sem, sync, ag_send, ag_recv, e_sem, er_sem, xt_sem, xtr_sem, run_send, run_recv,
              bc_send, bc_recv, ls_sem, rs_send, rs_recv, credit, dw_send, dw_recv, dw_credit, dwo_sem, dxo_sem):
    chips = group // 2
    side = math.isqrt(chips)
    rows = xa.shape[0]
    slot_rows = 2 * rows
    rt = slot_rows // RINGS
    hb = xg.shape[2]
    pc = hb
    shard = w.shape[1]
    tokens = rows * group
    mb_rows = w.shape[0] // MBLOCKS
    lanes = lab_in.shape[2]

    me = lax.axis_index("tp")
    core = lax.rem(me, 2)
    chip = me // 2
    partner = me + 1 - 2 * core
    cx = lax.rem(chip, side)
    cy = chip // side
    diag = lax.rem(cx + cy, side)
    pos = (side * cy + diag, side * lax.rem(cx + 1, side) + diag)

    def dev(c):
        return {"tp": 2 * c + core}

    def chip_at(cycle, p):
        major, minor = p // side, lax.rem(p, side)
        if cycle == 0:
            yy = major
            xx = lax.rem(minor - major + side, side)
        else:
            xx = lax.rem(major + side - 1, side)
            yy = lax.rem(minor + 1 - major + side, side)
        return yy * side + xx

    def source(r, k):
        sign = -1 if r % 2 == 0 else 1
        return chip_at(r // 2, lax.rem(pos[r // 2] + sign * k + 2 * chips, chips))

    up = [source(r, 1) for r in range(RINGS)]
    down = [source(r, -1) for r in range(RINGS)]

    for b in range(BLOCKS):
        cols = pl.ds(b * hb, hb)
        pltpu.make_async_copy(xa.at[:, cols], xg.at[b, pl.ds(0, rows)], x_sem.at[2 * b]).start()
        pltpu.make_async_copy(xb.at[:, cols], xg.at[b, pl.ds(rows, rows)], x_sem.at[2 * b + 1]).start()

    def w_load(h):
        return pltpu.make_async_copy(w.at[:, pl.ds(h * pc, pc)], wv.at[h], w_sem.at[h])

    def w_swap(h):
        return pltpu.make_async_remote_copy(
            src_ref=w.at[:, pl.ds(h * pc, pc)], dst_ref=wv.at[HALF + h], send_sem=wp_sem.at[0, h],
            recv_sem=wp_sem.at[1, h], device_id={"tp": partner}, device_id_type=MESH)

    for h in range(HALF):
        w_load(h).start()

    barrier = pltpu.get_barrier_semaphore()

    def is_near(c):
        near = c == up[0]
        for r in range(1, RINGS):
            near = near | (c == up[r])
        return near

    for r in range(RINGS):
        pl.semaphore_signal(barrier, inc=1, device_id=dev(up[r]), device_id_type=MESH)
    pl.semaphore_signal(barrier, inc=1, device_id={"tp": partner}, device_id_type=MESH)
    my_lab = lab_in.at[chip]
    my_lab[0:1, :] = la[...].astype(F32)
    my_lab[1:2, :] = lb[...].astype(F32)
    buf[0] = jnp.zeros(buf.shape[1:], F32)
    with jax.named_scope("barrier"):
        pl.semaphore_wait(barrier, RINGS + 1)
    for h in range(HALF):
        w_swap(h).start()


    def ag_copy(k, j, r):
        src = xg.at[j, pl.ds(pl.multiple_of(k * slot_rows + r * rt, rt), rt)]
        dst = xg.at[j, pl.ds(pl.multiple_of((k + 1) * slot_rows + r * rt, rt), rt)]
        return pltpu.make_async_remote_copy(
            src_ref=src, dst_ref=dst, send_sem=ag_send.at[lax.rem(k, 4), j * RINGS + r],
            recv_sem=ag_recv.at[k + 1, j * RINGS + r], device_id=dev(down[r]), device_id_type=MESH)

    for b in range(BLOCKS):
        cols = pl.ds(b * hb, hb)
        pltpu.make_async_copy(xa.at[:, cols], xg.at[b, pl.ds(0, rows)], x_sem.at[2 * b]).wait()
        pltpu.make_async_copy(xb.at[:, cols], xg.at[b, pl.ds(rows, rows)], x_sem.at[2 * b + 1]).wait()
        for r in range(RINGS):
            ag_copy(0, b, r).start()

    def lab_copy(d):
        return pltpu.make_async_remote_copy(
            src_ref=lab_in.at[chip], dst_ref=lab_in.at[chip], send_sem=lab_sem.at[0, d], recv_sem=lab_sem.at[1, d],
            device_id=dev(lax.rem(chip + d, chips)), device_id_type=MESH)

    def lab_start(near):
        def go(d, carry):
            is_to = is_near(lax.rem(chip + d, chips))

            @pl.when(is_to if near else jnp.logical_not(is_to))
            def _():
                lab_copy(d).start()
            return carry
        lax.fori_loop(1, chips, go, 0)

    def lab_wait(near):
        def go(d, carry):
            is_from = is_near(lax.rem(chip + chips - d, chips))

            @pl.when(is_from if near else jnp.logical_not(is_from))
            def _():
                lab_copy(d).wait_recv()
            return carry
        lax.fori_loop(1, chips, go, 0)

    def sync_signal(n):
        for r in range(RINGS):
            pl.semaphore_signal(sync.at[n], inc=1, device_id=dev(up[r]), device_id_type=MESH)

    def sync_wait(n):
        pl.semaphore_wait(sync.at[n], RINGS)

    lab_start(True)
    sync_signal(0)
    for h in range(HALF):
        w_load(h).wait()

    sub_i = lax.broadcasted_iota(jnp.int32, (rt, 128), 0)
    lane_i = lax.broadcasted_iota(jnp.int32, (rt, 128), 1)
    eye = sub_i == lane_i
    row_lane = lax.broadcasted_iota(jnp.int32, (1, 128), 1)
    lab_sub = lax.broadcasted_iota(jnp.int32, (rt, lanes), 0)
    lab_lane = lax.broadcasted_iota(jnp.int32, (rt, lanes), 1)

    def to_row(col):
        return jnp.sum(jnp.where(eye, col, 0.0), axis=0, keepdims=True)

    def to_col(row):
        return jnp.sum(jnp.where(eye, row, 0.0), axis=1, keepdims=True)

    def fill_labels(lab, sources):
        for r in range(RINGS):
            row = lab_in[sources[r], r // 2:r // 2 + 1, :]
            col = jnp.sum(jnp.where(lab_lane == lab_sub + (r % 2) * rt, row, 0.0), axis=1, keepdims=True)
            lab[r * rt:(r + 1) * rt, :] = jnp.broadcast_to(col.astype(jnp.int32), (rt, 128))

    def sources_of(k):
        return [source(r, k) for r in range(RINGS)]

    def base(lp):
        owner = me if lp < HALF else partner
        return owner * shard + (lp % HALF) * pc

    chunk = slot_rows // 8
    per = pc // 128
    lane_at = [lax.broadcasted_iota(jnp.int32, (chunk, 128), 1) + i * 128 for i in range(per)]
    vregs = [(i // per, i % per, slice(i % per * 128, (i % per + 1) * 128)) for i in range(2 * per)]

    def hits(lab_rows, pair):
        rel = [lab_rows - base(2 * pair), lab_rows - base(2 * pair + 1)]
        return [lane_at[n] == rel[h] for h, n, _ in vregs]

    def z_dot(k0, lp):
        z = None
        for b in range(BLOCKS):
            part = jnp.dot(xg[b, pl.ds(k0, slot_rows), :], wv[lp, b * hb:(b + 1) * hb, :], preferred_element_type=F32)
            z = part if z is None else z + part
        stage[0, lp // 2, lp % 2] = z

    def z_stats(pair, lab):
        for c in range(8):
            rs = slice(c * chunk, (c + 1) * chunk)
            z = [stage[0, pair, h, rs, cs] for h, _, cs in vregs]
            m = functools.reduce(jnp.maximum, z)
            e = [jnp.exp(v - m) for v in z]
            t = functools.reduce(jnp.add, [jnp.where(h, v, 0.0) for h, v in zip(hits(lab[rs, :], pair), z)])
            s = functools.reduce(jnp.add, e)
            for (h, _, cs), v in zip(vregs, e):
                stage[0, pair, h, rs, cs] = v
            shift[0, pair, rs, :] = m
            if pair == 0:
                m_run[rs, :] = m
                s_run[rs, :] = s
                t_run[rs, :] = t
            else:
                old = m_run[rs, :]
                new = jnp.maximum(old, m)
                m_run[rs, :] = new
                s_run[rs, :] = s_run[rs, :] * jnp.exp(old - new) + s * jnp.exp(m - new)
                t_run[rs, :] = t_run[rs, :] + t

    def e_write(slot, pair):
        return Both(pltpu.make_async_copy(stage.at[0, pair], e_hbm.at[slot, pair], e_sem.at[0, pair]),
                    pltpu.make_async_copy(shift.at[0, pair], m_hbm.at[slot, pair], e_sem.at[1, pair]))

    def xt_write(slot, mb):
        return pltpu.make_async_copy(
            xtb.at[1, :, pl.ds(mb * mb_rows, slot_rows)],
            xt_hbm.at[pl.ds(mb * mb_rows, mb_rows), pl.ds(pl.multiple_of(slot * slot_rows, slot_rows), slot_rows)],
            xt_sem.at[mb])

    def run_copy(slot, r):
        return pltpu.make_async_remote_copy(
            src_ref=run_out.at[slot, r], dst_ref=run_in.at[slot + 1, r], send_sem=run_send.at[slot, r],
            recv_sem=run_recv.at[slot + 1, r], device_id=dev(down[r]), device_id_type=MESH)

    def join_stats(slot):
        with jax.named_scope("stats"):
            lane_m = m_run[...]
            m = jnp.max(lane_m, axis=1, keepdims=True)
            s = jnp.sum(s_run[...] * jnp.exp(lane_m - m), axis=1, keepdims=True)
            t = jnp.sum(t_run[...], axis=1, keepdims=True)
            rows_mst = [[to_row(v[r * rt:(r + 1) * rt]) for v in (m, s, t)] for r in range(RINGS)]

        @pl.when(slot >= 1)
        def _():
            for r in range(RINGS):
                run_copy(slot - 1, r).wait_recv()
        for r in range(RINGS):
            m_r, s_r, t_r = rows_mst[r]
            m_in = run_in[slot, r, 0:1, :]
            m_new = jnp.maximum(m_in, m_r)
            run_out[slot, r, 0:1, :] = m_new
            run_out[slot, r, 1:2, :] = s_r * jnp.exp(m_r - m_new) + run_in[slot, r, 1:2, :] * jnp.exp(m_in - m_new)
            run_out[slot, r, 2:3, :] = t_r + run_in[slot, r, 2:3, :]

    def poll(k, j):
      with jax.named_scope("poll"):
        @pl.when(k < chips)
        def _():
            for r in range(RINGS):
                ag_copy(k - 1, j, r).wait_recv()

        @pl.when(k < chips - 1)
        def _():
            @pl.when(k >= 4)
            def _():
                for r in range(RINGS):
                    ag_copy(k - 4, j, r).wait_send()
            for r in range(RINGS):
                ag_copy(k, j, r).start()

    fill_labels(labc.at[0], [chip] * RINGS)
    for r in range(RINGS):
        run_in[0, r, 0:1, :] = jnp.full((1, 128), -jnp.inf, F32)
        run_in[0, r, 1:3, :] = jnp.zeros((2, 128), F32)

    def poll_ahead(k, n):
        for lead, (first, end) in enumerate(((AHEAD[2] + 1, chips + 1), (AHEAD[1] + 1, AHEAD[2] + 1), (AHEAD[0] + 1, AHEAD[1] + 1))):
            @pl.when((k >= first) & (k < end))
            def _():
                poll(k + (n + lead) // BLOCKS, (n + lead) % BLOCKS)

        @pl.when(k <= AHEAD[0])
        def _():
            poll(k + (1 if n == 3 else 0), 2 if n == 3 else n)

    def gather_step(k, carry):
        slot = k - 1
        k0 = pl.multiple_of(slot * slot_rows, slot_rows)
        here = labc.at[lax.rem(slot, 2)]
        other = labc.at[lax.rem(slot + 1, 2)]
        ahead = sources_of(lax.rem(slot + 1, chips))

        @pl.when(slot >= 1)
        def _():
            e_write(slot - 1, 0).wait()

        with jax.named_scope("u0"):
            z_dot(k0, 0)
            z_dot(k0, 1)
            z_stats(2, other)

        @pl.when(slot == 0)
        def _():
            poll(k, 0)
        poll_ahead(k, 1)

        @pl.when(slot >= 1)
        def _():
            e_write(slot - 1, 2).start()
            join_stats(slot - 1)
            for r in range(RINGS):
                run_copy(slot - 1, r).start()
            e_write(slot - 1, 1).wait()

        @pl.when(slot == 0)
        def _():
            sync_wait(0)
            sync_signal(1)
            w_swap(0).wait()

        with jax.named_scope("u1"):
            z_dot(k0, 2)
            z_dot(k0, 3)
            z_stats(0, here)
        e_write(slot, 0).start()
        poll_ahead(k, 2)

        @pl.when(slot == 0)
        def _():
            sync_wait(1)
            sync_signal(2)
            lab_wait(True)
            poll(k, 3)
            poll(k + 1, 0)
            poll(k + 1, 1)
            w_swap(1).wait()
            w_swap(2).wait()

        @pl.when(slot >= 1)
        def _():
            e_write(slot - 1, 2).wait()
            for mb in range(MBLOCKS):
                xt_write(slot - 1, mb).wait()

        @pl.when(slot == 1)
        def _():
            lab_wait(False)

        with jax.named_scope("u2"):
            z_dot(k0, 4)
            z_dot(k0, 5)
            z_stats(1, here)
            fill_labels(other, ahead)
            for mb in range(MBLOCKS):
                at = mb * mb_rows % hb
                xtb[1, :, mb * mb_rows:(mb + 1) * mb_rows] = xg[mb * mb_rows // hb, pl.ds(k0, slot_rows), at:at + mb_rows].T
        e_write(slot, 1).start()
        for mb in range(MBLOCKS):
            xt_write(slot, mb).start()

        poll_ahead(k, 3)

        @pl.when((k != AHEAD[0]) & (k != AHEAD[1]) & (k != AHEAD[2]))
        def _():
            poll_ahead(k, 4)

        @pl.when(slot == 0)
        def _():
            sync_wait(2)
            lab_start(False)
        return carry

    lax.fori_loop(1, chips + 1, gather_step, 0)
    with jax.named_scope("flush"):
        z_stats(2, labc.at[(chips - 1) % 2])
    e_write(chips - 1, 2).start()
    join_stats(chips - 1)

    inside = row_lane < rt
    parts = []
    for r in range(RINGS):
        m, s, t = (run_out[chips - 1, r, i:i + 1, :] for i in range(3))
        bc_out[r:r + 1, :] = m
        bc_out[RINGS + r:RINGS + r + 1, :] = s
        parts.append(jnp.sum(jnp.where(inside, m + jnp.log(s) - t, 0.0), axis=1, keepdims=True))
    for mb in range(2):
        both = jnp.broadcast_to(parts[2 * mb] + parts[2 * mb + 1], (1, 128))
        bc_out[mb:mb + 1, :] = jnp.where(inside, bc_out[mb:mb + 1, :], both)
    bc_in[chip] = bc_out[...]

    def bc_copy(d):
        return pltpu.make_async_remote_copy(
            src_ref=bc_out, dst_ref=bc_in.at[chip], send_sem=bc_send.at[d], recv_sem=bc_recv.at[d],
            device_id=dev(lax.rem(chip + d, chips)), device_id_type=MESH)

    def bc_start(d, carry):
        bc_copy(d).start()
        return carry

    first_four = [source(r, 2) for r in range(RINGS)]

    def is_first(c):
        near = c == first_four[0]
        for r in range(1, RINGS):
            near = near | (c == first_four[r])
        return near

    def bc_wait_first(d, carry):
        @pl.when(is_first(lax.rem(chip + chips - d, chips)))
        def _():
            bc_copy(d).wait_recv()
        return carry

    def bc_wait_rest(d, carry):
        @pl.when(jnp.logical_not(is_first(lax.rem(chip + chips - d, chips))))
        def _():
            bc_copy(d).wait_recv()
        bc_copy(d).wait_send()
        lab_copy(d).wait_send()
        for r in range(RINGS):
            run_copy(d - 1, r).wait_send()
        return carry

    ls_copy = pltpu.make_async_remote_copy(
        src_ref=ls_out, dst_ref=ls_in, send_sem=ls_sem.at[0], recv_sem=ls_sem.at[1],
        device_id={"tp": partner}, device_id_type=MESH)

    lax.fori_loop(1, chips, bc_start, 0)

    def e_read(g):
        slot, half = lax.rem(g, chips), lax.rem(g, 2)
        return Both(pltpu.make_async_copy(e_hbm.at[slot], stage.at[half], er_sem.at[0, half]),
                    pltpu.make_async_copy(m_hbm.at[slot], shift.at[half], er_sem.at[1, half]))

    e_read(1).start()
    for pair in range(HALF):
        e_write(chips - 1, pair).wait()
    e_read(2).start()
    for mb in range(MBLOCKS):
        xt_write(chips - 1, mb).wait()

    def xt_read(mb):
        return pltpu.make_async_copy(
            xt_hbm.at[pl.ds(pl.multiple_of(mb * mb_rows, mb_rows), mb_rows), :], xtb.at[lax.rem(mb, 2)],
            xtr_sem.at[lax.rem(mb, 2)])

    xt_read(0).start()
    for k in range(chips - 5, chips - 1):
        for j in range(BLOCKS):
            for r in range(RINGS):
                ag_copy(k, j, r).wait_send()

    with jax.named_scope("bc_first"):
        lax.fori_loop(1, chips, bc_wait_first, 0)

    def form_g(g):
        slot = lax.rem(g, chips)
        half = lax.rem(g, 2)
        k0 = pl.multiple_of(slot * slot_rows, slot_rows)
        sources = sources_of(slot)
        holders = sources_of(lax.rem(slot + 1, chips))
        lab = labc.at[0]
        fill_labels(lab, sources)
        for r in range(RINGS):
            rs = slice(r * rt, (r + 1) * rt)
            m_run[rs, :] = jnp.broadcast_to(to_col(bc_in[holders[r], r:r + 1, :]), (rt, 128))
            s_run[rs, :] = jnp.broadcast_to(
                1.0 / (to_col(bc_in[holders[r], RINGS + r:RINGS + r + 1, :]) * tokens), (rt, 128))
        for pair in range(HALF):
            for c in range(8):
                rs = slice(c * chunk, (c + 1) * chunk)
                krs = pl.ds(pl.multiple_of(k0 + c * chunk, chunk), chunk)
                scale = jnp.exp(shift[half, pair, rs, :] - m_run[rs, :]) * s_run[rs, :]
                for (h, _, cs), hit in zip(vregs, hits(lab[rs, :], pair)):
                    v = stage[half, pair, h, rs, cs] * scale - jnp.where(hit, 1.0 / tokens, 0.0)
                    xg[2 * pair + h, krs, cs] = v.astype(BF16)

    e_read(1).wait()
    with jax.named_scope("g_first"):
        form_g(1)
    e_read(3).start()

    def rs_copy(s, j, r):
        b0, b1 = lax.rem(s, BUFS), lax.rem(s + 1, BUFS)
        return pltpu.make_async_remote_copy(
            src_ref=buf.at[b0, j, pl.ds(r * rt, rt)], dst_ref=buf.at[b1, j, pl.ds(r * rt, rt)],
            send_sem=rs_send.at[b0, j, r], recv_sem=rs_recv.at[b1, j, r],
            device_id=dev(down[r]), device_id_type=MESH)

    def tile_at(h, o):
        return (h, o // 2, lax.rem(o, 2))

    def dw_copy(mb, o):
        return pltpu.make_async_remote_copy(
            src_ref=stage.at[tile_at(0, o)], dst_ref=stage.at[tile_at(1, lax.rem(mb, 2) * HALF + o)],
            send_sem=dw_send.at[o],
            recv_sem=dw_recv.at[lax.rem(mb, 2), o], device_id={"tp": partner}, device_id_type=MESH)

    def dw_out(mb, o):
        return pltpu.make_async_copy(
            dwb.at[o], dw.at[pl.ds(pl.multiple_of(mb * mb_rows, mb_rows), mb_rows),
                             pl.ds(pl.multiple_of(o * pc, pc), pc)], dwo_sem.at[o])

    def dx_out(j):
        cols = pl.ds(pl.multiple_of(j * hb, hb), hb)
        return (pltpu.make_async_copy(xtb.at[0, pl.ds(0, rows), cols], dxa.at[:, cols], dxo_sem.at[j, 0]),
                pltpu.make_async_copy(xtb.at[0, pl.ds(rows, rows), cols], dxb.at[:, cols], dxo_sem.at[j, 1]))

    last = chips - 1
    dw_from = 3 * BLOCKS
    own_from = last * BLOCKS
    assert own_from - dw_from == MBLOCKS * PIECES and dw_from - 1 + BLOCKS == chips - 1

    def dx_dot(slot, j):
        k0 = pl.multiple_of(slot * slot_rows, slot_rows)
        tile = None
        for lp in range(PIECES):
            part = lax.dot_general(
                xg[lp, pl.ds(k0, slot_rows), :],
                wv[lp, pl.ds(pl.multiple_of(j * hb, hb), hb), :],
                (((1,), (1,)), ((), ())), preferred_element_type=F32)
            tile = part if tile is None else tile + part
        return tile

    def rs_arrive(s, j):
        with jax.named_scope("rs_wait"):
            for r in range(RINGS):
                rs_copy(s - 1, j, r).wait_recv()

    def rs_send_on(s, j):
        @pl.when(s >= 2)
        def _():
            for r in range(RINGS):
                pl.semaphore_wait(credit.at[j, r], 1)
        for r in range(RINGS):
            rs_copy(s, j, r).start()

    def rs_release(s, j):
        for r in range(RINGS):
            rs_copy(s - 1, j, r).wait_send()

        @pl.when(s - 1 <= last - 3)
        def _():
            for r in range(RINGS):
                pl.semaphore_signal(credit.at[j, r], inc=1, device_id=dev(up[r]), device_id_type=MESH)

    def scatter_g(i, carry):
        s = i // BLOCKS
        j = lax.rem(i, BLOCKS)
        b0 = lax.rem(s, BUFS)
        double = s == 1
        g = jnp.where(s == 0, i + 1, jnp.where(double, 2 * i - BLOCKS + 1, i + BLOCKS + 1))

        @pl.when(s >= 1)
        def _():
            rs_arrive(s, j)

        e_read(g).wait()
        with jax.named_scope("dx_g"):
            buf[b0, j] = buf[b0, j] + dx_dot(s + 1, j)
            form_g(g)
        rs_send_on(s, j)

        @pl.when(g + 2 <= chips)
        def _():
            e_read(g + 2).start()

        @pl.when(double)
        def _():
            e_read(g + 1).wait()
            with jax.named_scope("g"):
                form_g(g + 1)

            @pl.when(g + 3 <= chips)
            def _():
                e_read(g + 3).start()

        @pl.when(s >= 1)
        def _():
            rs_release(s, j)
        return carry

    with jax.named_scope("dx_first"):
        buf[0, 0] = dx_dot(1, 0)
    rs_send_on(0, 0)
    with jax.named_scope("bc_far"):
        lax.fori_loop(1, chips, bc_wait_rest, 0)
    lax.fori_loop(1, dw_from, scatter_g, 0)
    pl.semaphore_signal(dw_credit, inc=1, device_id={"tp": partner}, device_id_type=MESH)
    total = bc_in[0]
    for c in range(1, chips):
        total = total + bc_in[c]
    ls_out[...] = total
    ls_copy.start()

    def scatter_dw(i, carry):
        s = i // BLOCKS
        j = lax.rem(i, BLOCKS)
        b0 = lax.rem(s, BUFS)
        q = i - dw_from
        mb = q // PIECES
        o = lax.rem(q, PIECES)
        rs_arrive(s, j)

        @pl.when(o == 0)
        def _():
            xt_read(mb).wait()

            @pl.when(mb < MBLOCKS - 1)
            def _():
                xt_read(mb + 1).start()

        @pl.when((o < HALF) & (mb >= 1))
        def _():
            dw_copy(mb - 1, o).wait_send()

        with jax.named_scope("dx_dw"):
            buf[b0, j] = buf[b0, j] + dx_dot(s + 1, j)
            stage[tile_at(0, o)] = jnp.dot(xtb[lax.rem(mb, 2)], xg[lax.rem(o + HALF, PIECES)], preferred_element_type=F32)
        rs_send_on(s, j)

        @pl.when((o == 0) & (mb != 1))
        def _():
            pl.semaphore_wait(dw_credit, 1)

        @pl.when(o < HALF)
        def _():
            dw_copy(mb, o).start()

        @pl.when(o >= HALF)
        def _():
            h = o - HALF
            dw_copy(mb, h).wait_recv()

            @pl.when(mb >= 1)
            def _():
                dw_out(mb - 1, h).wait()
            dwb[h] = (stage[tile_at(0, o)] + stage[tile_at(1, lax.rem(mb, 2) * HALF + h)]).astype(BF16)
            dw_out(mb, h).start()

            @pl.when((h == HALF - 1) & (mb < MBLOCKS - 2))
            def _():
                pl.semaphore_signal(dw_credit, inc=1, device_id={"tp": partner}, device_id_type=MESH)

        rs_release(s, j)
        return carry

    lax.fori_loop(dw_from, own_from, scatter_dw, 0)

    def scatter_last(j, carry):
        with jax.named_scope("own"):
            stage[0, HALF - 1, 1] = dx_dot(0, j)
        rs_arrive(last, j)
        with jax.named_scope("out"):
            xtb[0, 0:slot_rows, pl.ds(pl.multiple_of(j * hb, hb), hb)] = (
                buf[last % BUFS, j] + stage[0, HALF - 1, 1]).astype(BF16)
        for c in dx_out(j):
            c.start()
        rs_release(last, j)
        return carry

    lax.fori_loop(0, BLOCKS, scatter_last, 0)

    ls_copy.wait()
    both = (ls_out[...] + ls_in[...]) * (1.0 / tokens)
    loss[0] = both[0, lanes - 1]
    loss[1] = both[1, lanes - 1]
    for o in range(HALF):
        dw_copy(MBLOCKS - 1, o).wait_send()
        dw_out(MBLOCKS - 1, o).wait()
    for j in range(BLOCKS):
        for c in dx_out(j):
            c.wait()


def copy_kernel(loss, dw, dxa, dxb, loss_out, dw_out, dxa_out, dxb_out, dw_v, dxa_v, dxb_v, in_sem, out_sem):
    moves = []
    for n, (src, via, dst) in enumerate(((dw, dw_v, dw_out), (dxa, dxa_v, dxa_out), (dxb, dxb_v, dxb_out))):
        parts = 2 * MBLOCKS if n == 0 else 2
        size = src.shape[0] // parts
        for p in range(parts):
            at = pl.ds(p * size, size)
            moves.append((pltpu.make_async_copy(src.at[at], via.at[at], in_sem.at[n, p]),
                          pltpu.make_async_copy(via.at[at], dst.at[at], out_sem.at[n, p])))
    for load, _ in moves:
        load.start()
    loss_out[0] = loss[0]
    loss_out[1] = loss[1]
    for load, store in moves:
        load.wait()
        store.start()
    for _, store in moves:
        store.wait()


def solution(mesh):
    group = mesh.shape["tp"]
    chips = group // 2

    def local_step(x_a, x_b, labels_a, labels_b, w_local):
        rows, hidden = x_a.shape
        shard = w_local.shape[1]
        slot_rows = 2 * rows
        all_rows = chips * slot_rows
        hb = hidden // BLOCKS
        pc = shard // HALF
        mb_rows = hidden // MBLOCKS
        any_spec = pl.BlockSpec(memory_space=pl.ANY)
        vmem_spec = pl.BlockSpec(memory_space=pltpu.VMEM)
        out = pl.pallas_call(
            functools.partial(head_kernel, group),
            name="head",
            out_shape=(
                jax.ShapeDtypeStruct((2,), F32),
                jax.ShapeDtypeStruct((hidden, shard), BF16),
                jax.ShapeDtypeStruct((rows, hidden), BF16),
                jax.ShapeDtypeStruct((rows, hidden), BF16),
                jax.ShapeDtypeStruct((chips, HALF, 2, slot_rows, pc), F32),
                jax.ShapeDtypeStruct((chips, HALF, slot_rows, 128), F32),
                jax.ShapeDtypeStruct((hidden, all_rows), BF16),
            ),
            in_specs=[any_spec, any_spec, vmem_spec, vmem_spec, any_spec],
            out_specs=(pl.BlockSpec(memory_space=pltpu.SMEM),) + (any_spec,) * 6,
            scratch_shapes=[
                pltpu.VMEM((PIECES, hidden, pc), BF16),
                pltpu.VMEM((PIECES, all_rows, pc), BF16),
                pltpu.VMEM((2, HALF, 2, slot_rows, pc), F32),
                pltpu.VMEM((2, HALF, slot_rows, 128), F32),
                pltpu.VMEM((2, mb_rows, all_rows), BF16),
                pltpu.VMEM((BUFS, BLOCKS, slot_rows, hb), F32),
                pltpu.VMEM((HALF, mb_rows, pc), BF16),
                pltpu.VMEM((slot_rows, 128), F32),
                pltpu.VMEM((slot_rows, 128), F32),
                pltpu.VMEM((slot_rows, 128), F32),
                pltpu.VMEM((2, slot_rows, 128), jnp.int32),
                pltpu.VMEM((chips, 2, rows), F32),
                pltpu.VMEM((chips, RINGS, 4, 128), F32),
                pltpu.VMEM((chips, RINGS, 4, 128), F32),
                pltpu.VMEM((chips, 8, 128), F32),
                pltpu.VMEM((8, 128), F32),
                pltpu.VMEM((8, 128), F32),
                pltpu.VMEM((8, 128), F32),
            ],
            compiler_params=pltpu.CompilerParams(
                collective_id=0, has_side_effects=True, vmem_limit_bytes=67043328),
        )(x_a, x_b, labels_a.reshape(1, rows), labels_b.reshape(1, rows), w_local)
        results = out[:4]
        return pl.pallas_call(
            copy_kernel,
            name="results",
            out_shape=tuple(jax.ShapeDtypeStruct(v.shape, v.dtype) for v in results),
            in_specs=[pl.BlockSpec(memory_space=pltpu.SMEM), any_spec, any_spec, any_spec],
            out_specs=(pl.BlockSpec(memory_space=pltpu.SMEM), any_spec, any_spec, any_spec),
            scratch_shapes=[pltpu.VMEM(v.shape, v.dtype) for v in results[1:]] + [
                pltpu.SemaphoreType.DMA((3, 2 * MBLOCKS)), pltpu.SemaphoreType.DMA((3, 2 * MBLOCKS))],
        )(*results)

    row_spec = P(("dp", "tp"), None)
    label_spec = P(("dp", "tp"))
    return jax.shard_map(local_step, mesh=mesh, in_specs=(row_spec, row_spec, label_spec, label_spec, P(None, "tp")), out_specs=(P("dp"), P("dp", "tp"), row_spec, row_spec), check_vma=False)
```

```python
import functools
import math

import jax
import jax.numpy as jnp
from jax import lax
from jax.experimental import pallas as pl
from jax.experimental.pallas import tpu as pltpu
from jax.sharding import PartitionSpec as P

MESH = pl.DeviceIdType.MESH
F32 = jnp.float32
BF16 = jnp.bfloat16
RINGS = 4
BLOCKS = 4
HALF = 3
PIECES = 2 * HALF
MBLOCKS = 8
BUFS = 3
AHEAD = (1, 5, 10)


class Both:
    def __init__(self, *copies):
        self.copies = copies

    def start(self):
        for c in self.copies:
            c.start()

    def wait(self):
        for c in self.copies:
            c.wait()


def head_kernel(group, *refs):
    chips = group // 2
    dma = pltpu.SemaphoreType.DMA
    regular = pltpu.SemaphoreType.REGULAR
    pl.run_scoped(
        functools.partial(head_body, group, *refs),
        x_sem=dma((2 * BLOCKS,)), w_sem=dma((HALF,)), wp_sem=dma((2, HALF)), lab_sem=dma((2, chips)), sync=regular((3,)),
        ag_send=dma((4, BLOCKS * RINGS)), ag_recv=dma((chips, BLOCKS * RINGS)),
        e_sem=dma((2, HALF)), er_sem=dma((2, 2)), xt_sem=dma((MBLOCKS,)), xtr_sem=dma((2,)),
        run_send=dma((chips, RINGS)), run_recv=dma((chips, RINGS)), bc_send=dma((chips,)), bc_recv=dma((chips,)),
        ls_sem=dma((2,)), rs_send=dma((BUFS, BLOCKS, RINGS)), rs_recv=dma((BUFS, BLOCKS, RINGS)),
        credit=regular((BLOCKS, RINGS)), dw_send=dma((HALF,)), dw_recv=dma((2, HALF)), dw_credit=regular,
        dwo_sem=dma((HALF,)), dxo_sem=dma((BLOCKS, 2)))


def head_body(group, xa, xb, la, lb, w, loss, dw, dxa, dxb, e_hbm, m_hbm, xt_hbm,
              wv, xg, stage, shift, xtb, buf, dwb, m_run, s_run, t_run, labc,
              lab_in, run_out, run_in, bc_in, bc_out, ls_out, ls_in,
              x_sem, w_sem, wp_sem, lab_sem, sync, ag_send, ag_recv, e_sem, er_sem, xt_sem, xtr_sem, run_send, run_recv,
              bc_send, bc_recv, ls_sem, rs_send, rs_recv, credit, dw_send, dw_recv, dw_credit, dwo_sem, dxo_sem):
    chips = group // 2
    side = math.isqrt(chips)
    rows = xa.shape[0]
    slot_rows = 2 * rows
    rt = slot_rows // RINGS
    hb = xg.shape[2]
    pc = hb
    shard = w.shape[1]
    tokens = rows * group
    mb_rows = w.shape[0] // MBLOCKS
    lanes = lab_in.shape[2]

    me = lax.axis_index("tp")
    core = lax.rem(me, 2)
    chip = me // 2
    partner = me + 1 - 2 * core
    cx = lax.rem(chip, side)
    cy = chip // side
    diag = lax.rem(cx + cy, side)
    pos = (side * cy + diag, side * lax.rem(cx + 1, side) + diag)

    def dev(c):
        return {"tp": 2 * c + core}

    def chip_at(cycle, p):
        major, minor = p // side, lax.rem(p, side)
        if cycle == 0:
            yy = major
            xx = lax.rem(minor - major + side, side)
        else:
            xx = lax.rem(major + side - 1, side)
            yy = lax.rem(minor + 1 - major + side, side)
        return yy * side + xx

    def source(r, k):
        sign = -1 if r % 2 == 0 else 1
        return chip_at(r // 2, lax.rem(pos[r // 2] + sign * k + 2 * chips, chips))

    up = [source(r, 1) for r in range(RINGS)]
    down = [source(r, -1) for r in range(RINGS)]

    for b in range(BLOCKS):
        cols = pl.ds(b * hb, hb)
        pltpu.make_async_copy(xa.at[:, cols], xg.at[b, pl.ds(0, rows)], x_sem.at[2 * b]).start()
        pltpu.make_async_copy(xb.at[:, cols], xg.at[b, pl.ds(rows, rows)], x_sem.at[2 * b + 1]).start()

    def w_load(h):
        return pltpu.make_async_copy(w.at[:, pl.ds(h * pc, pc)], wv.at[h], w_sem.at[h])

    def w_swap(h):
        return pltpu.make_async_remote_copy(
            src_ref=w.at[:, pl.ds(h * pc, pc)], dst_ref=wv.at[HALF + h], send_sem=wp_sem.at[0, h],
            recv_sem=wp_sem.at[1, h], device_id={"tp": partner}, device_id_type=MESH)

    for h in range(HALF):
        w_load(h).start()

    barrier = pltpu.get_barrier_semaphore()

    def is_near(c):
        near = c == up[0]
        for r in range(1, RINGS):
            near = near | (c == up[r])
        return near

    for r in range(RINGS):
        pl.semaphore_signal(barrier, inc=1, device_id=dev(up[r]), device_id_type=MESH)
    pl.semaphore_signal(barrier, inc=1, device_id={"tp": partner}, device_id_type=MESH)
    my_lab = lab_in.at[chip]
    my_lab[0:1, :] = la[...].astype(F32)
    my_lab[1:2, :] = lb[...].astype(F32)
    buf[0] = jnp.zeros(buf.shape[1:], F32)
    with jax.named_scope("barrier"):
        pl.semaphore_wait(barrier, RINGS + 1)
    for h in range(HALF):
        w_swap(h).start()


    def ag_copy(k, j, r):
        src = xg.at[j, pl.ds(pl.multiple_of(k * slot_rows + r * rt, rt), rt)]
        dst = xg.at[j, pl.ds(pl.multiple_of((k + 1) * slot_rows + r * rt, rt), rt)]
        return pltpu.make_async_remote_copy(
            src_ref=src, dst_ref=dst, send_sem=ag_send.at[lax.rem(k, 4), j * RINGS + r],
            recv_sem=ag_recv.at[k + 1, j * RINGS + r], device_id=dev(down[r]), device_id_type=MESH)

    for b in range(BLOCKS):
        cols = pl.ds(b * hb, hb)
        pltpu.make_async_copy(xa.at[:, cols], xg.at[b, pl.ds(0, rows)], x_sem.at[2 * b]).wait()
        pltpu.make_async_copy(xb.at[:, cols], xg.at[b, pl.ds(rows, rows)], x_sem.at[2 * b + 1]).wait()
        for r in range(RINGS):
            ag_copy(0, b, r).start()

    def lab_copy(d):
        return pltpu.make_async_remote_copy(
            src_ref=lab_in.at[chip], dst_ref=lab_in.at[chip], send_sem=lab_sem.at[0, d], recv_sem=lab_sem.at[1, d],
            device_id=dev(lax.rem(chip + d, chips)), device_id_type=MESH)

    def lab_start(near):
        def go(d, carry):
            is_to = is_near(lax.rem(chip + d, chips))

            @pl.when(is_to if near else jnp.logical_not(is_to))
            def _():
                lab_copy(d).start()
            return carry
        lax.fori_loop(1, chips, go, 0)

    def lab_wait(near):
        def go(d, carry):
            is_from = is_near(lax.rem(chip + chips - d, chips))

            @pl.when(is_from if near else jnp.logical_not(is_from))
            def _():
                lab_copy(d).wait_recv()
            return carry
        lax.fori_loop(1, chips, go, 0)

    def sync_signal(n):
        for r in range(RINGS):
            pl.semaphore_signal(sync.at[n], inc=1, device_id=dev(up[r]), device_id_type=MESH)

    def sync_wait(n):
        pl.semaphore_wait(sync.at[n], RINGS)

    lab_start(True)
    sync_signal(0)
    for h in range(HALF):
        w_load(h).wait()

    sub_i = lax.broadcasted_iota(jnp.int32, (rt, 128), 0)
    lane_i = lax.broadcasted_iota(jnp.int32, (rt, 128), 1)
    eye = sub_i == lane_i
    row_lane = lax.broadcasted_iota(jnp.int32, (1, 128), 1)
    lab_sub = lax.broadcasted_iota(jnp.int32, (rt, lanes), 0)
    lab_lane = lax.broadcasted_iota(jnp.int32, (rt, lanes), 1)

    def to_row(col):
        return jnp.sum(jnp.where(eye, col, 0.0), axis=0, keepdims=True)

    def to_col(row):
        return jnp.sum(jnp.where(eye, row, 0.0), axis=1, keepdims=True)

    def fill_labels(lab, sources):
        for r in range(RINGS):
            row = lab_in[sources[r], r // 2:r // 2 + 1, :]
            col = jnp.sum(jnp.where(lab_lane == lab_sub + (r % 2) * rt, row, 0.0), axis=1, keepdims=True)
            lab[r * rt:(r + 1) * rt, :] = jnp.broadcast_to(col.astype(jnp.int32), (rt, 128))

    def sources_of(k):
        return [source(r, k) for r in range(RINGS)]

    def base(lp):
        owner = me if lp < HALF else partner
        return owner * shard + (lp % HALF) * pc

    chunk = slot_rows // 8
    per = pc // 128
    lane_at = [lax.broadcasted_iota(jnp.int32, (chunk, 128), 1) + i * 128 for i in range(per)]
    vregs = [(i // per, i % per, slice(i % per * 128, (i % per + 1) * 128)) for i in range(2 * per)]

    def hits(lab_rows, pair):
        rel = [lab_rows - base(2 * pair), lab_rows - base(2 * pair + 1)]
        return [lane_at[n] == rel[h] for h, n, _ in vregs]

    def z_dot(k0, lp):
        z = None
        for b in range(BLOCKS):
            part = jnp.dot(xg[b, pl.ds(k0, slot_rows), :], wv[lp, b * hb:(b + 1) * hb, :], preferred_element_type=F32)
            z = part if z is None else z + part
        stage[0, lp // 2, lp % 2] = z

    def z_stats(pair, lab):
        for c in range(8):
            rs = slice(c * chunk, (c + 1) * chunk)
            z = [stage[0, pair, h, rs, cs] for h, _, cs in vregs]
            m = functools.reduce(jnp.maximum, z)
            e = [jnp.exp(v - m) for v in z]
            t = functools.reduce(jnp.add, [jnp.where(h, v, 0.0) for h, v in zip(hits(lab[rs, :], pair), z)])
            s = functools.reduce(jnp.add, e)
            for (h, _, cs), v in zip(vregs, e):
                stage[0, pair, h, rs, cs] = v
            shift[0, pair, rs, :] = m
            if pair == 0:
                m_run[rs, :] = m
                s_run[rs, :] = s
                t_run[rs, :] = t
            else:
                old = m_run[rs, :]
                new = jnp.maximum(old, m)
                m_run[rs, :] = new
                s_run[rs, :] = s_run[rs, :] * jnp.exp(old - new) + s * jnp.exp(m - new)
                t_run[rs, :] = t_run[rs, :] + t

    def e_write(slot, pair):
        return Both(pltpu.make_async_copy(stage.at[0, pair], e_hbm.at[slot, pair], e_sem.at[0, pair]),
                    pltpu.make_async_copy(shift.at[0, pair], m_hbm.at[slot, pair], e_sem.at[1, pair]))

    def xt_write(slot, mb):
        return pltpu.make_async_copy(
            xtb.at[1, :, pl.ds(mb * mb_rows, slot_rows)],
            xt_hbm.at[pl.ds(mb * mb_rows, mb_rows), pl.ds(pl.multiple_of(slot * slot_rows, slot_rows), slot_rows)],
            xt_sem.at[mb])

    def run_copy(slot, r):
        return pltpu.make_async_remote_copy(
            src_ref=run_out.at[slot, r], dst_ref=run_in.at[slot + 1, r], send_sem=run_send.at[slot, r],
            recv_sem=run_recv.at[slot + 1, r], device_id=dev(down[r]), device_id_type=MESH)

    def join_stats(slot):
        with jax.named_scope("stats"):
            lane_m = m_run[...]
            m = jnp.max(lane_m, axis=1, keepdims=True)
            s = jnp.sum(s_run[...] * jnp.exp(lane_m - m), axis=1, keepdims=True)
            t = jnp.sum(t_run[...], axis=1, keepdims=True)
            rows_mst = [[to_row(v[r * rt:(r + 1) * rt]) for v in (m, s, t)] for r in range(RINGS)]

        @pl.when(slot >= 1)
        def _():
            for r in range(RINGS):
                run_copy(slot - 1, r).wait_recv()
        for r in range(RINGS):
            m_r, s_r, t_r = rows_mst[r]
            m_in = run_in[slot, r, 0:1, :]
            m_new = jnp.maximum(m_in, m_r)
            run_out[slot, r, 0:1, :] = m_new
            run_out[slot, r, 1:2, :] = s_r * jnp.exp(m_r - m_new) + run_in[slot, r, 1:2, :] * jnp.exp(m_in - m_new)
            run_out[slot, r, 2:3, :] = t_r + run_in[slot, r, 2:3, :]

    def poll(k, j):
      with jax.named_scope("poll"):
        @pl.when(k < chips)
        def _():
            for r in range(RINGS):
                ag_copy(k - 1, j, r).wait_recv()

        @pl.when(k < chips - 1)
        def _():
            @pl.when(k >= 4)
            def _():
                for r in range(RINGS):
                    ag_copy(k - 4, j, r).wait_send()
            for r in range(RINGS):
                ag_copy(k, j, r).start()

    fill_labels(labc.at[0], [chip] * RINGS)
    for r in range(RINGS):
        run_in[0, r, 0:1, :] = jnp.full((1, 128), -jnp.inf, F32)
        run_in[0, r, 1:3, :] = jnp.zeros((2, 128), F32)

    def poll_ahead(k, n):
        for lead, (first, end) in enumerate(((AHEAD[2] + 1, chips + 1), (AHEAD[1] + 1, AHEAD[2] + 1), (AHEAD[0] + 1, AHEAD[1] + 1))):
            @pl.when((k >= first) & (k < end))
            def _():
                poll(k + (n + lead) // BLOCKS, (n + lead) % BLOCKS)

        @pl.when(k <= AHEAD[0])
        def _():
            poll(k + (1 if n == 3 else 0), 2 if n == 3 else n)

    def gather_step(k, carry):
        slot = k - 1
        k0 = pl.multiple_of(slot * slot_rows, slot_rows)
        here = labc.at[lax.rem(slot, 2)]
        other = labc.at[lax.rem(slot + 1, 2)]
        ahead = sources_of(lax.rem(slot + 1, chips))

        @pl.when(slot >= 1)
        def _():
            e_write(slot - 1, 0).wait()

        with jax.named_scope("u0"):
            z_dot(k0, 0)
            z_dot(k0, 1)
            z_stats(2, other)

        @pl.when(slot == 0)
        def _():
            poll(k, 0)
        poll_ahead(k, 1)

        @pl.when(slot >= 1)
        def _():
            e_write(slot - 1, 2).start()
            join_stats(slot - 1)
            for r in range(RINGS):
                run_copy(slot - 1, r).start()
            e_write(slot - 1, 1).wait()

        @pl.when(slot == 0)
        def _():
            sync_wait(0)
            sync_signal(1)
            w_swap(0).wait()

        with jax.named_scope("u1"):
            z_dot(k0, 2)
            z_dot(k0, 3)
            z_stats(0, here)
        e_write(slot, 0).start()
        poll_ahead(k, 2)

        @pl.when(slot == 0)
        def _():
            sync_wait(1)
            sync_signal(2)
            lab_wait(True)
            poll(k, 3)
            poll(k + 1, 0)
            poll(k + 1, 1)
            w_swap(1).wait()
            w_swap(2).wait()

        @pl.when(slot >= 1)
        def _():
            e_write(slot - 1, 2).wait()
            for mb in range(MBLOCKS):
                xt_write(slot - 1, mb).wait()

        @pl.when(slot == 1)
        def _():
            lab_wait(False)

        with jax.named_scope("u2"):
            z_dot(k0, 4)
            z_dot(k0, 5)
            z_stats(1, here)
            fill_labels(other, ahead)
            for mb in range(MBLOCKS):
                at = mb * mb_rows % hb
                xtb[1, :, mb * mb_rows:(mb + 1) * mb_rows] = xg[mb * mb_rows // hb, pl.ds(k0, slot_rows), at:at + mb_rows].T
        e_write(slot, 1).start()
        for mb in range(MBLOCKS):
            xt_write(slot, mb).start()

        poll_ahead(k, 3)

        @pl.when((k != AHEAD[0]) & (k != AHEAD[1]) & (k != AHEAD[2]))
        def _():
            poll_ahead(k, 4)

        @pl.when(slot == 0)
        def _():
            sync_wait(2)
            lab_start(False)
        return carry

    lax.fori_loop(1, chips + 1, gather_step, 0)
    def e_read(g):
        slot, half = lax.rem(2 * chips - g, chips), lax.rem(g + 1, 2)
        return Both(pltpu.make_async_copy(e_hbm.at[slot], stage.at[half], er_sem.at[0, half]),
                    pltpu.make_async_copy(m_hbm.at[slot], shift.at[half], er_sem.at[1, half]))

    e_read(2).start()
    with jax.named_scope("flush"):
        z_stats(2, labc.at[(chips - 1) % 2])
    e_write(chips - 1, 2).start()
    join_stats(chips - 1)

    inside = row_lane < rt
    parts = []
    for r in range(RINGS):
        m, s, t = (run_out[chips - 1, r, i:i + 1, :] for i in range(3))
        bc_out[r:r + 1, :] = m
        bc_out[RINGS + r:RINGS + r + 1, :] = s
        parts.append(jnp.sum(jnp.where(inside, m + jnp.log(s) - t, 0.0), axis=1, keepdims=True))
    for mb in range(2):
        both = jnp.broadcast_to(parts[2 * mb] + parts[2 * mb + 1], (1, 128))
        bc_out[mb:mb + 1, :] = jnp.where(inside, bc_out[mb:mb + 1, :], both)
    bc_in[chip] = bc_out[...]

    def bc_copy(d):
        return pltpu.make_async_remote_copy(
            src_ref=bc_out, dst_ref=bc_in.at[chip], send_sem=bc_send.at[d], recv_sem=bc_recv.at[d],
            device_id=dev(lax.rem(chip + d, chips)), device_id_type=MESH)

    def bc_start(d, carry):
        bc_copy(d).start()
        return carry

    def bc_wait_first(d, carry):
        @pl.when(is_near(lax.rem(chip + chips - d, chips)))
        def _():
            bc_copy(d).wait_recv()
        return carry

    def bc_wait_rest(d, carry):
        @pl.when(jnp.logical_not(is_near(lax.rem(chip + chips - d, chips))))
        def _():
            bc_copy(d).wait_recv()
        bc_copy(d).wait_send()
        lab_copy(d).wait_send()
        for r in range(RINGS):
            run_copy(d - 1, r).wait_send()
        return carry

    ls_copy = pltpu.make_async_remote_copy(
        src_ref=ls_out, dst_ref=ls_in, send_sem=ls_sem.at[0], recv_sem=ls_sem.at[1],
        device_id={"tp": partner}, device_id_type=MESH)

    lax.fori_loop(1, chips, bc_start, 0)

    def xt_read(mb):
        return pltpu.make_async_copy(
            xt_hbm.at[pl.ds(pl.multiple_of(mb * mb_rows, mb_rows), mb_rows), :], xtb.at[lax.rem(mb, 2)],
            xtr_sem.at[lax.rem(mb, 2)])

    def form_g(g):
        slot = lax.rem(2 * chips - g, chips)
        half = lax.rem(g + 1, 2)
        k0 = pl.multiple_of(slot * slot_rows, slot_rows)
        sources = sources_of(slot)
        holders = sources_of(lax.rem(slot + 1, chips))
        lab = labc.at[0]
        fill_labels(lab, sources)
        for r in range(RINGS):
            rs = slice(r * rt, (r + 1) * rt)
            m_run[rs, :] = jnp.broadcast_to(to_col(bc_in[holders[r], r:r + 1, :]), (rt, 128))
            s_run[rs, :] = jnp.broadcast_to(
                1.0 / (to_col(bc_in[holders[r], RINGS + r:RINGS + r + 1, :]) * tokens), (rt, 128))
        for pair in range(HALF):
            for c in range(8):
                rs = slice(c * chunk, (c + 1) * chunk)
                krs = pl.ds(pl.multiple_of(k0 + c * chunk, chunk), chunk)
                scale = jnp.exp(shift[half, pair, rs, :] - m_run[rs, :]) * s_run[rs, :]
                for (h, _, cs), hit in zip(vregs, hits(lab[rs, :], pair)):
                    v = stage[half, pair, h, rs, cs] * scale - jnp.where(hit, 1.0 / tokens, 0.0)
                    xg[2 * pair + h, krs, cs] = v.astype(BF16)

    with jax.named_scope("g_first"):
        form_g(1)

    def rs_copy(s, j, r):
        b0, b1 = lax.rem(s, BUFS), lax.rem(s + 1, BUFS)
        return pltpu.make_async_remote_copy(
            src_ref=buf.at[b0, j, pl.ds(r * rt, rt)], dst_ref=buf.at[b1, j, pl.ds(r * rt, rt)],
            send_sem=rs_send.at[b0, j, r], recv_sem=rs_recv.at[b1, j, r],
            device_id=dev(up[r]), device_id_type=MESH)

    def tile_at(h, o):
        return (h, o // 2, lax.rem(o, 2))

    def dw_copy(mb, o):
        return pltpu.make_async_remote_copy(
            src_ref=stage.at[tile_at(0, o)], dst_ref=stage.at[tile_at(1, lax.rem(mb, 2) * HALF + o)],
            send_sem=dw_send.at[o],
            recv_sem=dw_recv.at[lax.rem(mb, 2), o], device_id={"tp": partner}, device_id_type=MESH)

    def dw_out(mb, o):
        return pltpu.make_async_copy(
            dwb.at[o], dw.at[pl.ds(pl.multiple_of(mb * mb_rows, mb_rows), mb_rows),
                             pl.ds(pl.multiple_of(o * pc, pc), pc)], dwo_sem.at[o])

    def dx_out(j):
        cols = pl.ds(pl.multiple_of(j * hb, hb), hb)
        return (pltpu.make_async_copy(xtb.at[0, pl.ds(0, rows), cols], dxa.at[:, cols], dxo_sem.at[j, 0]),
                pltpu.make_async_copy(xtb.at[0, pl.ds(rows, rows), cols], dxb.at[:, cols], dxo_sem.at[j, 1]))

    last = chips - 1
    dw_from = 3 * BLOCKS
    own_from = last * BLOCKS
    assert own_from - dw_from == MBLOCKS * PIECES and dw_from - 1 + BLOCKS == chips - 1

    def dx_dot(slot, j):
        k0 = pl.multiple_of(slot * slot_rows, slot_rows)
        tile = None
        for lp in range(PIECES):
            part = lax.dot_general(
                xg[lp, pl.ds(k0, slot_rows), :],
                wv[lp, pl.ds(pl.multiple_of(j * hb, hb), hb), :],
                (((1,), (1,)), ((), ())), preferred_element_type=F32)
            tile = part if tile is None else tile + part
        return tile

    def rs_arrive(s, j):
        with jax.named_scope("rs_wait"):
            for r in range(RINGS):
                rs_copy(s - 1, j, r).wait_recv()

    def rs_send_on(s, j):
        @pl.when(s >= 2)
        def _():
            for r in range(RINGS):
                pl.semaphore_wait(credit.at[j, r], 1)
        for r in range(RINGS):
            rs_copy(s, j, r).start()

    def rs_release(s, j):
        for r in range(RINGS):
            rs_copy(s - 1, j, r).wait_send()

        @pl.when(s - 1 <= last - 3)
        def _():
            for r in range(RINGS):
                pl.semaphore_signal(credit.at[j, r], inc=1, device_id=dev(down[r]), device_id_type=MESH)

    def scatter_g(i, carry):
        s = i // BLOCKS
        j = lax.rem(i, BLOCKS)
        b0 = lax.rem(s, BUFS)
        double = s == 1
        g = jnp.where(s == 0, i + 1, jnp.where(double, 2 * i - BLOCKS + 1, i + BLOCKS + 1))

        @pl.when(s >= 1)
        def _():
            rs_arrive(s, j)

        @pl.when(i == 2)
        def _():
            with jax.named_scope("bc_rest"):
                lax.fori_loop(1, chips, bc_wait_rest, 0)

        e_read(g).wait()
        with jax.named_scope("dx_g"):
            buf[b0, j] = buf[b0, j] + dx_dot(last - s, j)
            form_g(g)
        rs_send_on(s, j)

        @pl.when(g + 2 <= chips)
        def _():
            e_read(g + 2).start()

        @pl.when(double)
        def _():
            e_read(g + 1).wait()
            with jax.named_scope("g"):
                form_g(g + 1)

            @pl.when(g + 3 <= chips)
            def _():
                e_read(g + 3).start()

        @pl.when(s >= 1)
        def _():
            rs_release(s, j)
        return carry

    with jax.named_scope("dx_first"):
        buf[0, 0] = dx_dot(last, 0)
    rs_send_on(0, 0)
    for pair in range(HALF):
        e_write(chips - 1, pair).wait()
    e_read(3).start()
    for mb in range(MBLOCKS):
        xt_write(chips - 1, mb).wait()
    xt_read(0).start()
    for k in range(chips - 5, chips - 1):
        for j in range(BLOCKS):
            for r in range(RINGS):
                ag_copy(k, j, r).wait_send()

    with jax.named_scope("bc_first"):
        lax.fori_loop(1, chips, bc_wait_first, 0)

    lax.fori_loop(1, dw_from, scatter_g, 0)
    pl.semaphore_signal(dw_credit, inc=1, device_id={"tp": partner}, device_id_type=MESH)
    total = bc_in[0]
    for c in range(1, chips):
        total = total + bc_in[c]
    ls_out[...] = total
    ls_copy.start()

    def scatter_dw(i, carry):
        s = i // BLOCKS
        j = lax.rem(i, BLOCKS)
        b0 = lax.rem(s, BUFS)
        q = i - dw_from
        mb = q // PIECES
        o = lax.rem(q, PIECES)
        rs_arrive(s, j)

        @pl.when(o == 0)
        def _():
            xt_read(mb).wait()

            @pl.when(mb < MBLOCKS - 1)
            def _():
                xt_read(mb + 1).start()

        @pl.when((o < HALF) & (mb >= 1))
        def _():
            dw_copy(mb - 1, o).wait_send()

        with jax.named_scope("dx_dw"):
            buf[b0, j] = buf[b0, j] + dx_dot(last - s, j)
            stage[tile_at(0, o)] = jnp.dot(xtb[lax.rem(mb, 2)], xg[lax.rem(o + HALF, PIECES)], preferred_element_type=F32)
        rs_send_on(s, j)

        @pl.when((o == 0) & (mb != 1))
        def _():
            pl.semaphore_wait(dw_credit, 1)

        @pl.when(o < HALF)
        def _():
            dw_copy(mb, o).start()

        @pl.when(o >= HALF)
        def _():
            h = o - HALF
            dw_copy(mb, h).wait_recv()

            @pl.when(mb >= 1)
            def _():
                dw_out(mb - 1, h).wait()
            dwb[h] = (stage[tile_at(0, o)] + stage[tile_at(1, lax.rem(mb, 2) * HALF + h)]).astype(BF16)
            dw_out(mb, h).start()

            @pl.when((h == HALF - 1) & (mb < MBLOCKS - 2))
            def _():
                pl.semaphore_signal(dw_credit, inc=1, device_id={"tp": partner}, device_id_type=MESH)

        rs_release(s, j)
        return carry

    lax.fori_loop(dw_from, own_from, scatter_dw, 0)

    def scatter_last(j, carry):
        with jax.named_scope("own"):
            stage[0, HALF - 1, 1] = dx_dot(0, j)
        rs_arrive(last, j)
        with jax.named_scope("out"):
            xtb[0, 0:slot_rows, pl.ds(pl.multiple_of(j * hb, hb), hb)] = (
                buf[last % BUFS, j] + stage[0, HALF - 1, 1]).astype(BF16)
        for c in dx_out(j):
            c.start()
        rs_release(last, j)
        return carry

    lax.fori_loop(0, BLOCKS, scatter_last, 0)

    ls_copy.wait()
    both = (ls_out[...] + ls_in[...]) * (1.0 / tokens)
    loss[0] = both[0, lanes - 1]
    loss[1] = both[1, lanes - 1]
    for o in range(HALF):
        dw_copy(MBLOCKS - 1, o).wait_send()
        dw_out(MBLOCKS - 1, o).wait()
    for j in range(BLOCKS):
        for c in dx_out(j):
            c.wait()


def copy_kernel(loss, dw, dxa, dxb, loss_out, dw_out, dxa_out, dxb_out, dw_v, dxa_v, dxb_v, in_sem, out_sem):
    moves = []
    for n, (src, via, dst) in enumerate(((dw, dw_v, dw_out), (dxa, dxa_v, dxa_out), (dxb, dxb_v, dxb_out))):
        parts = MBLOCKS // 2 if n == 0 else 1
        size = src.shape[0] // parts
        for p in range(parts):
            at = pl.ds(p * size, size)
            moves.append((pltpu.make_async_copy(src.at[at], via.at[at], in_sem.at[n, p]),
                          pltpu.make_async_copy(via.at[at], dst.at[at], out_sem.at[n, p])))
    for load, _ in moves:
        load.start()
    loss_out[0] = loss[0]
    loss_out[1] = loss[1]
    for load, store in moves:
        load.wait()
        store.start()
    for _, store in moves:
        store.wait()


def solution(mesh):
    group = mesh.shape["tp"]
    chips = group // 2

    def local_step(x_a, x_b, labels_a, labels_b, w_local):
        rows, hidden = x_a.shape
        shard = w_local.shape[1]
        slot_rows = 2 * rows
        all_rows = chips * slot_rows
        hb = hidden // BLOCKS
        pc = shard // HALF
        mb_rows = hidden // MBLOCKS
        any_spec = pl.BlockSpec(memory_space=pl.ANY)
        vmem_spec = pl.BlockSpec(memory_space=pltpu.VMEM)
        out = pl.pallas_call(
            functools.partial(head_kernel, group),
            name="head",
            out_shape=(
                jax.ShapeDtypeStruct((2,), F32),
                jax.ShapeDtypeStruct((hidden, shard), BF16),
                jax.ShapeDtypeStruct((rows, hidden), BF16),
                jax.ShapeDtypeStruct((rows, hidden), BF16),
                jax.ShapeDtypeStruct((chips, HALF, 2, slot_rows, pc), F32),
                jax.ShapeDtypeStruct((chips, HALF, slot_rows, 128), F32),
                jax.ShapeDtypeStruct((hidden, all_rows), BF16),
            ),
            in_specs=[any_spec, any_spec, vmem_spec, vmem_spec, any_spec],
            out_specs=(pl.BlockSpec(memory_space=pltpu.SMEM),) + (any_spec,) * 6,
            scratch_shapes=[
                pltpu.VMEM((PIECES, hidden, pc), BF16),
                pltpu.VMEM((PIECES, all_rows, pc), BF16),
                pltpu.VMEM((2, HALF, 2, slot_rows, pc), F32),
                pltpu.VMEM((2, HALF, slot_rows, 128), F32),
                pltpu.VMEM((2, mb_rows, all_rows), BF16),
                pltpu.VMEM((BUFS, BLOCKS, slot_rows, hb), F32),
                pltpu.VMEM((HALF, mb_rows, pc), BF16),
                pltpu.VMEM((slot_rows, 128), F32),
                pltpu.VMEM((slot_rows, 128), F32),
                pltpu.VMEM((slot_rows, 128), F32),
                pltpu.VMEM((2, slot_rows, 128), jnp.int32),
                pltpu.VMEM((chips, 2, rows), F32),
                pltpu.VMEM((chips, RINGS, 4, 128), F32),
                pltpu.VMEM((chips, RINGS, 4, 128), F32),
                pltpu.VMEM((chips, 8, 128), F32),
                pltpu.VMEM((8, 128), F32),
                pltpu.VMEM((8, 128), F32),
                pltpu.VMEM((8, 128), F32),
            ],
            compiler_params=pltpu.CompilerParams(
                collective_id=0, has_side_effects=True, vmem_limit_bytes=67043328),
        )(x_a, x_b, labels_a.reshape(1, rows), labels_b.reshape(1, rows), w_local)
        results = out[:4]
        return pl.pallas_call(
            copy_kernel,
            name="results",
            out_shape=tuple(jax.ShapeDtypeStruct(v.shape, v.dtype) for v in results),
            in_specs=[pl.BlockSpec(memory_space=pltpu.SMEM), any_spec, any_spec, any_spec],
            out_specs=(pl.BlockSpec(memory_space=pltpu.SMEM), any_spec, any_spec, any_spec),
            scratch_shapes=[pltpu.VMEM(v.shape, v.dtype) for v in results[1:]] + [
                pltpu.SemaphoreType.DMA((3, MBLOCKS)), pltpu.SemaphoreType.DMA((3, MBLOCKS))],
        )(*results)

    row_spec = P(("dp", "tp"), None)
    label_spec = P(("dp", "tp"))
    return jax.shard_map(local_step, mesh=mesh, in_specs=(row_spec, row_spec, label_spec, label_spec, P(None, "tp")), out_specs=(P("dp"), P("dp", "tp"), row_spec, row_spec), check_vma=False)
```

```python
import functools
import math

import jax
import jax.numpy as jnp
from jax import lax
from jax.experimental import pallas as pl
from jax.experimental.pallas import tpu as pltpu
from jax.sharding import PartitionSpec as P

MESH = pl.DeviceIdType.MESH
F32 = jnp.float32
BF16 = jnp.bfloat16
RINGS = 4
BLOCKS = 4
HALF = 3
PIECES = 2 * HALF
MBLOCKS = 8
BUFS = 3
AHEAD = (1, 5, 10)


class Both:
    def __init__(self, *copies):
        self.copies = copies

    def start(self):
        for c in self.copies:
            c.start()

    def wait(self):
        for c in self.copies:
            c.wait()


def head_kernel(group, *refs):
    chips = group // 2
    dma = pltpu.SemaphoreType.DMA
    regular = pltpu.SemaphoreType.REGULAR
    pl.run_scoped(
        functools.partial(head_body, group, *refs),
        x_sem=dma((2 * BLOCKS,)), w_sem=dma((HALF,)), wp_sem=dma((2, HALF)), lab_sem=dma((2, chips)), sync=regular((3,)),
        ag_send=dma((4, BLOCKS * RINGS)), ag_recv=dma((chips, BLOCKS * RINGS)),
        e_sem=dma((2, HALF)), er_sem=dma((2, 2)), xt_sem=dma((2, MBLOCKS)), xtr_sem=dma((2,)),
        run_send=dma((chips, RINGS)), run_recv=dma((chips, RINGS)), bc_send=dma((chips,)), bc_recv=dma((chips,)),
        ls_sem=dma((2,)), rs_send=dma((BUFS, BLOCKS, RINGS)), rs_recv=dma((BUFS, BLOCKS, RINGS)),
        credit=regular((BLOCKS, RINGS)), dw_send=dma((HALF,)), dw_recv=dma((2, HALF)), dw_credit=regular,
        dwo_sem=dma((HALF,)), dxo_sem=dma((BLOCKS, 2)))


def head_body(group, xa, xb, la, lb, w, loss, dw, dxa, dxb, e_hbm, m_hbm, xt_hbm,
              wv, xg, stage, shift, xtb, buf, dwb, m_run, s_run, t_run, labc,
              lab_in, run_out, run_in, bc_in, bc_out, ls_out, ls_in,
              x_sem, w_sem, wp_sem, lab_sem, sync, ag_send, ag_recv, e_sem, er_sem, xt_sem, xtr_sem, run_send, run_recv,
              bc_send, bc_recv, ls_sem, rs_send, rs_recv, credit, dw_send, dw_recv, dw_credit, dwo_sem, dxo_sem):
    chips = group // 2
    side = math.isqrt(chips)
    rows = xa.shape[0]
    slot_rows = 2 * rows
    rt = slot_rows // RINGS
    hb = xg.shape[2]
    pc = hb
    shard = w.shape[1]
    tokens = rows * group
    mb_rows = w.shape[0] // MBLOCKS
    lanes = lab_in.shape[2]

    me = lax.axis_index("tp")
    core = lax.rem(me, 2)
    chip = me // 2
    partner = me + 1 - 2 * core
    cx = lax.rem(chip, side)
    cy = chip // side
    diag = lax.rem(cx + cy, side)
    pos = (side * cy + diag, side * lax.rem(cx + 1, side) + diag)

    def dev(c):
        return {"tp": 2 * c + core}

    def chip_at(cycle, p):
        major, minor = p // side, lax.rem(p, side)
        if cycle == 0:
            yy = major
            xx = lax.rem(minor - major + side, side)
        else:
            xx = lax.rem(major + side - 1, side)
            yy = lax.rem(minor + 1 - major + side, side)
        return yy * side + xx

    def source(r, k):
        sign = -1 if r % 2 == 0 else 1
        return chip_at(r // 2, lax.rem(pos[r // 2] + sign * k + 2 * chips, chips))

    up = [source(r, 1) for r in range(RINGS)]
    down = [source(r, -1) for r in range(RINGS)]

    for b in range(BLOCKS):
        cols = pl.ds(b * hb, hb)
        pltpu.make_async_copy(xa.at[:, cols], xg.at[b, pl.ds(0, rows)], x_sem.at[2 * b]).start()
        pltpu.make_async_copy(xb.at[:, cols], xg.at[b, pl.ds(rows, rows)], x_sem.at[2 * b + 1]).start()

    def w_load(h):
        return pltpu.make_async_copy(w.at[:, pl.ds(h * pc, pc)], wv.at[h], w_sem.at[h])

    def w_swap(h):
        return pltpu.make_async_remote_copy(
            src_ref=w.at[:, pl.ds(h * pc, pc)], dst_ref=wv.at[HALF + h], send_sem=wp_sem.at[0, h],
            recv_sem=wp_sem.at[1, h], device_id={"tp": partner}, device_id_type=MESH)

    for h in range(HALF):
        w_load(h).start()

    barrier = pltpu.get_barrier_semaphore()

    def is_near(c):
        near = c == up[0]
        for r in range(1, RINGS):
            near = near | (c == up[r])
        return near

    for r in range(RINGS):
        pl.semaphore_signal(barrier, inc=1, device_id=dev(up[r]), device_id_type=MESH)
    pl.semaphore_signal(barrier, inc=1, device_id={"tp": partner}, device_id_type=MESH)
    my_lab = lab_in.at[chip]
    my_lab[0:1, :] = la[...].astype(F32)
    my_lab[1:2, :] = lb[...].astype(F32)
    buf[0] = jnp.zeros(buf.shape[1:], F32)
    with jax.named_scope("barrier"):
        pl.semaphore_wait(barrier, RINGS + 1)
    for h in range(HALF):
        w_swap(h).start()


    def ag_copy(k, j, r):
        src = xg.at[j, pl.ds(pl.multiple_of(k * slot_rows + r * rt, rt), rt)]
        dst = xg.at[j, pl.ds(pl.multiple_of((k + 1) * slot_rows + r * rt, rt), rt)]
        return pltpu.make_async_remote_copy(
            src_ref=src, dst_ref=dst, send_sem=ag_send.at[lax.rem(k, 4), j * RINGS + r],
            recv_sem=ag_recv.at[k + 1, j * RINGS + r], device_id=dev(down[r]), device_id_type=MESH)

    for b in range(BLOCKS):
        cols = pl.ds(b * hb, hb)
        pltpu.make_async_copy(xa.at[:, cols], xg.at[b, pl.ds(0, rows)], x_sem.at[2 * b]).wait()
        pltpu.make_async_copy(xb.at[:, cols], xg.at[b, pl.ds(rows, rows)], x_sem.at[2 * b + 1]).wait()
        for r in range(RINGS):
            ag_copy(0, b, r).start()

    def lab_copy(d):
        return pltpu.make_async_remote_copy(
            src_ref=lab_in.at[chip], dst_ref=lab_in.at[chip], send_sem=lab_sem.at[0, d], recv_sem=lab_sem.at[1, d],
            device_id=dev(lax.rem(chip + d, chips)), device_id_type=MESH)

    def lab_start(near):
        def go(d, carry):
            is_to = is_near(lax.rem(chip + d, chips))

            @pl.when(is_to if near else jnp.logical_not(is_to))
            def _():
                lab_copy(d).start()
            return carry
        lax.fori_loop(1, chips, go, 0)

    def lab_wait(near):
        def go(d, carry):
            is_from = is_near(lax.rem(chip + chips - d, chips))

            @pl.when(is_from if near else jnp.logical_not(is_from))
            def _():
                lab_copy(d).wait_recv()
            return carry
        lax.fori_loop(1, chips, go, 0)

    def sync_signal(n):
        for r in range(RINGS):
            pl.semaphore_signal(sync.at[n], inc=1, device_id=dev(up[r]), device_id_type=MESH)

    def sync_wait(n):
        pl.semaphore_wait(sync.at[n], RINGS)

    lab_start(True)
    sync_signal(0)
    for h in range(HALF):
        w_load(h).wait()

    sub_i = lax.broadcasted_iota(jnp.int32, (rt, 128), 0)
    lane_i = lax.broadcasted_iota(jnp.int32, (rt, 128), 1)
    eye = sub_i == lane_i
    row_lane = lax.broadcasted_iota(jnp.int32, (1, 128), 1)
    lab_sub = lax.broadcasted_iota(jnp.int32, (rt, lanes), 0)
    lab_lane = lax.broadcasted_iota(jnp.int32, (rt, lanes), 1)

    def to_row(col):
        return jnp.sum(jnp.where(eye, col, 0.0), axis=0, keepdims=True)

    def to_col(row):
        return jnp.sum(jnp.where(eye, row, 0.0), axis=1, keepdims=True)

    def fill_labels(lab, sources):
        for r in range(RINGS):
            row = lab_in[sources[r], r // 2:r // 2 + 1, :]
            col = jnp.sum(jnp.where(lab_lane == lab_sub + (r % 2) * rt, row, 0.0), axis=1, keepdims=True)
            lab[r * rt:(r + 1) * rt, :] = jnp.broadcast_to(col.astype(jnp.int32), (rt, 128))

    def sources_of(k):
        return [source(r, k) for r in range(RINGS)]

    def base(lp):
        owner = me if lp < HALF else partner
        return owner * shard + (lp % HALF) * pc

    chunk = slot_rows // 8
    per = pc // 128
    lane_at = [lax.broadcasted_iota(jnp.int32, (chunk, 128), 1) + i * 128 for i in range(per)]
    vregs = [(i // per, i % per, slice(i % per * 128, (i % per + 1) * 128)) for i in range(2 * per)]

    def hits(lab_rows, pair):
        rel = [lab_rows - base(2 * pair), lab_rows - base(2 * pair + 1)]
        return [lane_at[n] == rel[h] for h, n, _ in vregs]

    def z_dot(k0, lp):
        z = None
        for b in range(BLOCKS):
            part = jnp.dot(xg[b, pl.ds(k0, slot_rows), :], wv[lp, b * hb:(b + 1) * hb, :], preferred_element_type=F32)
            z = part if z is None else z + part
        stage[0, lp // 2, lp % 2] = z

    def z_stats(pair, lab):
        for c in range(8):
            rs = slice(c * chunk, (c + 1) * chunk)
            z = [stage[0, pair, h, rs, cs] for h, _, cs in vregs]
            m = functools.reduce(jnp.maximum, z)
            e = [jnp.exp(v - m) for v in z]
            t = functools.reduce(jnp.add, [jnp.where(h, v, 0.0) for h, v in zip(hits(lab[rs, :], pair), z)])
            s = functools.reduce(jnp.add, e)
            for (h, _, cs), v in zip(vregs, e):
                stage[0, pair, h, rs, cs] = v
            shift[0, pair, rs, :] = m
            if pair == 0:
                m_run[rs, :] = m
                s_run[rs, :] = s
                t_run[rs, :] = t
            else:
                old = m_run[rs, :]
                new = jnp.maximum(old, m)
                m_run[rs, :] = new
                s_run[rs, :] = s_run[rs, :] * jnp.exp(old - new) + s * jnp.exp(m - new)
                t_run[rs, :] = t_run[rs, :] + t

    def e_write(slot, pair):
        return Both(pltpu.make_async_copy(stage.at[0, pair], e_hbm.at[slot, pair], e_sem.at[0, pair]),
                    pltpu.make_async_copy(shift.at[0, pair], m_hbm.at[slot, pair], e_sem.at[1, pair]))

    def xt_write(slot, mb):
        return pltpu.make_async_copy(
            xtb.at[lax.rem(slot, 2), :, pl.ds(mb * mb_rows, slot_rows)],
            xt_hbm.at[pl.ds(mb * mb_rows, mb_rows), pl.ds(pl.multiple_of(slot * slot_rows, slot_rows), slot_rows)],
            xt_sem.at[lax.rem(slot, 2), mb])

    def run_copy(slot, r):
        return pltpu.make_async_remote_copy(
            src_ref=run_out.at[slot, r], dst_ref=run_in.at[slot + 1, r], send_sem=run_send.at[slot, r],
            recv_sem=run_recv.at[slot + 1, r], device_id=dev(down[r]), device_id_type=MESH)

    def join_stats(slot):
        with jax.named_scope("stats"):
            lane_m = m_run[...]
            m = jnp.max(lane_m, axis=1, keepdims=True)
            s = jnp.sum(s_run[...] * jnp.exp(lane_m - m), axis=1, keepdims=True)
            t = jnp.sum(t_run[...], axis=1, keepdims=True)
            rows_mst = [[to_row(v[r * rt:(r + 1) * rt]) for v in (m, s, t)] for r in range(RINGS)]

        @pl.when(slot >= 1)
        def _():
            for r in range(RINGS):
                run_copy(slot - 1, r).wait_recv()
        for r in range(RINGS):
            m_r, s_r, t_r = rows_mst[r]
            m_in = run_in[slot, r, 0:1, :]
            m_new = jnp.maximum(m_in, m_r)
            run_out[slot, r, 0:1, :] = m_new
            run_out[slot, r, 1:2, :] = s_r * jnp.exp(m_r - m_new) + run_in[slot, r, 1:2, :] * jnp.exp(m_in - m_new)
            run_out[slot, r, 2:3, :] = t_r + run_in[slot, r, 2:3, :]

    def poll(k, j):
      with jax.named_scope("poll"):
        @pl.when(k < chips)
        def _():
            for r in range(RINGS):
                ag_copy(k - 1, j, r).wait_recv()

        @pl.when(k < chips - 1)
        def _():
            @pl.when(k >= 4)
            def _():
                for r in range(RINGS):
                    ag_copy(k - 4, j, r).wait_send()
            for r in range(RINGS):
                ag_copy(k, j, r).start()

    fill_labels(labc.at[0], [chip] * RINGS)
    for r in range(RINGS):
        run_in[0, r, 0:1, :] = jnp.full((1, 128), -jnp.inf, F32)
        run_in[0, r, 1:3, :] = jnp.zeros((2, 128), F32)

    def poll_ahead(k, n):
        for lead, (first, end) in enumerate(((AHEAD[2] + 1, chips + 1), (AHEAD[1] + 1, AHEAD[2] + 1), (AHEAD[0] + 1, AHEAD[1] + 1))):
            @pl.when((k >= first) & (k < end))
            def _():
                poll(k + (n + lead) // BLOCKS, (n + lead) % BLOCKS)

        @pl.when(k <= AHEAD[0])
        def _():
            poll(k + (1 if n == 3 else 0), 2 if n == 3 else n)

    def gather_step(k, carry):
        slot = k - 1
        k0 = pl.multiple_of(slot * slot_rows, slot_rows)
        here = labc.at[lax.rem(slot, 2)]
        other = labc.at[lax.rem(slot + 1, 2)]
        ahead = sources_of(lax.rem(slot + 1, chips))

        @pl.when(slot >= 1)
        def _():
            e_write(slot - 1, 0).wait()

        @pl.when(slot >= 2)
        def _():
            for mb in range(MBLOCKS):
                xt_write(slot - 2, mb).wait()

        def transpose(first, end):
            for mb in range(first, end):
                at = mb * mb_rows % hb
                xtb[lax.rem(slot, 2), :, mb * mb_rows:(mb + 1) * mb_rows] = (
                    xg[mb * mb_rows // hb, pl.ds(k0, slot_rows), at:at + mb_rows].T)

        with jax.named_scope("u0"):
            transpose(0, 3)
            z_dot(k0, 0)
            z_dot(k0, 1)
            z_stats(2, other)

        @pl.when(slot == 0)
        def _():
            poll(k, 0)
        poll_ahead(k, 1)

        @pl.when(slot >= 1)
        def _():
            e_write(slot - 1, 2).start()
            join_stats(slot - 1)
            for r in range(RINGS):
                run_copy(slot - 1, r).start()
            e_write(slot - 1, 1).wait()

        @pl.when(slot == 0)
        def _():
            sync_wait(0)
            sync_signal(1)
            w_swap(0).wait()

        with jax.named_scope("u1"):
            transpose(3, 6)
            z_dot(k0, 2)
            z_dot(k0, 3)
            z_stats(0, here)
        e_write(slot, 0).start()
        poll_ahead(k, 2)

        @pl.when(slot == 0)
        def _():
            sync_wait(1)
            sync_signal(2)
            lab_wait(True)
            poll(k, 3)
            poll(k + 1, 0)
            poll(k + 1, 1)
            w_swap(1).wait()
            w_swap(2).wait()

        @pl.when(slot >= 1)
        def _():
            e_write(slot - 1, 2).wait()

        @pl.when(slot == 1)
        def _():
            lab_wait(False)

        with jax.named_scope("u2"):
            z_dot(k0, 4)
            z_dot(k0, 5)
            z_stats(1, here)
            fill_labels(other, ahead)
            transpose(6, 8)
        e_write(slot, 1).start()
        for mb in range(MBLOCKS):
            xt_write(slot, mb).start()

        poll_ahead(k, 3)

        @pl.when((k != AHEAD[0]) & (k != AHEAD[1]) & (k != AHEAD[2]))
        def _():
            poll_ahead(k, 4)

        @pl.when(slot == 0)
        def _():
            sync_wait(2)
            lab_start(False)
        return carry

    lax.fori_loop(1, chips + 1, gather_step, 0)
    def e_read(g):
        slot, half = lax.rem(2 * chips - g, chips), lax.rem(g + 1, 2)
        return Both(pltpu.make_async_copy(e_hbm.at[slot], stage.at[half], er_sem.at[0, half]),
                    pltpu.make_async_copy(m_hbm.at[slot], shift.at[half], er_sem.at[1, half]))

    e_read(2).start()
    with jax.named_scope("flush"):
        z_stats(2, labc.at[(chips - 1) % 2])
    e_write(chips - 1, 2).start()
    join_stats(chips - 1)

    inside = row_lane < rt
    parts = []
    for r in range(RINGS):
        m, s, t = (run_out[chips - 1, r, i:i + 1, :] for i in range(3))
        bc_out[r:r + 1, :] = m
        bc_out[RINGS + r:RINGS + r + 1, :] = s
        parts.append(jnp.sum(jnp.where(inside, m + jnp.log(s) - t, 0.0), axis=1, keepdims=True))
    for mb in range(2):
        both = jnp.broadcast_to(parts[2 * mb] + parts[2 * mb + 1], (1, 128))
        bc_out[mb:mb + 1, :] = jnp.where(inside, bc_out[mb:mb + 1, :], both)
    bc_in[chip] = bc_out[...]

    def bc_copy(d):
        return pltpu.make_async_remote_copy(
            src_ref=bc_out, dst_ref=bc_in.at[chip], send_sem=bc_send.at[d], recv_sem=bc_recv.at[d],
            device_id=dev(lax.rem(chip + d, chips)), device_id_type=MESH)

    def bc_start(d, carry):
        bc_copy(d).start()
        return carry

    def bc_wait_first(d, carry):
        @pl.when(is_near(lax.rem(chip + chips - d, chips)))
        def _():
            bc_copy(d).wait_recv()
        return carry

    def bc_wait_rest(d, carry):
        @pl.when(jnp.logical_not(is_near(lax.rem(chip + chips - d, chips))))
        def _():
            bc_copy(d).wait_recv()
        bc_copy(d).wait_send()
        lab_copy(d).wait_send()
        for r in range(RINGS):
            run_copy(d - 1, r).wait_send()
        return carry

    ls_copy = pltpu.make_async_remote_copy(
        src_ref=ls_out, dst_ref=ls_in, send_sem=ls_sem.at[0], recv_sem=ls_sem.at[1],
        device_id={"tp": partner}, device_id_type=MESH)

    lax.fori_loop(1, chips, bc_start, 0)

    def xt_read(mb):
        return pltpu.make_async_copy(
            xt_hbm.at[pl.ds(pl.multiple_of(mb * mb_rows, mb_rows), mb_rows), :], xtb.at[lax.rem(mb, 2)],
            xtr_sem.at[lax.rem(mb, 2)])

    def form_g(g):
        slot = lax.rem(2 * chips - g, chips)
        half = lax.rem(g + 1, 2)
        k0 = pl.multiple_of(slot * slot_rows, slot_rows)
        sources = sources_of(slot)
        holders = sources_of(lax.rem(slot + 1, chips))
        lab = labc.at[0]
        fill_labels(lab, sources)
        for r in range(RINGS):
            rs = slice(r * rt, (r + 1) * rt)
            m_run[rs, :] = jnp.broadcast_to(to_col(bc_in[holders[r], r:r + 1, :]), (rt, 128))
            s_run[rs, :] = jnp.broadcast_to(
                1.0 / (to_col(bc_in[holders[r], RINGS + r:RINGS + r + 1, :]) * tokens), (rt, 128))
        for pair in range(HALF):
            for c in range(8):
                rs = slice(c * chunk, (c + 1) * chunk)
                krs = pl.ds(pl.multiple_of(k0 + c * chunk, chunk), chunk)
                scale = jnp.exp(shift[half, pair, rs, :] - m_run[rs, :]) * s_run[rs, :]
                for (h, _, cs), hit in zip(vregs, hits(lab[rs, :], pair)):
                    v = stage[half, pair, h, rs, cs] * scale - jnp.where(hit, 1.0 / tokens, 0.0)
                    xg[2 * pair + h, krs, cs] = v.astype(BF16)

    with jax.named_scope("g_first"):
        form_g(1)

    def rs_copy(s, j, r):
        b0, b1 = lax.rem(s, BUFS), lax.rem(s + 1, BUFS)
        return pltpu.make_async_remote_copy(
            src_ref=buf.at[b0, j, pl.ds(r * rt, rt)], dst_ref=buf.at[b1, j, pl.ds(r * rt, rt)],
            send_sem=rs_send.at[b0, j, r], recv_sem=rs_recv.at[b1, j, r],
            device_id=dev(up[r]), device_id_type=MESH)

    def tile_at(h, o):
        return (h, o // 2, lax.rem(o, 2))

    def dw_copy(mb, o):
        return pltpu.make_async_remote_copy(
            src_ref=stage.at[tile_at(0, o)], dst_ref=stage.at[tile_at(1, lax.rem(mb, 2) * HALF + o)],
            send_sem=dw_send.at[o],
            recv_sem=dw_recv.at[lax.rem(mb, 2), o], device_id={"tp": partner}, device_id_type=MESH)

    def dw_out(mb, o):
        return pltpu.make_async_copy(
            dwb.at[o], dw.at[pl.ds(pl.multiple_of(mb * mb_rows, mb_rows), mb_rows),
                             pl.ds(pl.multiple_of(o * pc, pc), pc)], dwo_sem.at[o])

    def dx_out(j):
        cols = pl.ds(pl.multiple_of(j * hb, hb), hb)
        return (pltpu.make_async_copy(xtb.at[0, pl.ds(0, rows), cols], dxa.at[:, cols], dxo_sem.at[j, 0]),
                pltpu.make_async_copy(xtb.at[0, pl.ds(rows, rows), cols], dxb.at[:, cols], dxo_sem.at[j, 1]))

    last = chips - 1
    dw_from = 3 * BLOCKS
    own_from = last * BLOCKS
    assert own_from - dw_from == MBLOCKS * PIECES and dw_from - 1 + BLOCKS == chips - 1

    def dx_dot(slot, j):
        k0 = pl.multiple_of(slot * slot_rows, slot_rows)
        tile = None
        for lp in range(PIECES):
            part = lax.dot_general(
                xg[lp, pl.ds(k0, slot_rows), :],
                wv[lp, pl.ds(pl.multiple_of(j * hb, hb), hb), :],
                (((1,), (1,)), ((), ())), preferred_element_type=F32)
            tile = part if tile is None else tile + part
        return tile

    def rs_arrive(s, j):
        with jax.named_scope("rs_wait"):
            for r in range(RINGS):
                rs_copy(s - 1, j, r).wait_recv()

    def rs_send_on(s, j):
        @pl.when(s >= 2)
        def _():
            for r in range(RINGS):
                pl.semaphore_wait(credit.at[j, r], 1)
        for r in range(RINGS):
            rs_copy(s, j, r).start()

    def rs_release(s, j):
        for r in range(RINGS):
            rs_copy(s - 1, j, r).wait_send()

        @pl.when(s - 1 <= last - 3)
        def _():
            for r in range(RINGS):
                pl.semaphore_signal(credit.at[j, r], inc=1, device_id=dev(down[r]), device_id_type=MESH)

    def scatter_g(i, carry):
        s = i // BLOCKS
        j = lax.rem(i, BLOCKS)
        b0 = lax.rem(s, BUFS)
        double = s == 1
        g = jnp.where(s == 0, i + 1, jnp.where(double, 2 * i - BLOCKS + 1, i + BLOCKS + 1))

        @pl.when(s >= 1)
        def _():
            rs_arrive(s, j)

        @pl.when(i == 2)
        def _():
            with jax.named_scope("bc_rest"):
                lax.fori_loop(1, chips, bc_wait_rest, 0)

        e_read(g).wait()
        with jax.named_scope("dx_g"):
            buf[b0, j] = buf[b0, j] + dx_dot(last - s, j)
            form_g(g)
        rs_send_on(s, j)

        @pl.when(g + 2 <= chips)
        def _():
            e_read(g + 2).start()

        @pl.when(double)
        def _():
            e_read(g + 1).wait()
            with jax.named_scope("g"):
                form_g(g + 1)

            @pl.when(g + 3 <= chips)
            def _():
                e_read(g + 3).start()

        @pl.when(s >= 1)
        def _():
            rs_release(s, j)
        return carry

    with jax.named_scope("dx_first"):
        buf[0, 0] = dx_dot(last, 0)
    rs_send_on(0, 0)
    for pair in range(HALF):
        e_write(chips - 1, pair).wait()
    e_read(3).start()
    for mb in range(MBLOCKS):
        xt_write(chips - 2, mb).wait()
        xt_write(chips - 1, mb).wait()
    xt_read(0).start()
    for k in range(chips - 5, chips - 1):
        for j in range(BLOCKS):
            for r in range(RINGS):
                ag_copy(k, j, r).wait_send()

    with jax.named_scope("bc_first"):
        lax.fori_loop(1, chips, bc_wait_first, 0)

    lax.fori_loop(1, dw_from, scatter_g, 0)
    pl.semaphore_signal(dw_credit, inc=1, device_id={"tp": partner}, device_id_type=MESH)
    total = bc_in[0]
    for c in range(1, chips):
        total = total + bc_in[c]
    ls_out[...] = total
    ls_copy.start()

    def scatter_dw(i, carry):
        s = i // BLOCKS
        j = lax.rem(i, BLOCKS)
        b0 = lax.rem(s, BUFS)
        q = i - dw_from
        mb = q // PIECES
        o = lax.rem(q, PIECES)
        rs_arrive(s, j)

        @pl.when(o == 0)
        def _():
            xt_read(mb).wait()

            @pl.when(mb < MBLOCKS - 1)
            def _():
                xt_read(mb + 1).start()

        @pl.when((o < HALF) & (mb >= 1))
        def _():
            dw_copy(mb - 1, o).wait_send()

        with jax.named_scope("dx_dw"):
            buf[b0, j] = buf[b0, j] + dx_dot(last - s, j)
            stage[tile_at(0, o)] = jnp.dot(xtb[lax.rem(mb, 2)], xg[lax.rem(o + HALF, PIECES)], preferred_element_type=F32)
        rs_send_on(s, j)

        @pl.when((o == 0) & (mb != 1))
        def _():
            pl.semaphore_wait(dw_credit, 1)

        @pl.when(o < HALF)
        def _():
            dw_copy(mb, o).start()

        @pl.when(o >= HALF)
        def _():
            h = o - HALF
            dw_copy(mb, h).wait_recv()

            @pl.when(mb >= 1)
            def _():
                dw_out(mb - 1, h).wait()
            dwb[h] = (stage[tile_at(0, o)] + stage[tile_at(1, lax.rem(mb, 2) * HALF + h)]).astype(BF16)
            dw_out(mb, h).start()

            @pl.when((h == HALF - 1) & (mb < MBLOCKS - 2))
            def _():
                pl.semaphore_signal(dw_credit, inc=1, device_id={"tp": partner}, device_id_type=MESH)

        rs_release(s, j)
        return carry

    lax.fori_loop(dw_from, own_from, scatter_dw, 0)

    def scatter_last(j, carry):
        with jax.named_scope("own"):
            stage[0, HALF - 1, 1] = dx_dot(0, j)
        rs_arrive(last, j)
        with jax.named_scope("out"):
            xtb[0, 0:slot_rows, pl.ds(pl.multiple_of(j * hb, hb), hb)] = (
                buf[last % BUFS, j] + stage[0, HALF - 1, 1]).astype(BF16)
        for c in dx_out(j):
            c.start()
        rs_release(last, j)
        return carry

    lax.fori_loop(0, BLOCKS, scatter_last, 0)

    ls_copy.wait()
    both = (ls_out[...] + ls_in[...]) * (1.0 / tokens)
    loss[0] = both[0, lanes - 1]
    loss[1] = both[1, lanes - 1]
    for o in range(HALF):
        dw_copy(MBLOCKS - 1, o).wait_send()
        dw_out(MBLOCKS - 1, o).wait()
    for j in range(BLOCKS):
        for c in dx_out(j):
            c.wait()


def copy_kernel(loss, dw, dxa, dxb, loss_out, dw_out, dxa_out, dxb_out, dw_v, dxa_v, dxb_v, in_sem, out_sem):
    moves = []
    for n, (src, via, dst) in enumerate(((dw, dw_v, dw_out), (dxa, dxa_v, dxa_out), (dxb, dxb_v, dxb_out))):
        parts = MBLOCKS // 2 if n == 0 else 1
        size = src.shape[0] // parts
        for p in range(parts):
            at = pl.ds(p * size, size)
            moves.append((pltpu.make_async_copy(src.at[at], via.at[at], in_sem.at[n, p]),
                          pltpu.make_async_copy(via.at[at], dst.at[at], out_sem.at[n, p])))
    for load, _ in moves:
        load.start()
    loss_out[0] = loss[0]
    loss_out[1] = loss[1]
    for load, store in moves:
        load.wait()
        store.start()
    for _, store in moves:
        store.wait()


def solution(mesh):
    group = mesh.shape["tp"]
    chips = group // 2

    def local_step(x_a, x_b, labels_a, labels_b, w_local):
        rows, hidden = x_a.shape
        shard = w_local.shape[1]
        slot_rows = 2 * rows
        all_rows = chips * slot_rows
        hb = hidden // BLOCKS
        pc = shard // HALF
        mb_rows = hidden // MBLOCKS
        any_spec = pl.BlockSpec(memory_space=pl.ANY)
        vmem_spec = pl.BlockSpec(memory_space=pltpu.VMEM)
        out = pl.pallas_call(
            functools.partial(head_kernel, group),
            name="head",
            out_shape=(
                jax.ShapeDtypeStruct((2,), F32),
                jax.ShapeDtypeStruct((hidden, shard), BF16),
                jax.ShapeDtypeStruct((rows, hidden), BF16),
                jax.ShapeDtypeStruct((rows, hidden), BF16),
                jax.ShapeDtypeStruct((chips, HALF, 2, slot_rows, pc), F32),
                jax.ShapeDtypeStruct((chips, HALF, slot_rows, 128), F32),
                jax.ShapeDtypeStruct((hidden, all_rows), BF16),
            ),
            in_specs=[any_spec, any_spec, vmem_spec, vmem_spec, any_spec],
            out_specs=(pl.BlockSpec(memory_space=pltpu.SMEM),) + (any_spec,) * 6,
            scratch_shapes=[
                pltpu.VMEM((PIECES, hidden, pc), BF16),
                pltpu.VMEM((PIECES, all_rows, pc), BF16),
                pltpu.VMEM((2, HALF, 2, slot_rows, pc), F32),
                pltpu.VMEM((2, HALF, slot_rows, 128), F32),
                pltpu.VMEM((2, mb_rows, all_rows), BF16),
                pltpu.VMEM((BUFS, BLOCKS, slot_rows, hb), F32),
                pltpu.VMEM((HALF, mb_rows, pc), BF16),
                pltpu.VMEM((slot_rows, 128), F32),
                pltpu.VMEM((slot_rows, 128), F32),
                pltpu.VMEM((slot_rows, 128), F32),
                pltpu.VMEM((2, slot_rows, 128), jnp.int32),
                pltpu.VMEM((chips, 2, rows), F32),
                pltpu.VMEM((chips, RINGS, 4, 128), F32),
                pltpu.VMEM((chips, RINGS, 4, 128), F32),
                pltpu.VMEM((chips, 8, 128), F32),
                pltpu.VMEM((8, 128), F32),
                pltpu.VMEM((8, 128), F32),
                pltpu.VMEM((8, 128), F32),
            ],
            compiler_params=pltpu.CompilerParams(
                collective_id=0, has_side_effects=True, vmem_limit_bytes=67043328),
        )(x_a, x_b, labels_a.reshape(1, rows), labels_b.reshape(1, rows), w_local)
        results = out[:4]
        return pl.pallas_call(
            copy_kernel,
            name="results",
            out_shape=tuple(jax.ShapeDtypeStruct(v.shape, v.dtype) for v in results),
            in_specs=[pl.BlockSpec(memory_space=pltpu.SMEM), any_spec, any_spec, any_spec],
            out_specs=(pl.BlockSpec(memory_space=pltpu.SMEM), any_spec, any_spec, any_spec),
            scratch_shapes=[pltpu.VMEM(v.shape, v.dtype) for v in results[1:]] + [
                pltpu.SemaphoreType.DMA((3, MBLOCKS)), pltpu.SemaphoreType.DMA((3, MBLOCKS))],
        )(*results)

    row_spec = P(("dp", "tp"), None)
    label_spec = P(("dp", "tp"))
    return jax.shard_map(local_step, mesh=mesh, in_specs=(row_spec, row_spec, label_spec, label_spec, P(None, "tp")), out_specs=(P("dp"), P("dp", "tp"), row_spec, row_spec), check_vma=False)
```
